8 devices in a mesh: dp: 1 (over z), cp: 8 (over y, x, core).
Axes of the slice: x: 2, y: 2, z: 1, core: 2. Of those that a mesh axis runs over, the one named last changes fastest.
Arguments:
- x_in: bfloat16 [1, 6144, 2048], P('dp', 'cp')
- positions: int32 [6144], P(('dp', 'cp'))
- long_factor: float32 [32], replicated
- norm_gain: float32 [2048], replicated
- w_qkv: bfloat16 [2048, 6144], replicated
- w_out: bfloat16 [2048, 2048], replicated
- grad_y: bfloat16 [1, 6144, 2048], P('dp', 'cp')
Outputs:
- output 1: bfloat16 [1, 6144, 2048], P('dp', 'cp')
- output 2: bfloat16 [1, 6144, 2048], P('dp', 'cp')
- output 3: float32 [2048], P('dp')
- output 4: float32 [2048, 6144], P('dp')
- output 5: float32 [2048, 2048], P('dp')
All inputs are finite; a program needn't handle non-finite values.
Results may differ from the reference program's by a relative error of at most 0.0138761.
Values are sent between devices in bfloat16 or wider.
A program may use at most 1 GiB of HBM per device.

```python
import math
import jax
import jax.numpy as jnp
from jax import lax

BATCH = 1
SEQ_LEN = 6144
HIDDEN = 2048
HEADS = 32
HEAD_DIM = 64
HALF_DIM = HEAD_DIM // 2
WIDTH = HEADS * HEAD_DIM
NORM_EPS = 1e-5
MSCALE = math.sqrt(1.0 + math.log(32.0) / math.log(4096.0))
SCALE = 1.0 / math.sqrt(HEAD_DIM)
QK_GAIN = 1.6
MASK_VALUE = -1e30


def setup_inputs(seed: int = 0, part: int = 0) -> dict:
    part_keys = jax.random.split(jax.random.fold_in(jax.random.key(seed), part), 3)
    shared_keys = jax.random.split(jax.random.key(seed + 1), 4)
    x_in = jax.random.normal(part_keys[0], (BATCH, SEQ_LEN, HIDDEN), jnp.float32)
    gaps = jax.random.randint(part_keys[1], (SEQ_LEN,), 1, 3)
    positions = (jnp.cumsum(gaps) - 1).astype(jnp.int32)
    grad_y = jax.random.normal(part_keys[2], (BATCH, SEQ_LEN, HIDDEN), jnp.float32)
    long_factor = jnp.exp(jax.random.uniform(shared_keys[0], (HALF_DIM,), jnp.float32, 0.0, 2.5))
    norm_gain = jax.random.uniform(shared_keys[1], (HIDDEN,), jnp.float32, 0.5, 1.5)
    col_gain = jnp.concatenate([jnp.full((2 * WIDTH,), QK_GAIN, jnp.float32), jnp.ones((WIDTH,), jnp.float32)])
    w_qkv = jax.random.normal(shared_keys[2], (HIDDEN, 3 * WIDTH), jnp.float32) * (HIDDEN ** -0.5) * col_gain
    w_out = jax.random.normal(shared_keys[3], (WIDTH, HIDDEN), jnp.float32) * (WIDTH ** -0.5)
    return {'x_in': x_in.astype(jnp.bfloat16), 'positions': positions, 'long_factor': long_factor, 'norm_gain': norm_gain, 'w_qkv': w_qkv.astype(jnp.bfloat16), 'w_out': w_out.astype(jnp.bfloat16), 'grad_y': grad_y.astype(jnp.bfloat16)}


def rope_tables(positions, long_factor):
    exponent = jnp.arange(HALF_DIM, dtype=jnp.float32) * (2.0 / HEAD_DIM)
    inv_freq = 1.0 / (long_factor * jnp.power(10000.0, exponent))
    angles = positions.astype(jnp.float32)[:, None] * inv_freq[None, :]
    angle_pair = jnp.concatenate([angles, angles], axis=-1)
    return jnp.cos(angle_pair) * MSCALE, jnp.sin(angle_pair) * MSCALE


def rotate_half(values):
    return jnp.concatenate([-values[..., HALF_DIM:], values[..., :HALF_DIM]], axis=-1)


def head_attention(blocks):
    q_head, k_head, v_head = blocks
    scores = jnp.einsum('bqd,bkd->bqk', q_head.astype(jnp.float32), k_head.astype(jnp.float32)) * SCALE
    token_idx = jnp.arange(SEQ_LEN)
    scores = jnp.where(token_idx[None, :, None] >= token_idx[None, None, :], scores, MASK_VALUE)
    attn_probs = jax.nn.softmax(scores, axis=-1).astype(jnp.bfloat16)
    return jnp.einsum('bqk,bkd->bqd', attn_probs.astype(jnp.float32), v_head.astype(jnp.float32)).astype(jnp.bfloat16)


def heads_first(tensor):
    return jnp.transpose(tensor, (2, 0, 1, 3))


def block_forward(x_in, norm_gain, w_qkv32, w_out32, cos_tab, sin_tab):
    x_float = x_in.astype(jnp.float32)
    inv_rms = lax.rsqrt(jnp.mean(x_float * x_float, axis=-1, keepdims=True) + NORM_EPS)
    normed = (x_float * inv_rms * norm_gain).astype(jnp.bfloat16)
    qkv_all = jnp.dot(normed.reshape(BATCH * SEQ_LEN, HIDDEN).astype(jnp.float32), w_qkv32)
    qkv_all = qkv_all.reshape(BATCH, SEQ_LEN, 3, HEADS, HEAD_DIM)
    cos_b = cos_tab[None, :, None, :]
    sin_b = sin_tab[None, :, None, :]
    q_rot = (qkv_all[:, :, 0] * cos_b + rotate_half(qkv_all[:, :, 0]) * sin_b).astype(jnp.bfloat16)
    k_rot = (qkv_all[:, :, 1] * cos_b + rotate_half(qkv_all[:, :, 1]) * sin_b).astype(jnp.bfloat16)
    v_val = qkv_all[:, :, 2].astype(jnp.bfloat16)
    attn_out = lax.map(jax.checkpoint(head_attention), (heads_first(q_rot), heads_first(k_rot), heads_first(v_val)))
    attn_flat = jnp.transpose(attn_out, (1, 2, 0, 3)).reshape(BATCH * SEQ_LEN, WIDTH)
    proj = jnp.dot(attn_flat.astype(jnp.float32), w_out32).reshape(BATCH, SEQ_LEN, HIDDEN)
    return (x_float + proj).astype(jnp.bfloat16)


def reference(x_in, positions, long_factor, norm_gain, w_qkv, w_out, grad_y):
    cos_tab, sin_tab = rope_tables(positions, long_factor)

    def run(x_val, gain, w_first, w_second):
        return block_forward(x_val, gain, w_first, w_second, cos_tab, sin_tab)

    y_out, pullback = jax.vjp(run, x_in, norm_gain, w_qkv.astype(jnp.float32), w_out.astype(jnp.float32))
    grad_x, grad_gain, grad_wqkv, grad_wout = pullback(grad_y)
    return y_out, grad_x, grad_gain, grad_wqkv, grad_wout
```

```python
import math
import jax
import jax.numpy as jnp
from jax import lax
from jax.experimental import pallas as pl
from jax.experimental.pallas import tpu as pltpu
from jax.sharding import PartitionSpec as P

NORM_EPS = 1e-5
MSCALE = math.sqrt(1.0 + math.log(32.0) / math.log(4096.0))
MASK_VALUE = -1e30
LOG2E = math.log2(math.e)
BF16 = jnp.bfloat16
F32 = jnp.float32
BLK = 512
VMEM_LIMIT = 60 * 1024 * 1024


def dot_nn(a, b):
    return lax.dot_general(a, b, (((1,), (0,)), ((), ())), preferred_element_type=F32)


def dot_nt(a, b):
    return lax.dot_general(a, b, (((1,), (1,)), ((), ())), preferred_element_type=F32)


def params(n=1, **kw):
    return pltpu.CompilerParams(dimension_semantics=("arbitrary",) * n, vmem_limit_bytes=VMEM_LIMIT, **kw)


def cost(flops, nbytes, trans=0):
    return pl.CostEstimate(flops=int(flops), bytes_accessed=int(nbytes), transcendentals=int(trans))


def qkv_kernel(d_ref, r_ref, wq_ref, wk_ref, wv_ref, cos_ref, sin_ref, q_out, k_out, v_out, kn_out, w_scr):
    width = wq_ref.shape[1]

    @pl.when(pl.program_id(0) == 0)
    def _():
        w_scr[0:width] = wq_ref[...].T
        w_scr[width:2 * width] = wk_ref[...].T
        w_scr[2 * width:] = wv_ref[...].T

    cos = cos_ref[...]
    sin = sin_ref[...]
    r_blk = r_ref[...]
    half = cos.shape[0]

    def rope(t):
        rows = []
        for h in range(width // (2 * half)):
            t1 = t[2 * half * h:2 * half * h + half]
            t2 = t[2 * half * h + half:2 * half * (h + 1)]
            rows += [t1 * cos - t2 * sin, t2 * cos + t1 * sin]
        return jnp.concatenate(rows, axis=0).astype(BF16)

    q_out[...] = rope(dot_nt(w_scr[0:width], r_blk)) * BF16(0.125)
    k_rot = rope(dot_nt(w_scr[width:2 * width], r_blk))
    k_out[...] = k_rot
    kn_out[...] = k_rot.T
    v_out[...] = dot_nt(w_scr[2 * width:], r_blk).astype(BF16)


def qkv_call(dev, r_all, w_qkv, cos_t, sin_t):
    seq, hidden = r_all.shape
    width = 256
    ndev = w_qkv.shape[1] // (3 * width)
    half = cos_t.shape[0]
    tr = jax.ShapeDtypeStruct((width, seq), BF16)
    wspec = lambda which: pl.BlockSpec((hidden, width), lambda i, d: (0, which * ndev + d[0]))
    tspec = pl.BlockSpec((width, BLK), lambda i, d: (0, i))
    return pl.pallas_call(
        qkv_kernel,
        out_shape=(tr, tr, tr, jax.ShapeDtypeStruct((seq, width), BF16)),
        grid_spec=pltpu.PrefetchScalarGridSpec(
            num_scalar_prefetch=1,
            grid=(seq // BLK,),
            in_specs=[
                pl.BlockSpec((BLK, hidden), lambda i, d: (i, 0)),
                wspec(0), wspec(1), wspec(2),
                pl.BlockSpec((half, BLK), lambda i, d: (0, i)),
                pl.BlockSpec((half, BLK), lambda i, d: (0, i)),
            ],
            out_specs=(tspec, tspec, tspec, pl.BlockSpec((BLK, width), lambda i, d: (i, 0))),
            scratch_shapes=[pltpu.VMEM((3 * width, hidden), BF16)],
        ),
        compiler_params=params(1),
        cost_estimate=cost(2 * seq * hidden * 3 * width, seq * hidden * 2 + seq * width * 8),
        name="qkv",
    )(dev, r_all, w_qkv, w_qkv, w_qkv, cos_t, sin_t)


def fwd_kernel(q_ref, k_ref, v_ref, o_out, on_out, lse_out, qz_scr, acc_scr, m_scr, l_scr):
    i = pl.program_id(1)
    q_blk = q_ref[...]
    zero = jnp.zeros((64, BLK), BF16)
    qz_scr[0] = jnp.concatenate([q_blk[0:64], zero], axis=0)
    qz_scr[1] = jnp.concatenate([zero, q_blk[64:128]], axis=0)
    acc_scr[...] = jnp.zeros_like(acc_scr)
    m_scr[...] = jnp.full_like(m_scr, MASK_VALUE)
    l_scr[...] = jnp.zeros_like(l_scr)

    def step(j, masked):
        off = pl.multiple_of(j * BLK, BLK)
        k_blk = k_ref[pl.ds(off, BLK), :]
        scores = [dot_nn(k_blk, qz_scr[h]) * LOG2E for h in range(2)]
        for h in range(2):
            s = scores[h]
            if masked:
                krow = lax.broadcasted_iota(jnp.int32, s.shape, 0)
                qcol = lax.broadcasted_iota(jnp.int32, s.shape, 1)
                s = jnp.where(krow <= qcol, s, MASK_VALUE)
            m_old = m_scr[h:h + 1, :]
            m_new = jnp.maximum(m_old, jnp.max(s, axis=0, keepdims=True))
            m_scr[h:h + 1, :] = m_new
            alpha = jnp.exp2(m_old - m_new)
            p = jnp.exp2(s - m_new)
            l_scr[h:h + 1, :] = l_scr[h:h + 1, :] * alpha + jnp.sum(p, axis=0, keepdims=True)
            pv = dot_nn(v_ref[64 * h:64 * h + 64, pl.ds(off, BLK)], p.astype(BF16))
            acc_scr[h] = acc_scr[h] * alpha + pv

    def body(j, carry):
        step(j, False)
        return carry

    lax.fori_loop(0, i, body, 0)
    step(i, True)
    outs = []
    for h in range(2):
        l = l_scr[h:h + 1, :]
        outs.append((acc_scr[h] / l).astype(BF16))
        lse_out[h:h + 1, :] = m_scr[h:h + 1, :] * (1.0 / LOG2E) + jnp.log(l)
    o_blk = jnp.concatenate(outs, axis=0)
    o_out[...] = o_blk
    on_out[...] = o_blk.T


def fwd_call(q_t, k_n, v_t):
    width, seq = q_t.shape
    pairs = width // 128
    nblk = seq // BLK
    return pl.pallas_call(
        fwd_kernel,
        out_shape=(jax.ShapeDtypeStruct((width, seq), BF16), jax.ShapeDtypeStruct((seq, width), BF16), jax.ShapeDtypeStruct((8 * pairs, seq), F32)),
        grid=(pairs, nblk),
        in_specs=[
            pl.BlockSpec((128, BLK), lambda p, i: (p, i)),
            pl.BlockSpec((seq, 128), lambda p, i: (0, p)),
            pl.BlockSpec((128, seq), lambda p, i: (p, 0)),
        ],
        out_specs=(
            pl.BlockSpec((128, BLK), lambda p, i: (p, i)),
            pl.BlockSpec((BLK, 128), lambda p, i: (i, p)),
            pl.BlockSpec((8, BLK), lambda p, i: (p, i)),
        ),
        scratch_shapes=[pltpu.VMEM((2, 128, BLK), BF16), pltpu.VMEM((2, 64, BLK), F32), pltpu.VMEM((8, BLK), F32), pltpu.VMEM((8, BLK), F32)],
        compiler_params=params(2),
        cost_estimate=cost(2 * 2 * seq * seq * width * 2, seq * width * 10, seq * seq),
        name="attn_fwd",
    )(q_t, k_n, v_t)


def y_kernel(o_ref, w_ref, x_ref, y_out, acc_scr):
    s = pl.program_id(0)
    part = dot_nn(o_ref[0], w_ref[...])

    @pl.when(s == 0)
    def _():
        acc_scr[...] = part

    @pl.when(s > 0)
    def _():
        acc_scr[...] += part

    @pl.when(s == pl.num_programs(0) - 1)
    def _():
        y_out[...] = (x_ref[...].astype(F32) + acc_scr[...]).astype(BF16)


def y_call(o_parts, w_out, x):
    ndev, piece, width = o_parts.shape
    hidden = w_out.shape[1]
    return pl.pallas_call(
        y_kernel,
        out_shape=jax.ShapeDtypeStruct((piece, hidden), BF16),
        grid=(ndev,),
        in_specs=[
            pl.BlockSpec((1, piece, width), lambda s: (s, 0, 0)),
            pl.BlockSpec((width, hidden), lambda s: (s, 0)),
            pl.BlockSpec((piece, hidden), lambda s: (0, 0)),
        ],
        out_specs=pl.BlockSpec((piece, hidden), lambda s: (0, 0)),
        scratch_shapes=[pltpu.VMEM((piece, hidden), F32)],
        compiler_params=params(1),
        cost_estimate=cost(2 * piece * hidden * ndev * width, 20e6),
        name="y_proj",
    )(o_parts, w_out, x)


def do_kernel(d_ref, dy_ref, w_ref, o_ref, do_out, gw_out):
    dy = dy_ref[...]
    do_out[...] = dot_nt(w_ref[...], dy).astype(BF16)
    part = dot_nn(o_ref[...], dy)

    @pl.when(pl.program_id(0) == 0)
    def _():
        gw_out[...] = part

    @pl.when(pl.program_id(0) > 0)
    def _():
        gw_out[...] += part


def do_call(dev, dy_all, w_out, o_t):
    seq, hidden = dy_all.shape
    width = o_t.shape[0]
    return pl.pallas_call(
        do_kernel,
        out_shape=(jax.ShapeDtypeStruct((width, seq), BF16), jax.ShapeDtypeStruct((width, hidden), F32)),
        grid_spec=pltpu.PrefetchScalarGridSpec(
            num_scalar_prefetch=1,
            grid=(seq // BLK,),
            in_specs=[
                pl.BlockSpec((BLK, hidden), lambda i, d: (i, 0)),
                pl.BlockSpec((width, hidden), lambda i, d: (d[0], 0)),
                pl.BlockSpec((width, BLK), lambda i, d: (0, i)),
            ],
            out_specs=(pl.BlockSpec((width, BLK), lambda i, d: (0, i)), pl.BlockSpec((width, hidden), lambda i, d: (0, 0))),
        ),
        compiler_params=params(1),
        cost_estimate=cost(4 * seq * hidden * width, seq * hidden * 2),
        name="do_gwout",
    )(dev, dy_all, w_out, o_t)


def split3(value):
    hi = value.astype(BF16).astype(F32)
    mid = (value - hi).astype(BF16).astype(F32)
    return hi, mid, value - hi - mid


def bwd_kernel(q_ref, do_ref, o_ref, lse_ref, k_ref, v_ref, cos_ref, sin_ref, dq_out, dk_out, dv_out, dn_out, qa_scr, doa_scr, ka_scr, va_scr, dq_scr, dk_scr, dv_scr):
    j = pl.program_id(0)
    nblk = pl.num_programs(0)
    row64 = lax.broadcasted_iota(jnp.int32, (64, BLK), 0)

    def augment(data, stat):
        hi, mid, lo = split3(-stat)
        extra = jnp.where(row64 == 0, hi, jnp.where(row64 == 1, mid, jnp.where(row64 == 2, lo, 0.0))).astype(BF16)
        return jnp.concatenate([data, extra], axis=0).T

    @pl.when(j == 0)
    def _():
        dq_scr[...] = jnp.zeros_like(dq_scr)

        def prep(t, carry):
            cols = pl.ds(pl.multiple_of(t * BLK, BLK), BLK)
            for h in range(2):
                rows = slice(64 * h, 64 * h + 64)
                do_h = do_ref[rows, cols]
                delta = jnp.sum(do_h.astype(F32) * o_ref[rows, cols].astype(F32), axis=0, keepdims=True)
                qa_scr[h, cols, :] = augment(q_ref[rows, cols], lse_ref[h:h + 1, cols])
                doa_scr[h, cols, :] = augment(do_h, delta)
            return carry

        lax.fori_loop(0, nblk, prep, 0)

    ones = jnp.where(row64 < 3, 1.0, 0.0).astype(BF16)
    for h in range(2):
        rows = slice(64 * h, 64 * h + 64)
        ka_scr[h] = jnp.concatenate([k_ref[rows, :], ones], axis=0)
        va_scr[h] = jnp.concatenate([v_ref[rows, :], ones], axis=0)
    dk_scr[...] = jnp.zeros_like(dk_scr)
    dv_scr[...] = jnp.zeros_like(dv_scr)

    def step(i, masked):
        cols = pl.ds(pl.multiple_of(i * BLK, BLK), BLK)
        for h in range(2):
            rows = slice(64 * h, 64 * h + 64)
            s = dot_nn(qa_scr[h, cols, :], ka_scr[h])
            if masked:
                qrow = lax.broadcasted_iota(jnp.int32, s.shape, 0)
                kcol = lax.broadcasted_iota(jnp.int32, s.shape, 1)
                s = jnp.where(kcol <= qrow, s, MASK_VALUE)
            p = jnp.exp2(s * LOG2E)
            dp = dot_nn(doa_scr[h, cols, :], va_scr[h])
            ds = (p * dp).astype(BF16)
            dv_scr[h] += dot_nn(do_ref[rows, cols], p.astype(BF16))
            dk_scr[h] += dot_nn(q_ref[rows, cols], ds)
            dq_scr[rows, cols] += dot_nt(k_ref[rows, :], ds)

    def body(i, carry):
        step(i, False)
        return carry

    step(j, True)
    lax.fori_loop(j + 1, nblk, body, 0)

    cos = cos_ref[...]
    sin = sin_ref[...]

    def unrope(t, scale):
        t1 = t[0:32] * scale
        t2 = t[32:64] * scale
        return jnp.concatenate([t1 * cos + t2 * sin, t2 * cos - t1 * sin], axis=0).astype(BF16)

    own = pl.ds(pl.multiple_of(j * BLK, BLK), BLK)
    dq = jnp.concatenate([unrope(dq_scr[64 * h:64 * h + 64, own], 0.125) for h in range(2)], axis=0)
    dk = jnp.concatenate([unrope(dk_scr[h], 1.0) for h in range(2)], axis=0)
    dv = jnp.concatenate([dv_scr[h].astype(BF16) for h in range(2)], axis=0)
    dq_out[...] = dq
    dk_out[...] = dk
    dv_out[...] = dv
    dn_out[:, 0:128] = dq.T
    dn_out[:, 128:256] = dk.T
    dn_out[:, 256:384] = dv.T


def bwd_call(p, q_t, do_t, o_t, lse, k_t, v_t, cos_t, sin_t):
    seq = q_t.shape[1]
    half = cos_t.shape[0]
    full = pl.BlockSpec((128, seq), lambda j: (p, 0))
    blk = pl.BlockSpec((128, BLK), lambda j: (p, j))
    tab = pl.BlockSpec((half, BLK), lambda j: (0, j))
    tr = jax.ShapeDtypeStruct((128, seq), BF16)
    trs = pl.BlockSpec((128, BLK), lambda j: (0, j))
    return pl.pallas_call(
        bwd_kernel,
        out_shape=(tr, tr, tr, jax.ShapeDtypeStruct((seq, 384), BF16)),
        grid=(seq // BLK,),
        in_specs=[full, full, full, pl.BlockSpec((8, seq), lambda j: (p, 0)), blk, blk, tab, tab],
        out_specs=(trs, trs, trs, pl.BlockSpec((BLK, 384), lambda j: (j, 0))),
        scratch_shapes=[
            pltpu.VMEM((2, seq, 128), BF16), pltpu.VMEM((2, seq, 128), BF16),
            pltpu.VMEM((2, 128, BLK), BF16), pltpu.VMEM((2, 128, BLK), BF16),
            pltpu.VMEM((128, seq), F32), pltpu.VMEM((2, 64, BLK), F32), pltpu.VMEM((2, 64, BLK), F32),
        ],
        compiler_params=params(1),
        cost_estimate=cost(5 * seq * seq * 128 * 2, seq * 128 * 20, seq * seq),
        name=f"attn_bwd{p}",
    )(q_t, do_t, o_t, lse, k_t, v_t, cos_t, sin_t)


def gw_kernel(dq_ref, dk_ref, dv_ref, r_ref, gw_out, acc_scr):
    i = pl.program_id(0)
    lhs = jnp.concatenate([dq_ref[...], dk_ref[...], dv_ref[...]], axis=0)
    part = dot_nn(lhs, r_ref[...])

    @pl.when(i == 0)
    def _():
        acc_scr[...] = part

    @pl.when(i > 0)
    def _():
        acc_scr[...] += part

    @pl.when(i == pl.num_programs(0) - 1)
    def _():
        gw_out[...] = acc_scr[...].T


def gw_call(dq, dk, dv, r_all):
    seq, hidden = r_all.shape
    spec = pl.BlockSpec((128, BLK), lambda i: (0, i))
    return pl.pallas_call(
        gw_kernel,
        out_shape=jax.ShapeDtypeStruct((hidden, 384), F32),
        grid=(seq // BLK,),
        in_specs=[spec, spec, spec, pl.BlockSpec((BLK, hidden), lambda i: (i, 0))],
        out_specs=pl.BlockSpec((hidden, 384), lambda i: (0, 0)),
        scratch_shapes=[pltpu.VMEM((384, hidden), F32)],
        compiler_params=params(1),
        cost_estimate=cost(2 * seq * hidden * 384, seq * hidden * 2),
        name="gwqkv",
    )(dq, dk, dv, r_all)


def place_kernel(a_ref, b_ref, out):
    out[:, 0:128] = a_ref[0]
    out[:, 128:256] = b_ref[0]


def place_call(gw0, gw1):
    ndev, hidden, _ = gw0.shape
    spec = pl.BlockSpec((1, hidden, 128), lambda w, d: (d, 0, w))
    return pl.pallas_call(
        place_kernel,
        out_shape=jax.ShapeDtypeStruct((hidden, 3 * ndev * 256), F32),
        grid=(3, ndev),
        in_specs=[spec, spec],
        out_specs=pl.BlockSpec((hidden, 256), lambda w, d: (0, w * ndev + d)),
        compiler_params=params(2),
        name="place",
    )(gw0, gw1)


def dx_kernel(a_ref, b_ref, wq_ref, wk_ref, wv_ref, x_ref, inv_ref, g_ref, dy_ref, dx_out, gg_out, acc_scr):
    s = pl.program_id(0)
    a = a_ref[0]
    b = b_ref[0]
    part = None
    for which, w in enumerate((wq_ref, wk_ref, wv_ref)):
        cols = slice(128 * which, 128 * which + 128)
        lhs = jnp.concatenate([a[:, cols], b[:, cols]], axis=1)
        term = dot_nt(lhs, w[...])
        part = term if part is None else part + term

    @pl.when(s == 0)
    def _():
        acc_scr[...] = part

    @pl.when(s > 0)
    def _():
        acc_scr[...] += part

    @pl.when(s == pl.num_programs(0) - 1)
    def _():
        dn = acc_scr[...]
        inv = inv_ref[...]
        x_hat = x_ref[...].astype(F32) * inv
        gg_out[...] = jnp.sum(dn * x_hat, axis=0, keepdims=True)
        d_hat = dn * g_ref[...]
        mean = jnp.mean(d_hat * x_hat, axis=-1, keepdims=True)
        dx_out[...] = (dy_ref[...].astype(F32) + inv * (d_hat - x_hat * mean)).astype(BF16)


def dx_call(d0, d1, w_qkv, x, inv_rms, gain, dy):
    ndev, piece, _ = d0.shape
    hidden = w_qkv.shape[0]
    dspec = pl.BlockSpec((1, piece, 384), lambda s: (s, 0, 0))
    wspec = lambda which: pl.BlockSpec((hidden, 256), lambda s: (0, which * ndev + s))
    whole = lambda *shape: pl.BlockSpec(shape, lambda s: (0, 0))
    return pl.pallas_call(
        dx_kernel,
        out_shape=(jax.ShapeDtypeStruct((piece, hidden), BF16), jax.ShapeDtypeStruct((1, hidden), F32)),
        grid=(ndev,),
        in_specs=[dspec, dspec, wspec(0), wspec(1), wspec(2), whole(piece, hidden), whole(piece, 1), whole(1, hidden), whole(piece, hidden)],
        out_specs=(whole(piece, hidden), whole(1, hidden)),
        scratch_shapes=[pltpu.VMEM((piece, hidden), F32)],
        compiler_params=params(1),
        cost_estimate=cost(2 * piece * hidden * 3 * ndev * 256, 40e6),
        name="dx",
    )(d0, d1, w_qkv, w_qkv, w_qkv, x, inv_rms, gain, dy)


def solution(mesh):
    ndev = mesh.shape['cp']

    def device_fn(x_in, positions, long_factor, norm_gain, w_qkv, w_out, grad_y):
        _, piece, hidden = x_in.shape
        seq = piece * ndev
        dev = lax.axis_index('cp').astype(jnp.int32).reshape(1)
        x = x_in[0]
        dy = grad_y[0]
        x_float = x.astype(F32)
        inv_rms = lax.rsqrt(jnp.mean(x_float * x_float, axis=-1, keepdims=True) + NORM_EPS)
        normed = (x_float * inv_rms * norm_gain).astype(BF16)
        r_all = lax.all_gather(normed, 'cp', axis=0, tiled=True)
        dy_all = lax.all_gather(dy, 'cp', axis=0, tiled=True)

        pos_all = lax.all_gather(positions, 'cp', axis=0, tiled=True)
        half = long_factor.shape[0]
        exponent = jnp.arange(half, dtype=F32) * (1.0 / half)
        inv_freq = 1.0 / (long_factor * jnp.power(10000.0, exponent))
        angles = inv_freq[:, None] * pos_all.astype(F32)[None, :]
        cos_t = jnp.cos(angles) * MSCALE
        sin_t = jnp.sin(angles) * MSCALE

        q_t, k_t, v_t, k_n = qkv_call(dev, r_all, w_qkv, cos_t, sin_t)
        o_t, o_n, lse = fwd_call(q_t, k_n, v_t)
        o_parts = lax.all_to_all(o_n.reshape(ndev, piece, 256), 'cp', 0, 0)
        y_out = y_call(o_parts, w_out, x)
        do_t, gw_own = do_call(dev, dy_all, w_out, o_t)
        g_wout = lax.all_gather(gw_own, 'cp', axis=0, tiled=True)

        gws, dns = [], []
        for p in range(2):
            dq, dk, dv, dn = bwd_call(p, q_t, do_t, o_t, lse, k_t, v_t, cos_t, sin_t)
            dns.append(lax.all_to_all(dn.reshape(ndev, piece, 384), 'cp', 0, 0))
            gws.append(lax.all_gather(gw_call(dq, dk, dv, r_all), 'cp'))
        grad_x, gg = dx_call(dns[0], dns[1], w_qkv, x, inv_rms, norm_gain.reshape(1, hidden), dy)
        g_gain = lax.psum(gg.reshape(hidden), 'cp')
        g_wqkv = place_call(gws[0], gws[1])
        return y_out[None], grad_x[None], g_gain, g_wqkv, g_wout

    seq_spec = P('dp', 'cp', None)
    return jax.shard_map(device_fn, mesh=mesh, in_specs=(seq_spec, P(('dp', 'cp')), P(None), P(None), P(None, None), P(None, None), seq_spec), out_specs=(seq_spec, seq_spec, P('dp'), P('dp', None), P('dp', None)), check_vma=False)
```

```python
import math
import jax
import jax.numpy as jnp
from jax import lax
from jax.experimental import pallas as pl
from jax.experimental.pallas import tpu as pltpu
from jax.sharding import PartitionSpec as P

NORM_EPS = 1e-5
MSCALE = math.sqrt(1.0 + math.log(32.0) / math.log(4096.0))
MASK_VALUE = -1e30
LOG2E = math.log2(math.e)
BF16 = jnp.bfloat16
F32 = jnp.float32
BLK = 512
VMEM_LIMIT = 60 * 1024 * 1024


def dot_nn(a, b):
    return lax.dot_general(a, b, (((1,), (0,)), ((), ())), preferred_element_type=F32)


def dot_nt(a, b):
    return lax.dot_general(a, b, (((1,), (1,)), ((), ())), preferred_element_type=F32)


def params(n=1, **kw):
    return pltpu.CompilerParams(dimension_semantics=("arbitrary",) * n, vmem_limit_bytes=VMEM_LIMIT, **kw)


def cost(flops, nbytes, trans=0):
    return pl.CostEstimate(flops=int(flops), bytes_accessed=int(nbytes), transcendentals=int(trans))


MESH = pl.DeviceIdType.MESH


class Grid:
    def __init__(self):
        self.me = lax.axis_index('cp')
        self.core = self.me % 2
        self.x = (self.me // 2) % 2
        self.y = self.me // 4

    def flip(self, yf, xf, cf):
        return ((self.y + yf) % 2) * 4 + ((self.x + xf) % 2) * 2 + (self.core + cf) % 2

    def xor(self, mask):
        return self.flip(mask // 4, (mask // 2) % 2, mask % 2)


def barrier(grid, masks):
    sem = pltpu.get_barrier_semaphore()
    for mask in masks:
        pl.semaphore_signal(sem, inc=1, device_id={'cp': grid.xor(mask)}, device_id_type=MESH)
    pl.semaphore_wait(sem, len(masks))


class Gather:
    SENDS = {
        'xA': (0, 0, 1, 2), 'yB': (0, 1, 1, 4), 'xB': (0, 1, 1, 2), 'yA': (0, 0, 1, 4), 'own': (0, 0, 2, 1),
        'dA': (2, 0, 1, 4), 'dB': (4, 1, 1, 2),
        'cxA': (2, 0, 1, 1), 'cyB': (4, 1, 1, 1), 'cxB': (2, 1, 1, 1), 'cyA': (4, 0, 1, 1), 'cdA': (6, 0, 1, 1), 'cdB': (6, 1, 1, 1),
    }
    ORDER = tuple(SENDS)

    def __init__(self, grid, src, dst, ssem, rsem):
        self.grid, self.src, self.dst, self.ssem, self.rsem = grid, src, dst, ssem, rsem

    def desc(self, name, arriving=False):
        mask, first, halves, target = self.SENDS[name]
        k = self.ORDER.index(name)
        dst = self.dst(self.grid.xor(mask ^ target if arriving else mask), first, halves)
        src = dst if (mask or arriving or self.src is None) else self.src(first, halves)
        return pltpu.make_async_remote_copy(src, dst, self.ssem(k), self.rsem(k), device_id={'cp': self.grid.xor(target)}, device_id_type=MESH)

    def send(self, *names):
        for name in names:
            self.desc(name).start()

    def arrived(self, *names):
        for name in names:
            self.desc(name, True).wait_recv()

    def begin(self):
        self.send('xA', 'yB', 'xB', 'yA', 'own')

    def first(self):
        self.arrived('xA', 'yB')
        self.send('dA', 'dB', 'cxA', 'cyB')

    def second(self):
        self.arrived('xB', 'yA')
        self.send('cxB', 'cyA')

    def third(self):
        self.arrived('dA', 'dB')
        self.send('cdA', 'cdB')

    def last(self):
        self.arrived('own', 'cxA', 'cyB', 'cxB', 'cyA', 'cdA', 'cdB')
        self.sent()

    def sent(self):
        for name in self.ORDER:
            self.desc(name).wait_send()


def row_gather(grid, src, dst, piece, ssem, rsem):
    half = piece // 2

    def place(owner, first, halves):
        return dst.at[pl.ds(pl.multiple_of(owner * piece + first * half, half), halves * half)]

    own = None if src is None else lambda first, halves: src.at[pl.ds(first * half, halves * half)]
    return Gather(grid, own, place, lambda k: ssem.at[k], lambda k: rsem.at[k])


GATHER_SEMS = [pltpu.SemaphoreType.DMA((13,)), pltpu.SemaphoreType.DMA((13,))]


def qkv_kernel(r_own, pos_ref, inv_ref, w_hbm, r_all, q_hbm, k_hbm, v_hbm, kn_hbm, cos_hbm, sin_hbm,
               wtmp, w_scr, rbuf, pos_scr, q_st, k_st, v_st, kn_st, cos_st, sin_st, wsem, lsem, osem, csem, pssem, prsem, ssem, rsem):
    grid = Grid()
    piece, hidden = r_own.shape
    hp = piece // 2
    width = wtmp.shape[2]
    ndev = r_all.shape[0] // piece

    def w_copy(which):
        cols = pl.ds(pl.multiple_of(which * ndev * width + grid.me * width, width), width)
        return pltpu.make_async_copy(w_hbm.at[:, cols], wtmp.at[which], wsem.at[which])

    for which in range(3):
        w_copy(which).start()
    barrier(grid, range(1, 8))
    gather = row_gather(grid, r_own, r_all, piece, ssem, rsem)
    gather.begin()

    def pos_copy(mask, owner):
        return pltpu.make_async_remote_copy(pos_ref, pos_scr.at[pl.ds(2 * owner, 2)], pssem.at[mask], prsem.at[mask], device_id={'cp': grid.xor(mask)}, device_id_type=MESH)

    for mask in range(1, 8):
        pos_copy(mask, grid.me).start()
    pos_scr[pl.ds(2 * grid.me, 2)] = pos_ref[...]
    for which in range(3):
        w_copy(which).wait()
        w_scr[width * which:width * (which + 1)] = wtmp[which].T
    for mask in range(1, 8):
        pos_copy(mask, grid.xor(mask)).wait_recv()

    inv = inv_ref[...]
    nh = width // 64

    def group(g, carry):
        stage = g // 2
        one = (stage + 2) // 3
        two = stage // 3
        flips = ((two, one), (one, two))
        half0 = (stage // 2) * (1 - two)
        halves = (half0, 1 - half0)
        owners = [grid.flip(yf, xf, g % 2) for yf, xf in flips]
        offs = [pl.multiple_of(owners[u] * piece + halves[u] * hp, 128) for u in range(2)]

        def load(u):
            return pltpu.make_async_copy(r_all.at[pl.ds(offs[u], hp)], rbuf.at[u], lsem.at[u])

        def keep(u):
            return pltpu.make_async_copy(rbuf.at[u], r_all.at[pl.ds(offs[u], hp)], csem.at[u])

        @pl.when(g == 0)
        def _():
            for u in range(2):
                pltpu.make_async_copy(r_own.at[pl.ds(u * hp, hp)], rbuf.at[u], lsem.at[u]).start()

        @pl.when(g == 1)
        def _():
            gather.arrived('own')

        @pl.when(g == 2)
        def _():
            gather.first()

        @pl.when(g == 3)
        def _():
            gather.arrived('cxA', 'cyB')

        @pl.when(g == 4)
        def _():
            gather.second()

        @pl.when(g == 5)
        def _():
            gather.arrived('cxB', 'cyA')

        @pl.when(g == 6)
        def _():
            gather.third()

        @pl.when(g == 7)
        def _():
            gather.arrived('cdA', 'cdB')

        @pl.when(g > 0)
        def _():
            for u in range(2):
                load(u).start()

        outs = []
        for u in range(2):
            load(u).wait()

            @pl.when(g == 0)
            def _():
                keep(u).start()

            angles = inv * pos_scr[2 * owners[u] + halves[u]].astype(F32)
            cos = jnp.cos(angles) * MSCALE
            sin = jnp.sin(angles) * MSCALE
            cos_st[u] = cos
            sin_st[u] = sin
            r_blk = rbuf[u]

            def rope(t):
                rows = []
                for h in range(nh):
                    t1 = t[64 * h:64 * h + 32]
                    t2 = t[64 * h + 32:64 * h + 64]
                    rows += [t1 * cos - t2 * sin, t2 * cos + t1 * sin]
                return jnp.concatenate(rows, axis=0).astype(BF16)

            q_st[u] = rope(dot_nt(w_scr[0:width], r_blk)) * BF16(0.125)
            k_rot = rope(dot_nt(w_scr[width:2 * width], r_blk))
            k_st[u] = k_rot
            kn_st[u] = k_rot.T
            v_st[u] = dot_nt(w_scr[2 * width:], r_blk).astype(BF16)
            for n, (st, hbm) in enumerate(((q_st, q_hbm), (k_st, k_hbm), (v_st, v_hbm), (cos_st, cos_hbm), (sin_st, sin_hbm))):
                outs.append(pltpu.make_async_copy(st.at[u], hbm.at[:, pl.ds(offs[u], hp)], osem.at[u, n]))
            outs.append(pltpu.make_async_copy(kn_st.at[u], kn_hbm.at[pl.ds(offs[u], hp)], osem.at[u, 5]))
            for copy in outs[6 * u:]:
                copy.start()
        for copy in outs:
            copy.wait()

        @pl.when(g == 0)
        def _():
            for u in range(2):
                keep(u).wait()

        return carry

    lax.fori_loop(0, 8, group, 0)
    gather.sent()
    for mask in range(1, 8):
        pos_copy(mask, grid.me).wait_send()


def qkv_call(r_own, pos, inv_freq, w_qkv):
    piece, hidden = r_own.shape
    ndev = 8
    seq = piece * ndev
    hp = piece // 2
    width = 256
    half = inv_freq.shape[0]
    tr = jax.ShapeDtypeStruct((width, seq), BF16)
    tab = jax.ShapeDtypeStruct((half, seq), F32)
    hbm = pl.BlockSpec(memory_space=pl.ANY)
    vmem = pl.BlockSpec(memory_space=pltpu.VMEM)
    dma = pltpu.SemaphoreType.DMA
    return pl.pallas_call(
        qkv_kernel,
        out_shape=(jax.ShapeDtypeStruct((seq, hidden), BF16), tr, tr, tr, jax.ShapeDtypeStruct((seq, width), BF16), tab, tab),
        in_specs=[hbm, vmem, vmem, hbm],
        out_specs=(hbm,) * 7,
        scratch_shapes=[
            pltpu.VMEM((3, hidden, width), BF16), pltpu.VMEM((3 * width, hidden), BF16), pltpu.VMEM((2, hp, hidden), BF16),
            pltpu.VMEM((2 * ndev, 1, hp), jnp.int32),
            pltpu.VMEM((2, width, hp), BF16), pltpu.VMEM((2, width, hp), BF16), pltpu.VMEM((2, width, hp), BF16), pltpu.VMEM((2, hp, width), BF16),
            pltpu.VMEM((2, half, hp), F32), pltpu.VMEM((2, half, hp), F32),
            dma((3,)), dma((2,)), dma((2, 6)), dma((2,)), dma((8,)), dma((8,)),
        ] + GATHER_SEMS,
        compiler_params=pltpu.CompilerParams(collective_id=0, has_side_effects=True, vmem_limit_bytes=VMEM_LIMIT),
        cost_estimate=cost(2 * seq * hidden * 3 * width, 2 * seq * hidden * 2 + seq * width * 8),
        name="gather_qkv",
    )(r_own, pos.reshape(2, 1, hp), inv_freq.reshape(half, 1), w_qkv)


FWD_FIRST, FWD_SECOND, FWD_THIRD = 8, 11, 20


def fwd_kernel(q_ref, k_ref, v_ref, dy_own, o_out, on_out, lse_out, dy_all, qz_scr, acc_scr, m_scr, l_scr, keep, ksem, ssem, rsem):
    i = pl.program_id(1)
    t = pl.program_id(0) * pl.num_programs(1) + i
    grid = Grid()
    gather = row_gather(grid, dy_own, dy_all, dy_own.shape[0], ssem, rsem)
    keep_in = pltpu.make_async_copy(dy_own, keep, ksem)
    keep_out = pltpu.make_async_copy(keep, gather.dst(grid.me, 0, 2), ksem)

    @pl.when(t == 0)
    def _():
        barrier(grid, (1, 2, 4))
        gather.begin()
        keep_in.start()

    @pl.when(t == 1)
    def _():
        keep_in.wait()
        keep_out.start()

    @pl.when(t == FWD_FIRST)
    def _():
        gather.first()
        keep_out.wait()

    @pl.when(t == FWD_SECOND)
    def _():
        gather.second()

    @pl.when(t == FWD_THIRD)
    def _():
        gather.third()

    @pl.when(t == pl.num_programs(0) * pl.num_programs(1) - 1)
    def _():
        gather.last()

    q_blk = q_ref[...]
    zero = jnp.zeros((64, BLK), BF16)
    qz_scr[0] = jnp.concatenate([q_blk[0:64], zero], axis=0)
    qz_scr[1] = jnp.concatenate([zero, q_blk[64:128]], axis=0)
    acc_scr[...] = jnp.zeros_like(acc_scr)
    m_scr[...] = jnp.full_like(m_scr, MASK_VALUE)
    l_scr[...] = jnp.zeros_like(l_scr)

    def step(j, masked):
        off = pl.multiple_of(j * BLK, BLK)
        k_blk = k_ref[pl.ds(off, BLK), :]
        scores = [dot_nn(k_blk, qz_scr[h]) * LOG2E for h in range(2)]
        for h in range(2):
            s = scores[h]
            if masked:
                krow = lax.broadcasted_iota(jnp.int32, s.shape, 0)
                qcol = lax.broadcasted_iota(jnp.int32, s.shape, 1)
                s = jnp.where(krow <= qcol, s, MASK_VALUE)
            m_old = m_scr[h:h + 1, :]
            m_new = jnp.maximum(m_old, jnp.max(s, axis=0, keepdims=True))
            m_scr[h:h + 1, :] = m_new
            alpha = jnp.exp2(m_old - m_new)
            p = jnp.exp2(s - m_new)
            l_scr[h:h + 1, :] = l_scr[h:h + 1, :] * alpha + jnp.sum(p, axis=0, keepdims=True)
            pv = dot_nn(v_ref[64 * h:64 * h + 64, pl.ds(off, BLK)], p.astype(BF16))
            acc_scr[h] = acc_scr[h] * alpha + pv

    def body(j, carry):
        step(j, False)
        return carry

    lax.fori_loop(0, i, body, 0)
    step(i, True)
    outs = []
    for h in range(2):
        l = l_scr[h:h + 1, :]
        outs.append((acc_scr[h] / l).astype(BF16))
        lse_out[h:h + 1, :] = m_scr[h:h + 1, :] * (1.0 / LOG2E) + jnp.log(l)
    o_blk = jnp.concatenate(outs, axis=0)
    o_out[...] = o_blk
    on_out[...] = o_blk.T


def fwd_call(q_t, k_n, v_t, dy):
    width, seq = q_t.shape
    piece, hidden = dy.shape
    pairs = width // 128
    nblk = seq // BLK
    return pl.pallas_call(
        fwd_kernel,
        out_shape=(jax.ShapeDtypeStruct((width, seq), BF16), jax.ShapeDtypeStruct((seq, width), BF16), jax.ShapeDtypeStruct((8 * pairs, seq), F32), jax.ShapeDtypeStruct((seq, hidden), BF16)),
        grid=(pairs, nblk),
        in_specs=[
            pl.BlockSpec((128, BLK), lambda p, i: (p, i)),
            pl.BlockSpec((seq, 128), lambda p, i: (0, p)),
            pl.BlockSpec((128, seq), lambda p, i: (p, 0)),
            pl.BlockSpec(memory_space=pl.ANY),
        ],
        out_specs=(
            pl.BlockSpec((128, BLK), lambda p, i: (p, i)),
            pl.BlockSpec((BLK, 128), lambda p, i: (i, p)),
            pl.BlockSpec((8, BLK), lambda p, i: (p, i)),
            pl.BlockSpec(memory_space=pl.ANY),
        ),
        scratch_shapes=[
            pltpu.VMEM((2, 128, BLK), BF16), pltpu.VMEM((2, 64, BLK), F32), pltpu.VMEM((8, BLK), F32), pltpu.VMEM((8, BLK), F32),
            pltpu.VMEM((piece, hidden), BF16), pltpu.SemaphoreType.DMA,
        ] + GATHER_SEMS,
        compiler_params=params(2, collective_id=1, has_side_effects=True),
        cost_estimate=cost(2 * 2 * seq * seq * width * 2, seq * width * 10, seq * seq),
        name="attn_fwd",
    )(q_t, k_n, v_t, dy)


def y_kernel(d_ref, o_ref, own_ref, w_ref, x_ref, y_out, acc_scr):
    s = pl.program_id(0)
    part = dot_nn(jnp.where(s == d_ref[0], own_ref[...], o_ref[0]), w_ref[...])

    @pl.when(s == 0)
    def _():
        acc_scr[...] = part

    @pl.when(s > 0)
    def _():
        acc_scr[...] += part

    @pl.when(s == pl.num_programs(0) - 1)
    def _():
        y_out[...] = (x_ref[...].astype(F32) + acc_scr[...]).astype(BF16)


def y_call(dev, o_parts, o_n, w_out, x):
    ndev, piece, width = o_parts.shape
    hidden = w_out.shape[1]
    return pl.pallas_call(
        y_kernel,
        out_shape=jax.ShapeDtypeStruct((piece, hidden), BF16),
        grid_spec=pltpu.PrefetchScalarGridSpec(
            num_scalar_prefetch=1,
            grid=(ndev,),
            in_specs=[
                pl.BlockSpec((1, piece, width), lambda s, d: (s, 0, 0)),
                pl.BlockSpec((piece, width), lambda s, d: (d[0], 0)),
                pl.BlockSpec((width, hidden), lambda s, d: (s, 0)),
                pl.BlockSpec((piece, hidden), lambda s, d: (0, 0)),
            ],
            out_specs=pl.BlockSpec((piece, hidden), lambda s, d: (0, 0)),
            scratch_shapes=[pltpu.VMEM((piece, hidden), F32)],
        ),
        compiler_params=params(1),
        cost_estimate=cost(2 * piece * hidden * ndev * width, 20e6),
        name="y_proj",
    )(dev, o_parts, o_n, w_out, x)


def split3(value):
    hi = value.astype(BF16).astype(F32)
    mid = (value - hi).astype(BF16).astype(F32)
    return hi, mid, value - hi - mid


HEADS = 4
HD = 64
FIRST, SECOND, THIRD = 6, 9, 2


def bwd_kernel(dy_ref, r_ref, q_ref, o_ref, k_ref, v_ref, lse_ref, cos_ref, sin_ref, w_hbm, on_hbm,
               o_recv, gwo_all, dn_recv, gw_all,
               do_scr, w_scr, gwo_scr, qa_scr, doa_scr, ka_scr, va_scr, dq_scr, dk_scr, dv_scr, dn_scr, gw_scr,
               wsem, lsem, o_ssem, o_rsem, d_ssem, d_rsem, g_ssem, g_rsem):
    s = pl.program_id(0)
    nblk = do_scr.shape[1] // BLK
    grid = Grid()
    width, hidden = w_scr.shape
    piece = on_hbm.shape[0] // 8
    masks = range(1, 8)
    row64 = lax.broadcasted_iota(jnp.int32, (HD, BLK), 0)

    def blk(t):
        return pl.ds(pl.multiple_of(t * BLK, BLK), BLK)

    def o_copy(mask, owner):
        src = on_hbm.at[pl.ds(pl.multiple_of(grid.xor(mask) * piece, piece), piece)]
        return pltpu.make_async_remote_copy(src, o_recv.at[owner], o_ssem.at[mask], o_rsem.at[mask], device_id={'cp': grid.xor(mask)}, device_id_type=MESH)

    def dn_cols(owner):
        return pl.ds(pl.multiple_of(owner * piece, 128), piece)

    def dn_copy(h, mask, owner):
        src = dn_scr.at[h % 2, :, dn_cols(grid.xor(mask))]
        return pltpu.make_async_remote_copy(src, dn_recv.at[h, owner], d_ssem.at[h, mask], d_rsem.at[h, mask], device_id={'cp': grid.xor(mask)}, device_id_type=MESH)

    def dn_own(h):
        return pltpu.make_async_copy(dn_scr.at[h % 2, :, dn_cols(grid.me)], dn_recv.at[h, grid.me], lsem.at[0])

    def gw_own(h):
        return pltpu.make_async_copy(gw_scr.at[h % 2], gw_all.at[grid.me, h], lsem.at[1])

    def gw_gather(h):
        half = 3 * HD // 2
        return Gather(grid, None, lambda owner, first, halves: gw_all.at[owner, h, pl.ds(first * half, halves * half)], lambda k: g_ssem.at[h, k], lambda k: g_rsem.at[h, k])

    gwo_gather = row_gather(grid, None, gwo_all, width, g_ssem.at[HEADS], g_rsem.at[HEADS])

    @pl.when(s == 0)
    def _():
        w_copy = pltpu.make_async_copy(w_hbm.at[pl.ds(pl.multiple_of(grid.me * width, width), width)], w_scr, wsem)
        w_copy.start()
        barrier(grid, masks)
        for mask in masks:
            o_copy(mask, grid.me).start()
        w_copy.wait()
        gwo_scr[...] = jnp.zeros_like(gwo_scr)

    @pl.when(s < nblk)
    def _():
        cols = blk(s)
        dy = dy_ref[...]
        do_scr[:, cols] = dot_nt(w_scr[...], dy).astype(BF16)
        gwo_scr[...] += dot_nn(o_ref[:, cols], dy)

    @pl.when(s == nblk)
    def _():
        own = pltpu.make_async_copy(gwo_scr, gwo_gather.dst(grid.me, 0, 2), lsem.at[1])
        own.start()
        own.wait()
        gwo_gather.begin()

    t = s - nblk
    h = t // nblk
    j = t % nblk

    def send_head(h):
        dn_own(h).start()
        for mask in masks:
            dn_copy(h, mask, grid.me).start()
        gw_own(h).start()

    def begin_gw(h):
        gw_own(h).wait()
        dn_own(h).wait()
        gw_gather(h).begin()

    @pl.when((t >= 2 * nblk) & (j == 0))
    def _():
        for mask in masks:
            dn_copy(h - 2, mask, grid.me).wait_send()

    @pl.when((t >= nblk) & (j == 0))
    def _():
        send_head(h - 1)

    @pl.when((t >= nblk) & (j == 1))
    def _():
        begin_gw(h - 1)

    @pl.when((t >= nblk) & (j == FIRST))
    def _():
        gw_gather(h - 1).first()

    @pl.when((t >= nblk) & (j == SECOND))
    def _():
        gw_gather(h - 1).second()

    @pl.when((t >= 2 * nblk) & (j == THIRD))
    def _():
        gw_gather(h - 2).third()

    @pl.when(t == 5)
    def _():
        gwo_gather.first()

    @pl.when(t == 8)
    def _():
        gwo_gather.second()

    @pl.when(t == nblk + THIRD)
    def _():
        gwo_gather.third()

    @pl.when(t >= 0)
    def _():
        rows = pl.ds(pl.multiple_of(h * HD, HD), HD)

        @pl.when(j == 0)
        def _():
            dq_scr[...] = jnp.zeros_like(dq_scr)
            gw_scr[h % 2] = jnp.zeros(gw_scr.shape[1:], F32)

            def augment(data, stat):
                hi, mid, lo = split3(-stat)
                extra = jnp.where(row64 == 0, hi, jnp.where(row64 == 1, mid, jnp.where(row64 == 2, lo, 0.0))).astype(BF16)
                return jnp.concatenate([data, extra], axis=0).T

            def prep(i, carry):
                cols = blk(i)
                do_h = do_scr[rows, cols]
                delta = jnp.sum(do_h.astype(F32) * o_ref[rows, cols].astype(F32), axis=0, keepdims=True)
                qa_scr[cols, :] = augment(q_ref[rows, cols], lse_ref[pl.ds((h // 2) * 8 + h % 2, 1), cols])
                doa_scr[cols, :] = augment(do_h, delta)
                return carry

            lax.fori_loop(0, nblk, prep, 0)

        ones = jnp.where(row64 < 3, 1.0, 0.0).astype(BF16)
        ka_scr[...] = jnp.concatenate([k_ref[rows, :], ones], axis=0)
        va_scr[...] = jnp.concatenate([v_ref[rows, :], ones], axis=0)
        dk_scr[...] = jnp.zeros_like(dk_scr)
        dv_scr[...] = jnp.zeros_like(dv_scr)

        def step(i, masked):
            cols = blk(i)
            scores = dot_nn(qa_scr[cols, :], ka_scr[...])
            if masked:
                qrow = lax.broadcasted_iota(jnp.int32, scores.shape, 0)
                kcol = lax.broadcasted_iota(jnp.int32, scores.shape, 1)
                scores = jnp.where(kcol <= qrow, scores, MASK_VALUE)
            p = jnp.exp2(scores * LOG2E)
            dp = dot_nn(doa_scr[cols, :], va_scr[...])
            ds = (p * dp).astype(BF16)
            dv_scr[...] += dot_nn(do_scr[rows, cols], p.astype(BF16))
            dk_scr[...] += dot_nn(q_ref[rows, cols], ds)
            dq_scr[:, cols] += dot_nt(k_ref[rows, :], ds)

        def body(i, carry):
            step(i, False)
            return carry

        step(j, True)
        lax.fori_loop(j + 1, nblk, body, 0)

        cos = cos_ref[...]
        sin = sin_ref[...]

        def unrope(v, scale):
            v1 = v[0:HD // 2] * scale
            v2 = v[HD // 2:HD] * scale
            return [v1 * cos + v2 * sin, v2 * cos - v1 * sin]

        grads = jnp.concatenate(unrope(dq_scr[:, blk(j)], 0.125) + unrope(dk_scr[...], 1.0) + [dv_scr[...]], axis=0).astype(BF16)
        dn_scr[h % 2, :, blk(j)] = grads
        gw_scr[h % 2] += dot_nn(grads, r_ref[...])

    @pl.when(s == pl.num_programs(0) - 1)
    def _():
        end = HEADS - 1
        send_head(end)
        gw_gather(end - 1).third()
        begin_gw(end)
        gw_gather(end).first()
        gw_gather(end).second()
        gw_gather(end).third()
        for mask in masks:
            o_copy(mask, grid.xor(mask)).wait_recv()
            o_copy(mask, grid.me).wait_send()
            for head in range(HEADS):
                dn_copy(head, mask, grid.xor(mask)).wait_recv()
            for head in range(HEADS - 2, HEADS):
                dn_copy(head, mask, grid.me).wait_send()
        gwo_gather.last()
        for head in range(HEADS):
            gw_gather(head).last()


def bwd_call(dy_all, r_all, q_t, o_t, k_t, v_t, lse, cos_t, sin_t, w_out, o_n):
    seq, hidden = dy_all.shape
    width = q_t.shape[0]
    half = cos_t.shape[0]
    ndev = 8
    piece = seq // ndev
    nblk = seq // BLK
    hbm = pl.BlockSpec(memory_space=pl.ANY)
    whole = lambda *shape: pl.BlockSpec(shape, lambda s: (0, 0), pipeline_mode=pl.Buffered(1))
    jblk = lambda s: lax.rem(s, nblk)
    rblk = lambda s: jnp.where(s < nblk, 0, lax.rem(s, nblk))
    rows = 3 * HD
    dma = pltpu.SemaphoreType.DMA
    return pl.pallas_call(
        bwd_kernel,
        out_shape=(
            jax.ShapeDtypeStruct((ndev, piece, width), BF16),
            jax.ShapeDtypeStruct((ndev * width, hidden), F32),
            jax.ShapeDtypeStruct((HEADS, ndev, rows, piece), BF16),
            jax.ShapeDtypeStruct((ndev, HEADS, rows, hidden), F32),
        ),
        grid=(nblk * (1 + HEADS),),
        in_specs=[
            pl.BlockSpec((BLK, hidden), lambda s: (jnp.minimum(s, nblk - 1), 0)),
            pl.BlockSpec((BLK, hidden), lambda s: (rblk(s), 0)),
            whole(width, seq), whole(width, seq),
            pl.BlockSpec((width, BLK), lambda s: (0, jblk(s))),
            pl.BlockSpec((width, BLK), lambda s: (0, jblk(s))),
            whole(16, seq),
            pl.BlockSpec((half, BLK), lambda s: (0, jblk(s))),
            pl.BlockSpec((half, BLK), lambda s: (0, jblk(s))),
            hbm, hbm,
        ],
        out_specs=(hbm,) * 4,
        scratch_shapes=[
            pltpu.VMEM((width, seq), BF16), pltpu.VMEM((width, hidden), BF16), pltpu.VMEM((width, hidden), F32),
            pltpu.VMEM((seq, 2 * HD), BF16), pltpu.VMEM((seq, 2 * HD), BF16),
            pltpu.VMEM((2 * HD, BLK), BF16), pltpu.VMEM((2 * HD, BLK), BF16),
            pltpu.VMEM((HD, seq), F32), pltpu.VMEM((HD, BLK), F32), pltpu.VMEM((HD, BLK), F32),
            pltpu.VMEM((2, rows, seq), BF16), pltpu.VMEM((2, rows, hidden), F32),
            dma, dma((2,)), dma((8,)), dma((8,)), dma((HEADS, 8)), dma((HEADS, 8)), dma((HEADS + 1, 13)), dma((HEADS + 1, 13)),
        ],
        compiler_params=params(1, collective_id=2, has_side_effects=True),
        cost_estimate=cost(5 * seq * seq * width, seq * hidden * 12, seq * seq),
        name="backward",
    )(dy_all, r_all, q_t, o_t, k_t, v_t, lse, cos_t, sin_t, w_out, o_n)


def place_kernel(gw_ref, out):
    rows = jnp.concatenate([gw_ref[0, h] for h in range(HEADS)], axis=0)
    out[...] = rows.T


def place_call(gw_all):
    ndev, _, rows, hidden = gw_all.shape
    width = HEADS * HD
    return pl.pallas_call(
        place_kernel,
        out_shape=jax.ShapeDtypeStruct((hidden, 3 * ndev * width), F32),
        grid=(3, ndev),
        in_specs=[pl.BlockSpec((1, HEADS, HD, hidden), lambda w, d: (d, 0, w, 0))],
        out_specs=pl.BlockSpec((hidden, width), lambda w, d: (0, w * ndev + d)),
        compiler_params=params(2),
        cost_estimate=cost(1e6, 100e6),
        name="place",
    )(gw_all)


def dx_kernel(dn_ref, wq_ref, wk_ref, wv_ref, x_ref, inv_ref, g_ref, dy_ref, dx_out, gg_out, acc_scr):
    s = pl.program_id(0)
    part = None
    for which, w in enumerate((wq_ref, wk_ref, wv_ref)):
        rhs = jnp.concatenate([dn_ref[h, 0, HD * which:HD * (which + 1)] for h in range(HEADS)], axis=0)
        term = dot_nn(w[...], rhs)
        part = term if part is None else part + term

    @pl.when(s == 0)
    def _():
        acc_scr[...] = part

    @pl.when(s > 0)
    def _():
        acc_scr[...] += part

    @pl.when(s == pl.num_programs(0) - 1)
    def _():
        dn = acc_scr[...].T
        inv = inv_ref[...]
        x_hat = x_ref[...].astype(F32) * inv
        gg_out[...] = jnp.sum(dn * x_hat, axis=0, keepdims=True)
        d_hat = dn * g_ref[...]
        mean = jnp.mean(d_hat * x_hat, axis=-1, keepdims=True)
        dx_out[...] = (dy_ref[...].astype(F32) + inv * (d_hat - x_hat * mean)).astype(BF16)


def dx_call(dn_recv, w_qkv, x, inv_rms, gain, dy):
    _, ndev, rows, piece = dn_recv.shape
    hidden = w_qkv.shape[0]
    width = HEADS * HD
    wspec = lambda which: pl.BlockSpec((hidden, width), lambda s: (0, which * ndev + s))
    whole = lambda *shape: pl.BlockSpec(shape, lambda s: (0, 0), pipeline_mode=pl.Buffered(1))
    return pl.pallas_call(
        dx_kernel,
        out_shape=(jax.ShapeDtypeStruct((piece, hidden), BF16), jax.ShapeDtypeStruct((1, hidden), F32)),
        grid=(ndev,),
        in_specs=[pl.BlockSpec((HEADS, 1, rows, piece), lambda s: (0, s, 0, 0)), wspec(0), wspec(1), wspec(2), whole(piece, hidden), whole(piece, 1), whole(1, hidden), whole(piece, hidden)],
        out_specs=(whole(piece, hidden), whole(1, hidden)),
        scratch_shapes=[pltpu.VMEM((hidden, piece), F32)],
        compiler_params=params(1),
        cost_estimate=cost(2 * piece * hidden * 3 * ndev * width, 40e6),
        name="dx",
    )(dn_recv, w_qkv, w_qkv, w_qkv, x, inv_rms, gain, dy)


def solution(mesh):
    ndev = mesh.shape['cp']

    def device_fn(x_in, positions, long_factor, norm_gain, w_qkv, w_out, grad_y):
        _, piece, hidden = x_in.shape
        seq = piece * ndev
        dev = lax.axis_index('cp').astype(jnp.int32).reshape(1)
        x = x_in[0]
        dy = grad_y[0]
        x_float = x.astype(F32)
        inv_rms = lax.rsqrt(jnp.mean(x_float * x_float, axis=-1, keepdims=True) + NORM_EPS)
        normed = (x_float * inv_rms * norm_gain).astype(BF16)
        half = long_factor.shape[0]
        exponent = jnp.arange(half, dtype=F32) * (1.0 / half)
        inv_freq = 1.0 / (long_factor * jnp.power(10000.0, exponent))
        r_all, q_t, k_t, v_t, k_n, cos_t, sin_t = qkv_call(normed, positions, inv_freq, w_qkv)
        o_t, o_n, lse, dy_all = fwd_call(q_t, k_n, v_t, dy)
        o_recv, g_wout, dn_recv, gw_all = bwd_call(dy_all, r_all, q_t, o_t, k_t, v_t, lse, cos_t, sin_t, w_out, o_n)
        y_out = y_call(dev, o_recv, o_n, w_out, x)
        grad_x, gg = dx_call(dn_recv, w_qkv, x, inv_rms, norm_gain.reshape(1, hidden), dy)
        g_gain = lax.psum(gg.reshape(hidden), 'cp')
        g_wqkv = place_call(gw_all)
        return y_out[None], grad_x[None], g_gain, g_wqkv, g_wout

    seq_spec = P('dp', 'cp', None)
    return jax.shard_map(device_fn, mesh=mesh, in_specs=(seq_spec, P(('dp', 'cp')), P(None), P(None), P(None, None), P(None, None), seq_spec), out_specs=(seq_spec, seq_spec, P('dp'), P('dp', None), P('dp', None)), check_vma=False)
```

```python
import math
import jax
import jax.numpy as jnp
from jax import lax
from jax.experimental import pallas as pl
from jax.experimental.pallas import tpu as pltpu
from jax.sharding import PartitionSpec as P

NORM_EPS = 1e-5
MSCALE = math.sqrt(1.0 + math.log(32.0) / math.log(4096.0))
MASK_VALUE = -1e30
LOG2E = math.log2(math.e)
BF16 = jnp.bfloat16
F32 = jnp.float32
BLK = 512
VMEM_LIMIT = 60 * 2 ** 20
FLOPS_PER_BYTE = 1000
ROWS = 8
NDEV = 8
HEADS = 4
HD = 64
PAIR = 2 * HD
HALF = HD // 2
WIDTH = HEADS * HD


def dot_nn(a, b):
    return lax.dot_general(a, b, (((1,), (0,)), ((), ())), preferred_element_type=F32)


def dot_nt(a, b):
    return lax.dot_general(a, b, (((1,), (1,)), ((), ())), preferred_element_type=F32)


def inverse_rms(x):
    return lax.rsqrt(jnp.mean(x * x, axis=-1, keepdims=True) + NORM_EPS)


def params(n=1, **kw):
    return pltpu.CompilerParams(dimension_semantics=("arbitrary",) * n, vmem_limit_bytes=VMEM_LIMIT, **kw)


def cost(flops):
    return pl.CostEstimate(flops=int(flops), bytes_accessed=int(flops) // FLOPS_PER_BYTE, transcendentals=0)


def clear(ref):
    ref[...] = jnp.zeros_like(ref)


MESH = pl.DeviceIdType.MESH


class Grid:
    def __init__(self):
        self.me = lax.axis_index('cp')
        self.core = self.me % 2
        self.x = (self.me // 2) % 2
        self.y = self.me // 4

    def flip(self, yf, xf, cf):
        return ((self.y + yf) % 2) * 4 + ((self.x + xf) % 2) * 2 + (self.core + cf) % 2

    def xor(self, mask):
        return self.flip(mask // 4, (mask // 2) % 2, mask % 2)


def barrier(grid):
    sem = pltpu.get_barrier_semaphore()
    for mask in MASKS:
        pl.semaphore_signal(sem, inc=1, device_id={'cp': grid.xor(mask)}, device_id_type=MESH)
    pl.semaphore_wait(sem, len(MASKS))


class Gather:
    SENDS = {
        'xA': '0012', 'yB': '0114', 'xB': '0112', 'yA': '0014', 'own': '0021', 'dA': '2014', 'dB': '4112',
        'cxA': '2011', 'cyB': '4111', 'cxB': '2111', 'cyA': '4011', 'cdA': '6011', 'cdB': '6111',
    }
    ORDER = tuple(SENDS)

    def __init__(self, grid, src, dst, ssem, rsem):
        self.grid, self.src, self.dst, self.ssem, self.rsem = grid, src, dst, ssem, rsem

    def desc(self, name, arriving=False):
        mask, first, halves, target = map(int, self.SENDS[name])
        k = self.ORDER.index(name)
        dst = self.dst(self.grid.xor(mask ^ target if arriving else mask), first, halves)
        src = dst if (mask or arriving or self.src is None) else self.src(first, halves)
        return pltpu.make_async_remote_copy(src, dst, self.ssem(k), self.rsem(k), device_id={'cp': self.grid.xor(target)}, device_id_type=MESH)

    def send(self, *names):
        for name in names:
            self.desc(name).start()

    def arrived(self, *names):
        for name in names:
            self.desc(name, True).wait_recv()

    def begin(self):
        self.send('xA', 'yB', 'xB', 'yA', 'own')

    def first(self):
        self.arrived('xA', 'yB')
        self.send('dA', 'dB', 'cxA', 'cyB')

    def second(self):
        self.arrived('xB', 'yA')
        self.send('cxB', 'cyA')

    def third(self):
        self.arrived('dA', 'dB')
        self.send('cdA', 'cdB')

    def last(self):
        self.arrived('own', 'cxA', 'cyB', 'cxB', 'cyA', 'cdA', 'cdB')
        self.sent()

    def sent(self):
        for name in self.ORDER:
            self.desc(name).wait_send()


def row_gather(grid, src, dst, piece, ssem, rsem):
    half = piece // 2

    def place(owner, first, halves):
        return dst.at[pl.ds(pl.multiple_of(owner * piece + first * half, half), halves * half)]

    own = None if src is None else lambda first, halves: src.at[pl.ds(first * half, halves * half)]
    return Gather(grid, own, place, lambda k: ssem.at[k], lambda k: rsem.at[k])


COPIES = len(Gather.ORDER)
GATHER_SEMS = [pltpu.SemaphoreType.DMA((COPIES,))] * 2


MASKS = range(1, NDEV)
SEGMENTS = 11, 27, 33


def front_kernel(x_hbm, g_ref, pos_ref, inv_ref, w_hbm, dy_hbm,
                 r_all, dy_all, q_hbm, k_hbm, v_hbm, cos_hbm, sin_hbm, o_hbm, on_hbm, lse_hbm,
                 wtmp, w_scr, xbuf, rbuf, pos_scr, q_st, k_st, cos_st, sin_st, qz_scr, kn_scr, v_scr,
                 acc_scr, m_scr, l_scr, s_scr0, s_scr1, s_scr2, s_scr3, mx_scr, o_scr, on_scr, lse_scr,
                 wsem, lsem, osem, csem, fsem, pssem, prsem, ssem, rsem, dy_ssem, dy_rsem):
    grid = Grid()
    _, hp, hidden = xbuf.shape
    piece = 2 * hp
    nblk = qz_scr.shape[2] // BLK

    def w_copy(which):
        cols = pl.ds(pl.multiple_of((which * NDEV + grid.me) * WIDTH, WIDTH), WIDTH)
        return pltpu.make_async_copy(w_hbm.at[:, cols], wtmp.at[which], wsem.at[which])

    def pos_copy(mask, owner):
        return pltpu.make_async_remote_copy(pos_ref, pos_scr.at[pl.ds(2 * owner, 2)], pssem.at[mask], prsem.at[mask], device_id={'cp': grid.xor(mask)}, device_id_type=MESH)

    def own_half(hbm, u):
        return pltpu.make_async_copy(hbm.at[pl.ds(u * hp, hp)], xbuf.at[u], lsem.at[u])

    def keep(buf, gather, u):
        return pltpu.make_async_copy(buf.at[u], gather.dst(grid.me, u, 1), csem.at[u])

    gather = row_gather(grid, None, r_all, piece, ssem, rsem)
    gather_dy = row_gather(grid, dy_hbm, dy_all, piece, dy_ssem, dy_rsem)
    for u in range(2):
        own_half(x_hbm, u).start()
    for which in range(3):
        w_copy(which).start()
    for u in range(2):
        own_half(x_hbm, u).wait()

        def norm(c, carry):
            some = pl.ds(pl.multiple_of(c * HD, HD), HD)
            x = xbuf[u, some, :].astype(F32)
            rbuf[u, some, :] = (x * inverse_rms(x) * g_ref[...]).astype(BF16)
            return carry

        lax.fori_loop(0, hp // HD, norm, 0)
        keep(rbuf, gather, u).start()
        own_half(dy_hbm, u).start()
    barrier(grid)
    for mask in MASKS:
        pos_copy(mask, grid.me).start()
    for u in range(2):
        keep(rbuf, gather, u).wait()
    gather.begin()
    pos_scr[pl.ds(2 * grid.me, 2)] = pos_ref[...]
    clear(qz_scr)
    clear(acc_scr)
    for u in range(2):
        own_half(dy_hbm, u).wait()
        keep(xbuf, gather_dy, u).start()
    for which in range(3):
        w_copy(which).wait()
        w_scr[WIDTH * which:WIDTH * (which + 1)] = wtmp[which].T

    inv = inv_ref[...]

    def group(g, carry):
        stage = g // 2
        one = (stage + 2) // 3
        two = stage // 3
        first = (stage // 2) * (1 - two)
        halves = first, 1 - first
        owners = grid.flip(two, one, g % 2), grid.flip(one, two, g % 2)
        offs = [pl.multiple_of(owners[u] * piece + halves[u] * hp, PAIR) for u in range(2)]

        def load(u):
            return pltpu.make_async_copy(r_all.at[pl.ds(offs[u], hp)], rbuf.at[u], lsem.at[u])

        @pl.when(g == 1)
        def _():
            for mask in MASKS:
                pos_copy(mask, grid.xor(mask)).wait_recv()
            gather.arrived('own')

        @pl.when(g == 2)
        def _():
            gather.first()

        @pl.when(g == 3)
        def _():
            gather.arrived('cxA', 'cyB')

        @pl.when(g == 4)
        def _():
            gather.second()

        @pl.when(g == 5)
        def _():
            gather.arrived('cxB', 'cyA')

        @pl.when(g == 6)
        def _():
            gather.third()
            gather_dy.begin()

        @pl.when(g == 7)
        def _():
            gather.arrived('cdA', 'cdB')

        @pl.when(g > 0)
        def _():
            for u in range(2):
                load(u).start()

        outs = []
        for u in range(2):
            @pl.when(g > 0)
            def _():
                load(u).wait()

            angles = inv * pos_scr[2 * owners[u] + halves[u]].astype(F32)
            cos = jnp.cos(angles) * MSCALE
            sin = jnp.sin(angles) * MSCALE
            cos_st[u] = cos
            sin_st[u] = sin
            cols = pl.ds(offs[u], hp)

            def rope(t):
                t1, t2 = t[:HALF], t[HALF:]
                return jnp.concatenate([t1 * cos - t2 * sin, t2 * cos + t1 * sin], axis=0).astype(BF16)

            qkv = dot_nt(w_scr[...], rbuf[u])
            for h in range(HEADS):
                head = slice(HD * h, HD * (h + 1))
                q = rope(qkv[head]) * BF16(0.125)
                q_st[u, head] = q
                qz_scr[h, HD * (h % 2):HD * (h % 2 + 1), cols] = q
                k_st[u, head] = rope(qkv[WIDTH + HD * h:WIDTH + HD * (h + 1)])
            kn_scr[cols, :] = k_st[u].T
            v_scr[:, cols] = qkv[2 * WIDTH:].astype(BF16)
            some = [pltpu.make_async_copy(st.at[u], hbm.at[:, cols], osem.at[u, n]) for n, (st, hbm) in enumerate(((q_st, q_hbm), (k_st, k_hbm), (cos_st, cos_hbm), (sin_st, sin_hbm)))]
            for copy in some:
                copy.start()
            outs += some
        for copy in outs:
            copy.wait()
        return carry

    lax.fori_loop(0, NDEV, group, 0)
    v_out = pltpu.make_async_copy(v_scr, v_hbm, fsem.at[0])
    v_out.start()

    bufs = ((s_scr0, s_scr1), (s_scr2, s_scr3))

    def at(i):
        return pl.ds(pl.multiple_of(i * BLK, BLK), BLK)

    def two_heads(pair):
        return pl.ds(pl.multiple_of(pair * PAIR, PAIR), PAIR)

    def outputs(pair):
        rows = pl.ds(pl.multiple_of(pair * ROWS, ROWS), ROWS)
        return [
            pltpu.make_async_copy(o_scr.at[two_heads(pair)], o_hbm.at[two_heads(pair)], fsem.at[1]),
            pltpu.make_async_copy(on_scr.at[:, two_heads(pair)], on_hbm.at[:, two_heads(pair)], fsem.at[2]),
            pltpu.make_async_copy(lse_scr.at[rows], lse_hbm.at[rows], fsem.at[3]),
        ]

    def forward(pair, carry):
        m_scr[...] = jnp.full_like(m_scr, MASK_VALUE)
        clear(l_scr)

        def score(i, j, b, h, masked):
            s = dot_nn(kn_scr[at(j), two_heads(pair)], qz_scr[2 * pair + h, :, at(i)])
            if masked:
                krow = lax.broadcasted_iota(jnp.int32, s.shape, 0)
                qcol = lax.broadcasted_iota(jnp.int32, s.shape, 1)
                s = jnp.where(krow <= qcol, s, MASK_VALUE)
            bufs[b][h][...] = s
            row = 2 * b + h
            mx_scr[row:row + 1, :] = jnp.max(s, axis=0, keepdims=True)

        def weigh(i, j, b, h):
            row = slice(h, h + 1)
            m_old = m_scr[row, at(i)]
            m_new = jnp.maximum(m_old, mx_scr[2 * b + h:2 * b + h + 1, :])
            m_scr[row, at(i)] = m_new
            alpha = jnp.exp2((m_old - m_new) * LOG2E)
            p = jnp.exp2((bufs[b][h][...] - m_new) * LOG2E)
            l_scr[row, at(i)] = l_scr[row, at(i)] * alpha + jnp.sum(p, axis=0, keepdims=True)
            v = v_scr[pl.ds(pl.multiple_of((2 * pair + h) * HD, HD), HD), at(j)]
            acc_scr[h, :, at(i)] = acc_scr[h, :, at(i)] * alpha + dot_nn(v, p.astype(BF16))

        def both(later, now, b, masked):
            for h in range(2):
                score(*later, 1 - b, h, masked)
                weigh(*now, b, h)

        for h in range(2):
            score(0, 0, 0, h, True)

        def diagonal(t, carry):
            i = 2 * t
            both((i + 1, i + 1), (i, i), 0, True)
            e = jnp.minimum(i + 2, nblk - 1)
            both((e, e), (i + 1, i + 1), 1, True)
            return carry

        lax.fori_loop(0, nblk // 2, diagonal, 0)

        def following(i, j):
            wrap = (j + 1) // i
            return i + wrap, (j + 1) * (1 - wrap)

        for h in range(2):
            score(1, 0, 0, h, False)

        def below(t, carry):
            i, j = carry
            i1, j1 = following(i, j)
            both((i1, j1), (i, j), 0, False)
            i2, j2 = following(i1, j1)
            both((jnp.minimum(i2, nblk - 1), j2), (i1, j1), 1, False)
            return i2, j2

        def segment(g, carry):
            @pl.when((pair == 0) & (g == 1))
            def _():
                gather_dy.first()

            @pl.when((pair == 1) & (g == 0))
            def _():
                gather_dy.second()

            @pl.when((pair == 1) & (g == 2))
            def _():
                gather_dy.third()

            a, b, c = SEGMENTS
            start = jnp.where(g == 0, 0, jnp.where(g == 1, a, b))
            stop = jnp.where(g == 0, a, jnp.where(g == 1, b, c))
            return lax.fori_loop(start, stop, below, carry)

        lax.fori_loop(0, len(SEGMENTS), segment, (jnp.int32(1), jnp.int32(0)))

        @pl.when(pair == 1)
        def _():
            for copy in outputs(0):
                copy.wait()

        def finish(i, carry):
            outs = []
            for h in range(2):
                l = l_scr[h:h + 1, at(i)]
                outs.append((acc_scr[h, :, at(i)] / l).astype(BF16))
                lse_scr[pl.ds(pair * ROWS + h, 1), at(i)] = m_scr[h:h + 1, at(i)] + jnp.log(l)
            o = jnp.concatenate(outs, axis=0)
            o_scr[two_heads(pair), at(i)] = o
            on_scr[at(i), two_heads(pair)] = o.T
            return carry

        lax.fori_loop(0, nblk, finish, 0)
        for copy in outputs(pair):
            copy.start()
        return carry

    lax.fori_loop(0, 2, forward, 0)
    for copy in outputs(1):
        copy.wait()
    v_out.wait()
    for u in range(2):
        keep(xbuf, gather_dy, u).wait()
    gather.sent()
    for mask in MASKS:
        pos_copy(mask, grid.me).wait_send()
    gather_dy.last()


def front_call(x, gain, pos, inv_freq, w_qkv, dy):
    piece, hidden = x.shape
    seq = piece * NDEV
    hp = piece // 2
    hbm = pl.BlockSpec(memory_space=pl.ANY)
    vmem = pl.BlockSpec(memory_space=pltpu.VMEM)
    dma = pltpu.SemaphoreType.DMA
    all_b = lambda *shape: jax.ShapeDtypeStruct(shape, BF16)
    all_f = lambda *shape: jax.ShapeDtypeStruct(shape, F32)
    b = lambda *shape: pltpu.VMEM(shape, BF16)
    f = lambda *shape: pltpu.VMEM(shape, F32)
    tr = all_b(WIDTH, seq)
    tab = all_f(HALF, seq)
    return pl.pallas_call(
        front_kernel,
        out_shape=(all_b(seq, hidden), all_b(seq, hidden), tr, tr, tr, tab, tab, tr, all_b(seq, WIDTH), all_f(2 * ROWS, seq)),
        in_specs=[hbm, vmem, vmem, vmem, hbm, hbm],
        out_specs=(hbm,) * 10,
        scratch_shapes=[
            b(3, hidden, WIDTH), b(3 * WIDTH, hidden), b(2, hp, hidden), b(2, hp, hidden), pltpu.VMEM((2 * NDEV, 1, hp), jnp.int32),
            b(2, WIDTH, hp), b(2, WIDTH, hp), f(2, HALF, hp), f(2, HALF, hp), b(HEADS, PAIR, seq), b(seq, WIDTH), b(WIDTH, seq),
            f(2, HD, seq), f(ROWS, seq), f(ROWS, seq), f(BLK, BLK), f(BLK, BLK), f(BLK, BLK), f(BLK, BLK), f(ROWS, BLK),
            b(WIDTH, seq), b(seq, WIDTH), f(2 * ROWS, seq),
            dma((3,)), dma((2,)), dma((2, 4)), dma((2,)), dma((4,)), dma((NDEV,)), dma((NDEV,)),
        ] + GATHER_SEMS * 2,
        compiler_params=pltpu.CompilerParams(collective_id=0, has_side_effects=True, vmem_limit_bytes=VMEM_LIMIT),
        cost_estimate=cost(2 * seq * seq * WIDTH),
        name="front",
    )(x, gain, pos.reshape(2, 1, hp), inv_freq.reshape(HALF, 1), w_qkv, dy)


def split3(value):
    hi = value.astype(BF16).astype(F32)
    mid = (value - hi).astype(BF16).astype(F32)
    return hi, mid, value - hi - mid


FIRST, SECOND, THIRD = 6, 9, 2


def bwd_kernel(dy_ref, r_ref, q_ref, o_ref, k_ref, v_ref, lse_ref, cos_ref, sin_ref, w_hbm, on_hbm, x_hbm,
               y_hbm, o_recv, gwo_all, dn_recv, gw_all, gw_last,
               do_scr, w_scr, gwo_scr, qa_scr, doa_scr, ka_scr, va_scr, dq_scr, dk_scr, dv_scr, dn_scr, gw_scr, o_scr, x_scr, wc_scr,
               ysem, wsem, lsem, o_ssem, o_rsem, d_ssem, d_rsem, g_ssem, g_rsem):
    s = pl.program_id(0)
    nblk = do_scr.shape[1] // BLK
    grid = Grid()
    width, hidden = w_scr.shape
    piece = x_hbm.shape[0]
    row64 = lax.broadcasted_iota(jnp.int32, (HD, BLK), 0)

    def blk(t):
        return pl.ds(pl.multiple_of(t * BLK, BLK), BLK)

    def o_copy(mask, owner):
        src = on_hbm.at[pl.ds(pl.multiple_of(grid.xor(mask) * piece, piece), piece)]
        return pltpu.make_async_remote_copy(src, o_recv.at[owner], o_ssem.at[mask], o_rsem.at[mask], device_id={'cp': grid.xor(mask)}, device_id_type=MESH)

    def dn_cols(owner):
        return pl.ds(pl.multiple_of(owner * piece, 128), piece)

    def dn_copy(h, mask, owner):
        src = dn_scr.at[h % 2, :, dn_cols(grid.xor(mask))]
        return pltpu.make_async_remote_copy(src, dn_recv.at[h, owner], d_ssem.at[h, mask], d_rsem.at[h, mask], device_id={'cp': grid.xor(mask)}, device_id_type=MESH)

    def dn_own(h):
        return pltpu.make_async_copy(dn_scr.at[h % 2, :, dn_cols(grid.me)], dn_recv.at[h, grid.me], lsem.at[0])

    def gw_own(h):
        return pltpu.make_async_copy(gw_scr.at[h % 2], gw_all.at[grid.me, h], lsem.at[1])

    def keep_last():
        return pltpu.make_async_copy(gw_scr.at[(HEADS - 1) % 2], gw_last, lsem.at[1])

    def gw_gather(h):
        half = 3 * HALF
        return Gather(grid, None, lambda owner, first, halves: gw_all.at[owner, h, pl.ds(first * half, halves * half)], lambda k: g_ssem.at[h, k], lambda k: g_rsem.at[h, k])

    def project_y():
        wide = wc_scr.shape[2]

        def chunk(c):
            return slice(c * wide, (c + 1) * wide)

        def w_chunk(c):
            return pltpu.make_async_copy(w_hbm.at[:, chunk(c)], wc_scr.at[c % 2], ysem.at[c % 2])

        def o_part(owner):
            src = o_recv.at[owner] if owner is not None else on_hbm.at[pl.ds(pl.multiple_of(grid.me * piece, piece), piece)]
            col = owner if owner is not None else grid.me
            return pltpu.make_async_copy(src, o_scr.at[:, pl.ds(pl.multiple_of(col * width, width), width)], ysem.at[2])

        x_in = pltpu.make_async_copy(x_hbm, x_scr, ysem.at[2])
        parts = [o_part(grid.xor(mask)) for mask in MASKS] + [o_part(None), x_in]
        w_chunk(0).start()
        for part in parts:
            part.start()
        for part in parts:
            part.wait()
        for c in range(hidden // wide):
            w_chunk(c).wait()
            if c + 1 < hidden // wide:
                w_chunk(c + 1).start()
            part = dot_nn(o_scr[...], wc_scr[c % 2])
            x_scr[:, chunk(c)] = (x_scr[:, chunk(c)].astype(F32) + part).astype(BF16)
        out = pltpu.make_async_copy(x_scr, y_hbm, ysem.at[2])
        out.start()
        out.wait()

    gwo_gather = row_gather(grid, None, gwo_all, width, g_ssem.at[HEADS], g_rsem.at[HEADS])

    @pl.when(s == 0)
    def _():
        w_copy = pltpu.make_async_copy(w_hbm.at[pl.ds(pl.multiple_of(grid.me * width, width), width)], w_scr, wsem)
        w_copy.start()
        barrier(grid)
        for mask in MASKS:
            o_copy(mask, grid.me).start()
        w_copy.wait()
        clear(gwo_scr)

    @pl.when(s < nblk)
    def _():
        cols = blk(s)
        dy = dy_ref[...]
        do_scr[:, cols] = dot_nt(w_scr[...], dy).astype(BF16)
        gwo_scr[...] += dot_nn(o_ref[:, cols], dy)

    @pl.when(s == nblk)
    def _():
        own = pltpu.make_async_copy(gwo_scr, gwo_gather.dst(grid.me, 0, 2), lsem.at[1])
        own.start()
        own.wait()
        gwo_gather.begin()

    t = s - nblk
    h = t // nblk
    j = t % nblk

    def send_head(h):
        dn_own(h).start()
        for mask in MASKS:
            dn_copy(h, mask, grid.me).start()

    @pl.when((t >= nblk) & (j == 0))
    def _():
        send_head(h - 1)
        gw_own(h - 1).start()

    @pl.when((t >= nblk) & (j == 1))
    def _():
        gw_own(h - 1).wait()
        dn_own(h - 1).wait()
        gw_gather(h - 1).begin()

    @pl.when((t >= 2 * nblk) & (j == 0))
    def _():
        for mask in MASKS:
            dn_copy(h - 2, mask, grid.me).wait_send()

    @pl.when((t >= nblk) & (j == FIRST))
    def _():
        gw_gather(h - 1).first()

    @pl.when((t >= nblk) & (j == SECOND))
    def _():
        gw_gather(h - 1).second()

    @pl.when((t >= 2 * nblk) & (j == THIRD))
    def _():
        gw_gather(h - 2).third()

    @pl.when(t == 5)
    def _():
        gwo_gather.first()

    @pl.when(t == 8)
    def _():
        gwo_gather.second()

    @pl.when(t == nblk + THIRD)
    def _():
        gwo_gather.third()

    @pl.when(t >= 0)
    def _():
        rows = pl.ds(pl.multiple_of(h * HD, HD), HD)

        @pl.when(j == 0)
        def _():
            clear(dq_scr)
            gw_scr[h % 2] = jnp.zeros(gw_scr.shape[1:], F32)

            def augment(data, stat):
                hi, mid, lo = split3(-stat)
                extra = jnp.where(row64 == 0, hi, jnp.where(row64 == 1, mid, jnp.where(row64 == 2, lo, 0.0))).astype(BF16)
                return jnp.concatenate([data, extra], axis=0).T

            def prep(i, carry):
                cols = blk(i)
                do_h = do_scr[rows, cols]
                delta = jnp.sum(do_h.astype(F32) * o_ref[rows, cols].astype(F32), axis=0, keepdims=True)
                qa_scr[cols, :] = augment(q_ref[rows, cols], lse_ref[pl.ds((h // 2) * ROWS + h % 2, 1), cols])
                doa_scr[cols, :] = augment(do_h, delta)
                return carry

            lax.fori_loop(0, nblk, prep, 0)

        ones = jnp.where(row64 < 3, 1.0, 0.0).astype(BF16)
        ka_scr[...] = jnp.concatenate([k_ref[rows, :], ones], axis=0)
        va_scr[...] = jnp.concatenate([v_ref[rows, :], ones], axis=0)
        clear(dk_scr)
        clear(dv_scr)

        def step(i, masked):
            cols = blk(i)
            scores = dot_nn(qa_scr[cols, :], ka_scr[...])
            if masked:
                qrow = lax.broadcasted_iota(jnp.int32, scores.shape, 0)
                kcol = lax.broadcasted_iota(jnp.int32, scores.shape, 1)
                scores = jnp.where(kcol <= qrow, scores, MASK_VALUE)
            p = jnp.exp2(scores * LOG2E)
            dp = dot_nn(doa_scr[cols, :], va_scr[...])
            ds = (p * dp).astype(BF16)
            dv_scr[...] += dot_nn(do_scr[rows, cols], p.astype(BF16))
            dk_scr[...] += dot_nn(q_ref[rows, cols], ds)
            dq_scr[:, cols] += dot_nt(k_ref[rows, :], ds)

        def body(i, carry):
            step(i, False)
            return carry

        step(j, True)
        lax.fori_loop(j + 1, nblk, body, 0)

        cos = cos_ref[...]
        sin = sin_ref[...]

        def unrope(v, scale):
            v1 = v[0:HALF] * scale
            v2 = v[HALF:HD] * scale
            return [v1 * cos + v2 * sin, v2 * cos - v1 * sin]

        grads = jnp.concatenate(unrope(dq_scr[:, blk(j)], 0.125) + unrope(dk_scr[...], 1.0) + [dv_scr[...]], axis=0).astype(BF16)
        dn_scr[h % 2, :, blk(j)] = grads
        gw_scr[h % 2] += dot_nn(grads, r_ref[...])

    @pl.when(s == pl.num_programs(0) - 1)
    def _():
        end = HEADS - 1
        keep_last().start()
        send_head(end)
        for mask in MASKS:
            o_copy(mask, grid.xor(mask)).wait_recv()
        project_y()
        gw_gather(end - 1).third()
        keep_last().wait()
        dn_own(end).wait()
        for mask in MASKS:
            o_copy(mask, grid.me).wait_send()
            for head in range(HEADS):
                dn_copy(head, mask, grid.xor(mask)).wait_recv()
            for head in range(HEADS - 2, HEADS):
                dn_copy(head, mask, grid.me).wait_send()
        gwo_gather.last()
        for head in range(end):
            gw_gather(head).last()


def bwd_call(dy_all, r_all, q_t, o_t, k_t, v_t, lse, cos_t, sin_t, w_out, o_n, x):
    seq, hidden = dy_all.shape
    width = q_t.shape[0]
    half = cos_t.shape[0]
    ndev = NDEV
    piece = seq // ndev
    nblk = seq // BLK
    hbm = pl.BlockSpec(memory_space=pl.ANY)
    whole = lambda *shape: pl.BlockSpec(shape, lambda s: (0, 0), pipeline_mode=pl.Buffered(1))
    cols = lambda rows: pl.BlockSpec((rows, BLK), lambda s: (0, lax.rem(s, nblk)))
    rblk = lambda s: jnp.where(s < nblk, 0, lax.rem(s, nblk))
    rows = 3 * HD
    dma = pltpu.SemaphoreType.DMA
    return pl.pallas_call(
        bwd_kernel,
        out_shape=(
            jax.ShapeDtypeStruct((piece, hidden), BF16),
            jax.ShapeDtypeStruct((ndev, piece, width), BF16),
            jax.ShapeDtypeStruct((ndev * width, hidden), F32),
            jax.ShapeDtypeStruct((HEADS, ndev, rows, piece), BF16),
            jax.ShapeDtypeStruct((ndev, HEADS - 1, rows, hidden), F32),
            jax.ShapeDtypeStruct((rows, hidden), F32),
        ),
        grid=(nblk * (1 + HEADS),),
        in_specs=[
            pl.BlockSpec((BLK, hidden), lambda s: (jnp.minimum(s, nblk - 1), 0)),
            pl.BlockSpec((BLK, hidden), lambda s: (rblk(s), 0)),
            whole(width, seq), whole(width, seq),
            cols(width), cols(width),
            whole(2 * ROWS, seq),
            cols(half), cols(half),
            hbm, hbm, hbm,
        ],
        out_specs=(hbm,) * 6,
        scratch_shapes=[
            pltpu.VMEM((width, seq), BF16), pltpu.VMEM((width, hidden), BF16), pltpu.VMEM((width, hidden), F32),
            pltpu.VMEM((seq, PAIR), BF16), pltpu.VMEM((seq, PAIR), BF16),
            pltpu.VMEM((PAIR, BLK), BF16), pltpu.VMEM((PAIR, BLK), BF16),
            pltpu.VMEM((HD, seq), F32), pltpu.VMEM((HD, BLK), F32), pltpu.VMEM((HD, BLK), F32),
            pltpu.VMEM((2, rows, seq), BF16), pltpu.VMEM((2, rows, hidden), F32),
            pltpu.VMEM((piece, hidden), BF16), pltpu.VMEM((piece, hidden), BF16), pltpu.VMEM((2, hidden, BLK), BF16),
            dma((3,)), dma, dma((2,)), dma((ndev,)), dma((ndev,)), dma((HEADS, ndev)), dma((HEADS, ndev)), dma((HEADS + 1, COPIES)), dma((HEADS + 1, COPIES)),
        ],
        compiler_params=params(1, collective_id=2, has_side_effects=True),
        cost_estimate=cost(5 * seq * seq * width),
        name="backward",
    )(dy_all, r_all, q_t, o_t, k_t, v_t, lse, cos_t, sin_t, w_out, o_n, x)


PARTS = 4


def write_columns(step, steps, rows_of, column_of, out, stage, sem):
    lanes = PAIR
    slot = step % 2

    def copies(slot, column_of):
        return [pltpu.make_async_copy(stage.at[slot, :, lanes * k:lanes * (k + 1)], out.at[:, pl.ds(pl.multiple_of(column_of(k), lanes), lanes)], sem.at[slot, k]) for k in range(PARTS)]

    @pl.when(step >= 2)
    def _():
        for copy in copies(slot, column_of):
            copy.wait()

    for k in range(PARTS):
        stage[slot, :, lanes * k:lanes * (k + 1)] = rows_of(k).T
    for copy in copies(slot, column_of):
        copy.start()

    @pl.when(step == steps - 1)
    def _():
        for copy in copies(1 - slot, column_of) + copies(slot, column_of):
            copy.wait()


def stage_shapes(hidden):
    return [pltpu.VMEM((2, hidden, PARTS * PAIR), F32), pltpu.SemaphoreType.DMA((2, PARTS))]


def place_kernel(gw_ref, out, stage, sem):
    w, part = pl.program_id(0), pl.program_id(1)
    parts = pl.num_programs(1)
    rows = lambda k: jnp.concatenate([gw_ref[k, 0], gw_ref[k, 1]], axis=0)
    column = lambda k: (w * parts * PARTS + part * PARTS + k) * HEADS * HD
    write_columns(w * parts + part, 3 * parts, rows, column, out, stage, sem)


def place_call(gw_all):
    ndev, _, rows, hidden = gw_all.shape
    return pl.pallas_call(
        place_kernel,
        out_shape=jax.ShapeDtypeStruct((hidden, 3 * ndev * HEADS * HD), F32),
        grid=(3, ndev // PARTS),
        in_specs=[pl.BlockSpec((PARTS, 2, HD, hidden), lambda w, d: (d, 0, w, 0))],
        out_specs=pl.BlockSpec(memory_space=pl.ANY),
        scratch_shapes=stage_shapes(hidden),
        compiler_params=params(2),
        cost_estimate=cost(20e9),
        name="place_first",
    )(gw_all)


def copy_kernel(src, out):
    out[...] = src[...]


def copy_call(src):
    rows, cols = src.shape
    spec = pl.BlockSpec((BLK, cols), lambda i: (i, 0))
    return pl.pallas_call(
        copy_kernel,
        out_shape=jax.ShapeDtypeStruct(src.shape, src.dtype),
        grid=(rows // BLK,),
        in_specs=[spec],
        out_specs=spec,
        compiler_params=params(1),
        cost_estimate=cost(10e9),
        name="copy_wout",
    )(src)


def flip_bits(m, d):
    return sum((m // k + d // k) % 2 * k for k in (1, 2, 4))


def place_last_kernel(d_ref, *refs):
    thirds, refs = refs[:PARTS], refs[PARTS:]
    pieces, (_, out, stage, sem) = refs[:10], refs[10:]
    w, part = pl.program_id(0), pl.program_id(1)
    parts = pl.num_programs(1)
    last = [p[...] for p in pieces[:6]] + [jnp.concatenate([pieces[k][...], pieces[k + 1][...]], axis=1) for k in (6, 8)]
    rows = lambda k: jnp.concatenate([thirds[k][0, 0], jnp.where(part == 0, last[k], last[PARTS + k])], axis=0)
    column = lambda k: (w * parts * PARTS + flip_bits(part * PARTS + k, d_ref[0])) * HEADS * HD + PAIR
    write_columns(w * parts + part, 3 * parts, rows, column, out, stage, sem)


def place_last_call(dev, gw_all, pieces, g_wqkv):
    ndev, _, rows, hidden = gw_all.shape

    def third(k):
        return pl.BlockSpec((1, 1, HD, hidden), lambda w, p, d: (flip_bits(p * PARTS + k, d[0]), 2, w, 0))

    hbm = pl.BlockSpec(memory_space=pl.ANY)
    operands = [gw_all] * PARTS + list(pieces) + [g_wqkv]
    return pl.pallas_call(
        place_last_kernel,
        out_shape=jax.ShapeDtypeStruct(g_wqkv.shape, F32),
        grid_spec=pltpu.PrefetchScalarGridSpec(
            num_scalar_prefetch=1,
            grid=(3, ndev // PARTS),
            in_specs=[third(k) for k in range(PARTS)]
            + [pl.BlockSpec((HD, p.shape[1]), lambda w, q, d: (w, 0)) for p in pieces]
            + [hbm],
            out_specs=hbm,
            scratch_shapes=stage_shapes(hidden),
        ),
        input_output_aliases={len(operands): 0},
        compiler_params=params(2),
        cost_estimate=cost(1e6),
        name="place_last",
    )(dev, *operands)


def dx_kernel(dn_ref, wq_ref, wk_ref, wv_ref, x_ref, g_ref, dy_ref, dx_out, gg_out, acc_scr):
    s = pl.program_id(0)
    rhs = jnp.concatenate([dn_ref[h, 0, HD * w:HD * (w + 1)] for w in range(3) for h in range(HEADS)], axis=0)
    part = dot_nn(jnp.concatenate([wq_ref[...], wk_ref[...], wv_ref[...]], axis=1), rhs)

    @pl.when(s == 0)
    def _():
        acc_scr[...] = part

    @pl.when(s > 0)
    def _():
        acc_scr[...] += part

    @pl.when(s == pl.num_programs(0) - 1)
    def _():
        gain = g_ref[...]
        clear(gg_out)

        def tokens(c, carry):
            some = pl.ds(pl.multiple_of(c * PAIR, PAIR), PAIR)
            dn = acc_scr[:, some].T
            x = x_ref[some, :].astype(F32)
            inv = inverse_rms(x)
            x_hat = x * inv
            gg_out[...] += jnp.sum(dn * x_hat, axis=0, keepdims=True)
            d_hat = dn * gain
            mean = jnp.mean(d_hat * x_hat, axis=-1, keepdims=True)
            dx_out[some, :] = (dy_ref[some, :].astype(F32) + inv * (d_hat - x_hat * mean)).astype(BF16)
            return carry

        lax.fori_loop(0, x_ref.shape[0] // (PAIR), tokens, 0)


def dx_call(dn_recv, w_qkv, x, gain, dy):
    _, ndev, rows, piece = dn_recv.shape
    hidden = w_qkv.shape[0]
    width = HEADS * HD
    wspec = lambda which: pl.BlockSpec((hidden, width), lambda s: (0, which * ndev + s))
    whole = lambda *shape: pl.BlockSpec(shape, lambda s: (0, 0), pipeline_mode=pl.Buffered(1))
    return pl.pallas_call(
        dx_kernel,
        out_shape=(jax.ShapeDtypeStruct((piece, hidden), BF16), jax.ShapeDtypeStruct((1, hidden), F32)),
        grid=(ndev,),
        in_specs=[pl.BlockSpec((HEADS, 1, rows, piece), lambda s: (0, s, 0, 0)), wspec(0), wspec(1), wspec(2), whole(piece, hidden), whole(1, hidden), whole(piece, hidden)],
        out_specs=(whole(piece, hidden), whole(1, hidden)),
        scratch_shapes=[pltpu.VMEM((hidden, piece), F32)],
        compiler_params=params(1),
        cost_estimate=cost(2 * piece * hidden * 3 * ndev * width),
        name="dx",
    )(dn_recv, w_qkv, w_qkv, w_qkv, x, gain, dy)


def solution(mesh):
    ndev = mesh.shape['cp']

    def device_fn(x_in, positions, long_factor, norm_gain, w_qkv, w_out, grad_y):
        _, piece, hidden = x_in.shape
        seq = piece * ndev
        dev = lax.axis_index('cp').astype(jnp.int32).reshape(1)
        x = x_in[0]
        dy = grad_y[0]
        gain = norm_gain.reshape(1, hidden)
        half = long_factor.shape[0]
        exponent = jnp.arange(half, dtype=F32) * (1.0 / half)
        inv_freq = 1.0 / (long_factor * jnp.power(10000.0, exponent))
        r_all, dy_all, q_t, k_t, v_t, cos_t, sin_t, o_t, o_n, lse = front_call(x, gain, positions, inv_freq, w_qkv, dy)
        y_out, _, wout_all, dn_recv, gw_all, own = bwd_call(dy_all, r_all, q_t, o_t, k_t, v_t, lse, cos_t, sin_t, w_out, o_n, x)

        def swap(value, mask):
            return lax.ppermute(value, 'cp', [(i, i ^ mask) for i in range(ndev)])

        cut = hidden // 2
        from_x, from_y, from_c = swap(own, 2), swap(own, 4), swap(own, 1)
        grad_x, gg = dx_call(dn_recv, w_qkv, x, gain, dy)
        from_x, from_y, from_c, gain, gw_all = lax.optimization_barrier((from_x, from_y, from_c, gg, gw_all))
        diag_a, diag_b = swap(from_x[:, :cut], 4), swap(from_y[:, cut:], 2)
        from_cx, from_cy = swap(from_x, 1), swap(from_y, 1)
        gain_x = swap(gain, 2)
        g_wqkv = place_call(gw_all)
        diag_a, diag_b, gain_x, g_wqkv, wout_all = lax.optimization_barrier((diag_a, diag_b, gain_x, g_wqkv, wout_all))
        diag_ca, diag_cb = swap(diag_a, 1), swap(diag_b, 1)
        gain = gain + gain_x
        gain_y = swap(gain, 4)
        g_wout = copy_call(wout_all)
        diag_ca, diag_cb, gain_y, g_wout, g_wqkv = lax.optimization_barrier((diag_ca, diag_cb, gain_y, g_wout, g_wqkv))
        gain = gain + gain_y
        g_gain = (gain + swap(gain, 1)).reshape(hidden)
        pieces = own, from_c, from_x, from_cx, from_y, from_cy, diag_a, diag_b, diag_ca, diag_cb
        g_wqkv = place_last_call(dev, gw_all, pieces, g_wqkv)
        return y_out[None], grad_x[None], g_gain, g_wqkv, g_wout

    seq_spec = P('dp', 'cp', None)
    return jax.shard_map(device_fn, mesh=mesh, in_specs=(seq_spec, P(('dp', 'cp')), P(None), P(None), P(None, None), P(None, None), seq_spec), out_specs=(seq_spec, seq_spec, P('dp'), P('dp', None), P('dp', None)), check_vma=False)
```

```python
import math
import jax
import jax.numpy as jnp
from jax import lax
from jax.experimental import pallas as pl
from jax.experimental.pallas import tpu as pltpu
from jax.sharding import PartitionSpec as P

NORM_EPS = 1e-5
MSCALE = math.sqrt(1.0 + math.log(32.0) / math.log(4096.0))
MASK_VALUE = -1e30
LOG2E = math.log2(math.e)
BF16 = jnp.bfloat16
F32 = jnp.float32
BLK = 512
VMEM_LIMIT = 60 * 2 ** 20
FLOPS_PER_BYTE = 1000
ROWS = 8
NDEV = 8
HEADS = 4
HD = 64
PAIR = 2 * HD
HALF = HD // 2
WIDTH = HEADS * HD
BOTH = range(2)


def dot_nn(a, b):
    return lax.dot_general(a, b, (((1,), (0,)), ((), ())), preferred_element_type=F32)


def dot_nt(a, b):
    return lax.dot_general(a, b, (((1,), (1,)), ((), ())), preferred_element_type=F32)


def inverse_rms(x):
    return lax.rsqrt(jnp.mean(x * x, axis=-1, keepdims=True) + NORM_EPS)


def params(n=1, **kw):
    return pltpu.CompilerParams(dimension_semantics=("arbitrary",) * n, vmem_limit_bytes=VMEM_LIMIT, **kw)


def cost(flops):
    return pl.CostEstimate(flops=int(flops), bytes_accessed=int(flops) // FLOPS_PER_BYTE, transcendentals=0)


def stack(parts):
    return jnp.concatenate(parts, axis=0)


def beside(parts):
    return jnp.concatenate(parts, axis=1)


def column_sum(x):
    return jnp.sum(x, axis=0, keepdims=True)


def span(i, size):
    return slice(i * size, (i + 1) * size)


def block(i, size):
    return pl.ds(pl.multiple_of(i * size, size), size)


def clear(ref):
    ref[...] = jnp.zeros_like(ref)


MESH = pl.DeviceIdType.MESH


class Grid:
    def __init__(self):
        self.me = lax.axis_index('cp')
        self.core = self.me % 2
        self.x = (self.me // 2) % 2
        self.y = self.me // 4

    def flip(self, yf, xf, cf):
        return ((self.y + yf) % 2) * 4 + ((self.x + xf) % 2) * 2 + (self.core + cf) % 2

    def xor(self, mask):
        return self.flip(mask // 4, (mask // 2) % 2, mask % 2)


def barrier(grid):
    sem = pltpu.get_barrier_semaphore()
    for mask in MASKS:
        pl.semaphore_signal(sem, inc=1, device_id={'cp': grid.xor(mask)}, device_id_type=MESH)
    pl.semaphore_wait(sem, len(MASKS))


class Gather:
    SENDS = {
        'xA': '0012', 'yB': '0114', 'xB': '0112', 'yA': '0014', 'own': '0021', 'dA': '2014', 'dB': '4112',
        'cxA': '2011', 'cyB': '4111', 'cxB': '2111', 'cyA': '4011', 'cdA': '6011', 'cdB': '6111',
    }
    ORDER = tuple(SENDS)

    def __init__(self, grid, src, dst, ssem, rsem):
        self.grid, self.src, self.dst, self.ssem, self.rsem = grid, src, dst, ssem, rsem

    def desc(self, name, arriving=False):
        mask, first, halves, target = map(int, self.SENDS[name])
        k = self.ORDER.index(name)
        dst = self.dst(self.grid.xor(mask ^ target if arriving else mask), first, halves)
        src = dst if (mask or arriving or self.src is None) else self.src(first, halves)
        return pltpu.make_async_remote_copy(src, dst, self.ssem(k), self.rsem(k), device_id={'cp': self.grid.xor(target)}, device_id_type=MESH)

    def send(self, *names):
        for name in names:
            self.desc(name).start()

    def arrived(self, *names):
        for name in names:
            self.desc(name, True).wait_recv()

    def begin(self):
        self.send('xA', 'yB', 'xB', 'yA', 'own')

    def first(self):
        self.arrived('xA', 'yB')
        self.send('dA', 'dB', 'cxA', 'cyB')

    def second(self):
        self.arrived('xB', 'yA')
        self.send('cxB', 'cyA')

    def third(self):
        self.arrived('dA', 'dB')
        self.send('cdA', 'cdB')

    def last(self):
        self.arrived('own', 'cxA', 'cyB', 'cxB', 'cyA', 'cdA', 'cdB')
        self.sent()

    def sent(self):
        for name in self.ORDER:
            self.desc(name).wait_send()


def row_gather(grid, src, dst, piece, ssem, rsem):
    half = piece // 2

    def place(owner, first, halves):
        return dst.at[pl.ds(pl.multiple_of(owner * piece + first * half, half), halves * half)]

    own = None if src is None else lambda first, halves: src.at[pl.ds(first * half, halves * half)]
    return Gather(grid, own, place, lambda k: ssem.at[k], lambda k: rsem.at[k])


COPIES = len(Gather.ORDER)
GATHER_SEMS = [pltpu.SemaphoreType.DMA((COPIES,))] * 2


MASKS = range(1, NDEV)
SEGMENTS = 11, 27, 33


def exchange_o(grid, on_hbm, o_recv, pair, mask, owner, ssem, rsem):
    src = on_hbm.at[block(grid.xor(mask), o_recv.shape[1]), span(pair, PAIR)]
    return pltpu.make_async_remote_copy(src, o_recv.at[owner], ssem.at[mask], rsem.at[mask], device_id={'cp': grid.xor(mask)}, device_id_type=MESH)


def front_kernel(x_hbm, g_ref, pos_ref, inv_ref, w_hbm, dy_hbm,
                 r_all, dy_all, q_hbm, k_hbm, v_hbm, cos_hbm, sin_hbm, o_hbm, on_hbm, lse_hbm, o_recv,
                 wtmp, w_scr, buf, pos_scr, q_st, k_st, cos_st, sin_st, qz_scr, kn_scr, v_scr,
                 acc_scr, m_scr, l_scr, s_scr0, s_scr1, s_scr2, s_scr3, mx_scr, o_scr, on_scr, lse_scr,
                 wsem, lsem, osem, csem, fsem, pssem, prsem, o_ssem, o_rsem, ssem, rsem, dy_ssem, dy_rsem):
    grid = Grid()
    _, hp, hidden = buf.shape
    piece = 2 * hp
    nblk = qz_scr.shape[2] // BLK

    def w_copy(which):
        cols = pl.ds(pl.multiple_of((which * NDEV + grid.me) * WIDTH, WIDTH), WIDTH)
        return pltpu.make_async_copy(w_hbm.at[:, cols], wtmp.at[which], wsem.at[which])

    def pos_copy(mask, owner):
        return pltpu.make_async_remote_copy(pos_ref, pos_scr.at[pl.ds(2 * owner, 2)], pssem.at[mask], prsem.at[mask], device_id={'cp': grid.xor(mask)}, device_id_type=MESH)

    def own_half(hbm, u):
        return pltpu.make_async_copy(hbm.at[block(u, hp)], buf.at[2 + u], lsem.at[2 + u])

    def keep(slot, gather, u):
        return pltpu.make_async_copy(buf.at[slot + u], gather.dst(grid.me, u, 1), csem.at[slot + u])

    def o_copy(mask, owner):
        return exchange_o(grid, on_hbm, o_recv, 0, mask, owner, o_ssem, o_rsem)

    gather = row_gather(grid, None, r_all, piece, ssem, rsem)
    gather_dy = row_gather(grid, dy_hbm, dy_all, piece, dy_ssem, dy_rsem)
    for u in BOTH:
        own_half(x_hbm, u).start()
    for which in range(3):
        w_copy(which).start()
    for u in BOTH:
        own_half(x_hbm, u).wait()

        def norm(c, carry):
            some = block(c, HD)
            x = buf[2 + u, some, :].astype(F32)
            buf[u, some, :] = (x * inverse_rms(x) * g_ref[...]).astype(BF16)
            return carry

        lax.fori_loop(0, hp // HD, norm, 0)
        keep(0, gather, u).start()
        own_half(dy_hbm, u).start()
    barrier(grid)
    for mask in MASKS:
        pos_copy(mask, grid.me).start()
    for u in BOTH:
        keep(0, gather, u).wait()
    gather.begin()
    pos_scr[pl.ds(2 * grid.me, 2)] = pos_ref[...]
    clear(qz_scr)
    clear(acc_scr)
    for u in BOTH:
        own_half(dy_hbm, u).wait()
        keep(2, gather_dy, u).start()
    for which in range(3):
        w_copy(which).wait()
        w_scr[span(which, WIDTH)] = wtmp[which].T

    inv = inv_ref[...]

    def stores(u, cols):
        pairs = (q_st, q_hbm), (k_st, k_hbm), (cos_st, cos_hbm), (sin_st, sin_hbm)
        return [pltpu.make_async_copy(st.at[u], hbm.at[:, cols], osem.at[u, n]) for n, (st, hbm) in enumerate(pairs)]

    def group(g, carry):
        stage = g // 2
        one = (stage + 2) // 3
        two = stage // 3
        first = (stage // 2) * (1 - two)
        halves = first, 1 - first
        owners = grid.flip(two, one, g % 2), grid.flip(one, two, g % 2)
        offs = [pl.multiple_of(owners[u] * piece + halves[u] * hp, PAIR) for u in BOTH]

        slot = 2 * (g // 7)

        def load(u, slot, rows):
            return pltpu.make_async_copy(r_all.at[rows], buf.at[slot + u], lsem.at[slot + u])

        def loads():
            for u in BOTH:
                load(u, 0, pl.ds(offs[u], hp)).start()

        def partner():
            for mask in MASKS:
                pos_copy(mask, grid.xor(mask)).wait_recv()
            for u in BOTH:
                keep(2, gather_dy, u).wait()
            gather.arrived('own')
            loads()

        def far():
            gather.third()
            gather_dy.begin()
            loads()
            gather.arrived('cdA', 'cdB')
            for u in BOTH:
                load(u, 2, block(2 * grid.xor(7) + u, hp)).start()

        def then_load(event, *names):
            def run():
                event(*names)
                loads()

            return run

        events = (
            partner, then_load(gather.first), then_load(gather.arrived, 'cxA', 'cyB'),
            then_load(gather.second), then_load(gather.arrived, 'cxB', 'cyA'), far,
        )
        for number, event in enumerate(events):
            pl.when(g == number + 1)(event)

        for u in BOTH:
            cols = pl.ds(offs[u], hp)

            @pl.when(g > 0)
            def _():
                load(u, slot, cols).wait()
                for copy in stores(u, cols):
                    copy.wait()

            angles = inv * pos_scr[2 * owners[u] + halves[u]].astype(F32)
            cos = jnp.cos(angles) * MSCALE
            sin = jnp.sin(angles) * MSCALE
            cos_st[u] = cos
            sin_st[u] = sin

            def rope(t):
                t1, t2 = t[:HALF], t[HALF:]
                return stack([t1 * cos - t2 * sin, t2 * cos + t1 * sin]).astype(BF16)

            qkv = dot_nt(w_scr[...], buf[slot + u])
            for h in range(HEADS):
                q = rope(qkv[span(h, HD)]) * BF16(0.125)
                q_st[u, span(h, HD)] = q
                qz_scr[h, span(h % 2, HD), cols] = q
                k_st[u, span(h, HD)] = rope(qkv[span(HEADS + h, HD)])
            kn_scr[cols, :] = k_st[u].T
            v_scr[:, cols] = qkv[2 * WIDTH:].astype(BF16)
            for copy in stores(u, cols):
                copy.start()
        return carry

    lax.fori_loop(0, NDEV, group, 0)
    for u in BOTH:
        for copy in stores(u, block(u, hp)):
            copy.wait()
    v_out = pltpu.make_async_copy(v_scr, v_hbm, fsem.at[0])
    v_out.start()

    bufs = ((s_scr0, s_scr1), (s_scr2, s_scr3))

    def at(i):
        return block(i, BLK)

    def two_heads(pair):
        return block(pair, PAIR)

    def outputs(pair):
        rows = block(pair, ROWS)
        return [
            pltpu.make_async_copy(o_scr.at[two_heads(pair)], o_hbm.at[two_heads(pair)], fsem.at[1]),
            pltpu.make_async_copy(on_scr.at[:, two_heads(pair)], on_hbm.at[:, two_heads(pair)], fsem.at[2]),
            pltpu.make_async_copy(lse_scr.at[rows], lse_hbm.at[rows], fsem.at[3]),
        ]

    def forward(pair, carry):
        m_scr[...] = jnp.full_like(m_scr, MASK_VALUE)
        clear(l_scr)

        def score(i, j, b, h, masked):
            s = dot_nn(kn_scr[at(j), two_heads(pair)], qz_scr[2 * pair + h, :, at(i)])
            if masked:
                krow = lax.broadcasted_iota(jnp.int32, s.shape, 0)
                qcol = lax.broadcasted_iota(jnp.int32, s.shape, 1)
                s = jnp.where(krow <= qcol, s, MASK_VALUE)
            bufs[b][h][...] = s
            row = 2 * b + h
            mx_scr[span(row, 1), :] = jnp.max(s, axis=0, keepdims=True)

        def weigh(i, j, b, h):
            row = span(h, 1)
            m_old = m_scr[row, at(i)]
            m_new = jnp.maximum(m_old, mx_scr[span(2 * b + h, 1), :])
            m_scr[row, at(i)] = m_new
            alpha = jnp.exp2((m_old - m_new) * LOG2E)
            p = jnp.exp2((bufs[b][h][...] - m_new) * LOG2E)
            l_scr[row, at(i)] = l_scr[row, at(i)] * alpha + column_sum(p)
            v = v_scr[pl.ds(pl.multiple_of((2 * pair + h) * HD, HD), HD), at(j)]
            acc_scr[h, :, at(i)] = acc_scr[h, :, at(i)] * alpha + dot_nn(v, p.astype(BF16))

        def both(later, now, b, masked):
            for h in BOTH:
                score(*later, 1 - b, h, masked)
                weigh(*now, b, h)

        for h in BOTH:
            score(0, 0, 0, h, True)

        def diagonal(t, carry):
            i = 2 * t
            both((i + 1, i + 1), (i, i), 0, True)
            e = jnp.minimum(i + 2, nblk - 1)
            both((e, e), (i + 1, i + 1), 1, True)
            return carry

        lax.fori_loop(0, nblk // 2, diagonal, 0)

        def following(i, j):
            wrap = (j + 1) // i
            return i + wrap, (j + 1) * (1 - wrap)

        for h in BOTH:
            score(1, 0, 0, h, False)

        def below(t, carry):
            i, j = carry
            i1, j1 = following(i, j)
            both((i1, j1), (i, j), 0, False)
            i2, j2 = following(i1, j1)
            both((jnp.minimum(i2, nblk - 1), j2), (i1, j1), 1, False)
            return i2, j2

        def segment(g, carry):
            @pl.when((pair == 0) & (g == 1))
            def _():
                gather_dy.first()

            @pl.when((pair == 1) & (g == 0))
            def _():
                gather_dy.second()

            @pl.when((pair == 1) & (g == 2))
            def _():
                gather_dy.third()
                for copy in outputs(0):
                    copy.wait()
                for mask in MASKS:
                    o_copy(mask, grid.me).start()

            a, b, c = SEGMENTS
            start = jnp.where(g == 0, 0, jnp.where(g == 1, a, b))
            stop = jnp.where(g == 0, a, jnp.where(g == 1, b, c))
            return lax.fori_loop(start, stop, below, carry)

        lax.fori_loop(0, len(SEGMENTS), segment, (jnp.int32(1), jnp.int32(0)))

        def finish(i, carry):
            outs = []
            for h in BOTH:
                l = l_scr[span(h, 1), at(i)]
                outs.append((acc_scr[h, :, at(i)] / l).astype(BF16))
                lse_scr[pl.ds(pair * ROWS + h, 1), at(i)] = m_scr[span(h, 1), at(i)] + jnp.log(l)
            o = stack(outs)
            o_scr[two_heads(pair), at(i)] = o
            on_scr[at(i), two_heads(pair)] = o.T
            return carry

        lax.fori_loop(0, nblk, finish, 0)
        for copy in outputs(pair):
            copy.start()
        return carry

    lax.fori_loop(0, 2, forward, 0)
    for copy in outputs(1):
        copy.wait()
    v_out.wait()
    gather.sent()
    gather_dy.last()
    for mask in MASKS:
        pos_copy(mask, grid.me).wait_send()
        o_copy(mask, grid.xor(mask)).wait_recv()
        o_copy(mask, grid.me).wait_send()


def front_call(x, gain, pos, inv_freq, w_qkv, dy):
    piece, hidden = x.shape
    seq = piece * NDEV
    hp = piece // 2
    hbm = pl.BlockSpec(memory_space=pl.ANY)
    vmem = pl.BlockSpec(memory_space=pltpu.VMEM)
    dma = pltpu.SemaphoreType.DMA
    all_b = lambda *shape: jax.ShapeDtypeStruct(shape, BF16)
    all_f = lambda *shape: jax.ShapeDtypeStruct(shape, F32)
    b = lambda *shape: pltpu.VMEM(shape, BF16)
    f = lambda *shape: pltpu.VMEM(shape, F32)
    tr = all_b(WIDTH, seq)
    tab = all_f(HALF, seq)
    return pl.pallas_call(
        front_kernel,
        out_shape=(all_b(seq, hidden), all_b(seq, hidden), tr, tr, tr, tab, tab, tr, all_b(seq, WIDTH), all_f(2 * ROWS, seq), all_b(NDEV, piece, PAIR)),
        in_specs=[hbm, vmem, vmem, vmem, hbm, hbm],
        out_specs=(hbm,) * 11,
        scratch_shapes=[
            b(3, hidden, WIDTH), b(3 * WIDTH, hidden), b(4, hp, hidden), pltpu.VMEM((2 * NDEV, 1, hp), jnp.int32),
            b(2, WIDTH, hp), b(2, WIDTH, hp), f(2, HALF, hp), f(2, HALF, hp), b(HEADS, PAIR, seq), b(seq, WIDTH), b(WIDTH, seq),
            f(2, HD, seq), f(ROWS, seq), f(ROWS, seq), f(BLK, BLK), f(BLK, BLK), f(BLK, BLK), f(BLK, BLK), f(ROWS, BLK),
            b(WIDTH, seq), b(seq, WIDTH), f(2 * ROWS, seq),
            dma((3,)), dma((4,)), dma((2, 4)), dma((4,)), dma((4,)), dma((NDEV,)), dma((NDEV,)), dma((NDEV,)), dma((NDEV,)),
        ] + GATHER_SEMS * 2,
        compiler_params=pltpu.CompilerParams(collective_id=0, has_side_effects=True, vmem_limit_bytes=VMEM_LIMIT),
        cost_estimate=cost(2 * seq * seq * WIDTH),
        name="front",
    )(x, gain, pos.reshape(2, 1, hp), inv_freq.reshape(HALF, 1), w_qkv, dy)


def split3(value):
    hi = value.astype(BF16).astype(F32)
    mid = (value - hi).astype(BF16).astype(F32)
    return hi, mid, value - hi - mid


FIRST, SECOND, THIRD = 6, 9, 2


def bwd_kernel(dy_ref, r_ref, q_ref, o_ref, k_ref, v_ref, lse_ref, cos_ref, sin_ref, w_hbm, on_hbm, x_hbm, o_first,
               y_hbm, o_recv, gwo_all, dn_recv, gw_all, gw_last,
               do_scr, w_scr, gwo_scr, qa_scr, doa_scr, ka_scr, va_scr, dq_scr, dk_scr, dv_scr, dn_scr, gw_scr, o_scr, x_scr, wc_scr, p_scr0, ds_scr0, p_scr1, ds_scr1,
               ysem, wsem, lsem, o_ssem, o_rsem, d_ssem, d_rsem, g_ssem, g_rsem):
    s = pl.program_id(0)
    nblk = do_scr.shape[1] // BLK
    grid = Grid()
    width, hidden = w_scr.shape
    piece = x_hbm.shape[0]
    row64 = lax.broadcasted_iota(jnp.int32, (HD, BLK), 0)

    def blk(t):
        return block(t, BLK)

    def o_copy(mask, owner):
        return exchange_o(grid, on_hbm, o_recv, 1, mask, owner, o_ssem, o_rsem)

    def dn_cols(owner):
        return pl.ds(pl.multiple_of(owner * piece, 128), piece)

    def dn_copy(h, mask, owner):
        src = dn_scr.at[h % 2, :, dn_cols(grid.xor(mask))]
        return pltpu.make_async_remote_copy(src, dn_recv.at[h, owner], d_ssem.at[h, mask], d_rsem.at[h, mask], device_id={'cp': grid.xor(mask)}, device_id_type=MESH)

    def dn_own(h):
        return pltpu.make_async_copy(dn_scr.at[h % 2, :, dn_cols(grid.me)], dn_recv.at[h, grid.me], lsem.at[0])

    def gw_own(h):
        return pltpu.make_async_copy(gw_scr.at[h % 2], gw_all.at[grid.me, h], lsem.at[1])

    def keep_last():
        return pltpu.make_async_copy(gw_scr.at[(HEADS - 1) % 2], gw_last, lsem.at[1])

    def gw_gather(h):
        half = 3 * HALF
        return Gather(grid, None, lambda owner, first, halves: gw_all.at[owner, h, pl.ds(first * half, halves * half)], lambda k: g_ssem.at[h, k], lambda k: g_rsem.at[h, k])

    def project_y():
        wide = wc_scr.shape[2]

        def chunk(c):
            return span(c, wide)

        def w_chunk(c):
            return pltpu.make_async_copy(w_hbm.at[:, chunk(c)], wc_scr.at[c % 2], ysem.at[c % 2])

        def o_part(src, owner, pair):
            cols = pl.ds(pl.multiple_of(owner * width + pair * PAIR, PAIR), PAIR)
            return pltpu.make_async_copy(src, o_scr.at[:, cols], ysem.at[2])

        parts = [pltpu.make_async_copy(x_hbm, x_scr, ysem.at[2])]
        for pair, recv in enumerate((o_first, o_recv)):
            parts += [o_part(recv.at[grid.xor(mask)], grid.xor(mask), pair) for mask in MASKS]
            parts.append(o_part(on_hbm.at[block(grid.me, piece), span(pair, PAIR)], grid.me, pair))
        w_chunk(0).start()
        for part in parts:
            part.start()
        for part in parts:
            part.wait()
        for c in range(hidden // wide):
            w_chunk(c).wait()
            if c + 1 < hidden // wide:
                w_chunk(c + 1).start()
            part = dot_nn(o_scr[...], wc_scr[c % 2])
            x_scr[:, chunk(c)] = (x_scr[:, chunk(c)].astype(F32) + part).astype(BF16)
        out = pltpu.make_async_copy(x_scr, y_hbm, ysem.at[2])
        out.start()
        out.wait()

    gwo_gather = row_gather(grid, None, gwo_all, width, g_ssem.at[HEADS], g_rsem.at[HEADS])

    @pl.when(s == 0)
    def _():
        w_copy = pltpu.make_async_copy(w_hbm.at[block(grid.me, width)], w_scr, wsem)
        w_copy.start()
        barrier(grid)
        for mask in MASKS:
            o_copy(mask, grid.me).start()
        w_copy.wait()
        clear(gwo_scr)

    @pl.when(s < nblk)
    def _():
        gwo_scr[...] += dot_nn(o_ref[:, blk(s)], dy_ref[...])
        do_scr[:, blk(s)] = dot_nt(w_scr[...], dy_ref[...]).astype(BF16)

    @pl.when(s == nblk)
    def _():
        own = pltpu.make_async_copy(gwo_scr, gwo_gather.dst(grid.me, 0, 2), lsem.at[1])
        own.start()
        own.wait()
        gwo_gather.begin()

    t = s - nblk
    h = t // nblk
    j = t % nblk

    def send_head(h):
        dn_own(h).start()
        for mask in MASKS:
            dn_copy(h, mask, grid.me).start()

    @pl.when((t >= nblk) & (j == 0))
    def _():
        send_head(h - 1)
        gw_own(h - 1).start()

    @pl.when((t >= nblk) & (j == 1))
    def _():
        gw_own(h - 1).wait()
        dn_own(h - 1).wait()
        gw_gather(h - 1).begin()

    @pl.when((t >= 2 * nblk) & (j == 0))
    def _():
        for mask in MASKS:
            dn_copy(h - 2, mask, grid.me).wait_send()

    @pl.when((t >= nblk) & (j == FIRST))
    def _():
        gw_gather(h - 1).first()

    @pl.when((t >= nblk) & (j == SECOND))
    def _():
        gw_gather(h - 1).second()

    @pl.when((t >= 2 * nblk) & (j == THIRD))
    def _():
        gw_gather(h - 2).third()

    @pl.when(t == 5)
    def _():
        gwo_gather.first()

    @pl.when(t == 8)
    def _():
        gwo_gather.second()

    @pl.when(t == nblk + THIRD)
    def _():
        gwo_gather.third()

    @pl.when(t >= 0)
    def _():
        rows = block(h, HD)

        @pl.when(j == 0)
        def _():
            clear(dq_scr)
            gw_scr[h % 2] = jnp.zeros(gw_scr.shape[1:], F32)

            def augment(data, stat):
                hi, mid, lo = split3(-stat)
                extra = jnp.where(row64 == 0, hi, jnp.where(row64 == 1, mid, jnp.where(row64 == 2, lo, 0.0))).astype(BF16)
                return stack([data, extra]).T

            def prep(i, carry):
                cols = blk(i)
                do_h = do_scr[rows, cols]
                delta = column_sum(do_h.astype(F32) * o_ref[rows, cols].astype(F32))
                qa_scr[cols, :] = augment(q_ref[rows, cols], lse_ref[pl.ds((h // 2) * ROWS + h % 2, 1), cols])
                doa_scr[cols, :] = augment(do_h, delta)
                return carry

            lax.fori_loop(0, nblk, prep, 0)

        ones = jnp.where(row64 < 3, 1.0, 0.0).astype(BF16)
        ka_scr[...] = stack([k_ref[rows, :], ones])
        va_scr[...] = stack([v_ref[rows, :], ones])
        clear(dk_scr)
        clear(dv_scr)

        bufs = (p_scr0, ds_scr0), (p_scr1, ds_scr1)

        def scores(i):
            return dot_nn(qa_scr[blk(i), :], ka_scr[...])

        def weights(s, i, b):
            p = jnp.exp2(s * LOG2E)
            bufs[b][0][...] = p.astype(BF16)
            return p

        def score_grads(p, i, b):
            bufs[b][1][...] = (p * dot_nn(doa_scr[blk(i), :], va_scr[...])).astype(BF16)

        def add_dv(i, b):
            dv_scr[...] += dot_nn(do_scr[rows, blk(i)], bufs[b][0][...])

        def add_dk(i, b):
            dk_scr[...] += dot_nn(q_ref[rows, blk(i)], bufs[b][1][...])

        def add_dq(i, b):
            dq_scr[:, blk(i)] += dot_nt(k_ref[rows, :], bufs[b][1][...])

        def both(later, now, b):
            s = scores(later)
            add_dv(now, b)
            p = weights(s, later, 1 - b)
            add_dk(now, b)
            score_grads(p, later, 1 - b)
            add_dq(now, b)

        first = scores(j)
        qrow = lax.broadcasted_iota(jnp.int32, first.shape, 0)
        kcol = lax.broadcasted_iota(jnp.int32, first.shape, 1)
        score_grads(weights(jnp.where(kcol <= qrow, first, MASK_VALUE), j, 0), j, 0)

        def body(u, carry):
            i = j + 2 * u
            both(i + 1, i, 0)
            both(jnp.minimum(i + 2, nblk - 1), i + 1, 1)
            return carry

        lax.fori_loop(0, (nblk - j) // 2, body, 0)

        @pl.when((nblk - j) % 2 == 1)
        def _():
            for add in (add_dv, add_dk, add_dq):
                add(nblk - 1, 0)

        cos = cos_ref[...]
        sin = sin_ref[...]

        def unrope(v, scale):
            v1 = v[:HALF] * scale
            v2 = v[HALF:] * scale
            return [v1 * cos + v2 * sin, v2 * cos - v1 * sin]

        grads = stack(unrope(dq_scr[:, blk(j)], 0.125) + unrope(dk_scr[...], 1.0) + [dv_scr[...]]).astype(BF16)
        dn_scr[h % 2, :, blk(j)] = grads
        gw_scr[h % 2] += dot_nn(grads, r_ref[...])

    @pl.when(s == pl.num_programs(0) - 1)
    def _():
        end = HEADS - 1
        keep_last().start()
        send_head(end)
        for mask in MASKS:
            o_copy(mask, grid.xor(mask)).wait_recv()
        project_y()
        gw_gather(end - 1).third()
        keep_last().wait()
        dn_own(end).wait()
        for mask in MASKS:
            o_copy(mask, grid.me).wait_send()
            for head in range(HEADS):
                dn_copy(head, mask, grid.xor(mask)).wait_recv()
            for head in range(HEADS - 2, HEADS):
                dn_copy(head, mask, grid.me).wait_send()
        gwo_gather.last()
        for head in range(end):
            gw_gather(head).last()


def bwd_call(dy_all, r_all, q_t, o_t, k_t, v_t, lse, cos_t, sin_t, w_out, o_n, x, o_first):
    seq, hidden = dy_all.shape
    width = q_t.shape[0]
    half = cos_t.shape[0]
    ndev = NDEV
    piece = seq // ndev
    nblk = seq // BLK
    hbm = pl.BlockSpec(memory_space=pl.ANY)
    whole = lambda *shape: pl.BlockSpec(shape, lambda s: (0, 0), pipeline_mode=pl.Buffered(1))
    cols = lambda rows: pl.BlockSpec((rows, BLK), lambda s: (0, lax.rem(s, nblk)))
    rblk = lambda s: jnp.where(s < nblk, 0, lax.rem(s, nblk))
    rows = 3 * HD
    dma = pltpu.SemaphoreType.DMA
    return pl.pallas_call(
        bwd_kernel,
        out_shape=(
            jax.ShapeDtypeStruct((piece, hidden), BF16),
            jax.ShapeDtypeStruct((ndev, piece, PAIR), BF16),
            jax.ShapeDtypeStruct((ndev * width, hidden), F32),
            jax.ShapeDtypeStruct((HEADS, ndev, rows, piece), BF16),
            jax.ShapeDtypeStruct((ndev, HEADS - 1, rows, hidden), F32),
            jax.ShapeDtypeStruct((rows, hidden), F32),
        ),
        grid=(nblk * (1 + HEADS),),
        in_specs=[
            pl.BlockSpec((BLK, hidden), lambda s: (jnp.minimum(s, nblk - 1), 0)),
            pl.BlockSpec((BLK, hidden), lambda s: (rblk(s), 0)),
            whole(width, seq), whole(width, seq),
            cols(width), cols(width),
            whole(2 * ROWS, seq),
            cols(half), cols(half),
            hbm, hbm, hbm, hbm,
        ],
        out_specs=(hbm,) * 6,
        scratch_shapes=[
            pltpu.VMEM((width, seq), BF16), pltpu.VMEM((width, hidden), BF16), pltpu.VMEM((width, hidden), F32),
            pltpu.VMEM((seq, PAIR), BF16), pltpu.VMEM((seq, PAIR), BF16),
            pltpu.VMEM((PAIR, BLK), BF16), pltpu.VMEM((PAIR, BLK), BF16),
            pltpu.VMEM((HD, seq), F32), pltpu.VMEM((HD, BLK), F32), pltpu.VMEM((HD, BLK), F32),
            pltpu.VMEM((2, rows, seq), BF16), pltpu.VMEM((2, rows, hidden), F32),
            pltpu.VMEM((piece, hidden), BF16), pltpu.VMEM((piece, hidden), BF16), pltpu.VMEM((2, hidden, BLK), BF16),
        ] + [pltpu.VMEM((BLK, BLK), BF16)] * 4 + [
            dma((3,)), dma, dma((2,)), dma((ndev,)), dma((ndev,)), dma((HEADS, ndev)), dma((HEADS, ndev)), dma((HEADS + 1, COPIES)), dma((HEADS + 1, COPIES)),
        ],
        compiler_params=params(1, collective_id=2, has_side_effects=True),
        cost_estimate=cost(5 * seq * seq * width),
        name="backward",
    )(dy_all, r_all, q_t, o_t, k_t, v_t, lse, cos_t, sin_t, w_out, o_n, x, o_first)


def flip_bits(m, d):
    return sum((m // k + d // k) % 2 * k for k in (1, 2, 4))


def write_columns(step, steps, rows_of, place_of, out, stage, sem):
    parts = sem.shape[1]
    lanes = stage.shape[2] // parts
    slot = step % 2

    def copies(slot):
        places = [place_of(k) for k in range(parts)]
        return [pltpu.make_async_copy(stage.at[slot, :, span(k, lanes)], out.at[rows, pl.ds(pl.multiple_of(col, PAIR), lanes)], sem.at[slot, k]) for k, (rows, col) in enumerate(places)]

    @pl.when(step >= 2)
    def _():
        for copy in copies(slot):
            copy.wait()

    for k in range(parts):
        stage[slot, :, span(k, lanes)] = rows_of(k).T
    for copy in copies(slot):
        copy.start()

    @pl.when(step == steps - 1)
    def _():
        for copy in copies(1 - slot) + copies(slot):
            copy.wait()


NEAR = lambda p, k: (1 - p) * k + p * (2 + 2 * k)
FAR = lambda p, k: (1 - p) * (3 + 2 * k) + p * (6 + k)


def place_call(dev, gw_all, last, g_wqkv, first, mask_of):
    _, known, rows, hidden = gw_all.shape
    heads = known - first
    lanes = (heads + 1) * HD
    groups = len(last) // 2
    flat = [part for parts in last for part in parts]

    def kernel(d_ref, *refs):
        w, p = pl.program_id(0), pl.program_id(1)
        known_refs, flat_refs, (_, out, stage, sem) = refs[:2], list(refs[2:2 + len(flat)]), refs[2 + len(flat):]
        ends = [beside([flat_refs.pop(0)[...] for _ in parts]) for parts in last]

        def rows_of(k):
            end = jnp.where(p == 0, ends[k], ends[k - 2])
            return stack([known_refs[k][0, h] for h in range(heads)] + [end])

        def place_of(k):
            return slice(None), (w * NDEV + flip_bits(mask_of(p, k), d_ref[0])) * WIDTH + first * HD

        write_columns(groups * w + p, groups * 3, rows_of, place_of, out, stage, sem)

    def known_spec(k):
        return pl.BlockSpec((1, heads, HD, hidden), lambda w, p, d: (flip_bits(mask_of(p, k), d[0]), first // heads, w, 0))

    hbm = pl.BlockSpec(memory_space=pl.ANY)
    operands = [gw_all, gw_all, *flat, g_wqkv]
    return pl.pallas_call(
        kernel,
        out_shape=jax.ShapeDtypeStruct(g_wqkv.shape, F32),
        grid_spec=pltpu.PrefetchScalarGridSpec(
            num_scalar_prefetch=1,
            grid=(3, groups),
            in_specs=[known_spec(0), known_spec(1)] + [pl.BlockSpec((HD, part.shape[1]), lambda w, p, d: (w, 0)) for part in flat] + [hbm],
            out_specs=hbm,
            scratch_shapes=[pltpu.VMEM((2, hidden, 2 * lanes), F32), pltpu.SemaphoreType.DMA((2, 2))],
        ),
        input_output_aliases={len(operands): 0},
        compiler_params=params(2),
        cost_estimate=cost(20e9),
        name="place",
    )(dev, *operands)


def dx_kernel(d_ref, dn_ref, wq_ref, wk_ref, wv_ref, x_ref, g_ref, dy_ref, wout_ref, y_ref, gw_ref, dx_out, gg_out, wout_out, y_out, gw_out, acc_scr, stage, sem):
    s = pl.program_id(0)
    steps = pl.num_programs(0)
    hidden = acc_scr.shape[0]
    rhs = stack([dn_ref[h, 0, span(w, HD)] for w in range(3) for h in range(HEADS)])
    part = dot_nn(beside([wq_ref[...], wk_ref[...], wv_ref[...]]), rhs)
    wout_out[...] = wout_ref[...]
    y_out[...] = y_ref[...]

    def rows_of(w):
        return stack([gw_ref[0, h, span(w, HD)] for h in BOTH])

    def place_of(w):
        cut = hidden // 2
        owner = flip_bits(FAR(s // 4, s // 2 % 2), d_ref[0])
        return pl.ds(pl.multiple_of(s % 2 * cut, cut), cut), (w * NDEV + owner) * WIDTH

    write_columns(s, steps, rows_of, place_of, gw_out, stage, sem)

    @pl.when(s == 0)
    def _():
        acc_scr[...] = part

    @pl.when(s > 0)
    def _():
        acc_scr[...] += part

    @pl.when(s == steps - 1)
    def _():
        gain = g_ref[...]
        clear(gg_out)

        def tokens(c, carry):
            some = block(c, PAIR)
            dn = acc_scr[:, some].T
            x = x_ref[some, :].astype(F32)
            inv = inverse_rms(x)
            x_hat = x * inv
            gg_out[...] += column_sum(dn * x_hat)
            d_hat = dn * gain
            mean = jnp.mean(d_hat * x_hat, axis=-1, keepdims=True)
            dx_out[some, :] = (dy_ref[some, :].astype(F32) + inv * (d_hat - x_hat * mean)).astype(BF16)
            return carry

        lax.fori_loop(0, x_ref.shape[0] // PAIR, tokens, 0)


def dx_call(dev, dn_recv, w_qkv, x, gain, dy, wout_all, y, gw_all):
    _, ndev, rows, piece = dn_recv.shape
    hidden = w_qkv.shape[0]
    zero = lambda s, d: (0, 0)
    wspec = lambda which: pl.BlockSpec((hidden, WIDTH), lambda s, d: (0, which * ndev + s))
    whole = lambda *shape: pl.BlockSpec(shape, zero, pipeline_mode=pl.Buffered(1))
    rowblk = lambda rows: pl.BlockSpec((rows // ndev, hidden), lambda s, d: (s, 0))
    return pl.pallas_call(
        dx_kernel,
        out_shape=(
            jax.ShapeDtypeStruct((piece, hidden), BF16), jax.ShapeDtypeStruct((1, hidden), F32),
            jax.ShapeDtypeStruct((hidden, hidden), F32), jax.ShapeDtypeStruct((piece, hidden), BF16), jax.ShapeDtypeStruct((hidden, 3 * hidden), F32),
        ),
        grid_spec=pltpu.PrefetchScalarGridSpec(
            num_scalar_prefetch=1,
            grid=(ndev,),
            in_specs=[
                pl.BlockSpec((HEADS, 1, rows, piece), lambda s, d: (0, s, 0, 0)), wspec(0), wspec(1), wspec(2),
                whole(piece, hidden), whole(1, hidden), whole(piece, hidden), rowblk(hidden), rowblk(piece),
                pl.BlockSpec((1, 2, rows, hidden // 2), lambda s, d: (flip_bits(FAR(s // 4, s // 2 % 2), d[0]), 0, 0, s % 2)),
            ],
            out_specs=(whole(piece, hidden), whole(1, hidden), rowblk(hidden), rowblk(piece), pl.BlockSpec(memory_space=pl.ANY)),
            scratch_shapes=[pltpu.VMEM((hidden, piece), F32), pltpu.VMEM((2, hidden // 2, 3 * PAIR), F32), pltpu.SemaphoreType.DMA((2, 3))],
        ),
        compiler_params=params(1),
        cost_estimate=cost(2 * piece * hidden * 3 * hidden),
        name="dx",
    )(dev, dn_recv, w_qkv, w_qkv, w_qkv, x, gain, dy, wout_all, y, gw_all)


def solution(mesh):
    ndev = mesh.shape['cp']

    def device_fn(x_in, positions, long_factor, norm_gain, w_qkv, w_out, grad_y):
        _, piece, hidden = x_in.shape
        seq = piece * ndev
        dev = lax.axis_index('cp').astype(jnp.int32).reshape(1)
        x = x_in[0]
        dy = grad_y[0]
        gain = norm_gain.reshape(1, hidden)
        half = long_factor.shape[0]
        exponent = jnp.arange(half, dtype=F32) * (1.0 / half)
        inv_freq = 1.0 / (long_factor * jnp.power(10000.0, exponent))
        r_all, dy_all, q_t, k_t, v_t, cos_t, sin_t, o_t, o_n, lse, o_first = front_call(x, gain, positions, inv_freq, w_qkv, dy)
        y_out, _, wout_all, dn_recv, gw_all, own = bwd_call(dy_all, r_all, q_t, o_t, k_t, v_t, lse, cos_t, sin_t, w_out, o_n, x, o_first)

        def swap(value, mask):
            return lax.ppermute(value, 'cp', [(i, i ^ mask) for i in range(ndev)])

        cut = hidden // 2
        from_x, from_y, from_c = swap(own, 2), swap(own, 4), swap(own, 1)
        grad_x, gain, g_wout, y_out, g_wqkv = dx_call(dev, dn_recv, w_qkv, x, gain, dy, wout_all, y_out, gw_all)
        from_x, from_y, from_c, gain, g_wqkv = lax.optimization_barrier((from_x, from_y, from_c, gain, g_wqkv))
        diag = swap(from_x[:, :cut], 4), swap(from_y[:, cut:], 2)
        from_cx, from_cy, gain_x = swap(from_x, 1), swap(from_y, 1), swap(gain, 2)
        g_wqkv = place_call(dev, gw_all, [(own,), (from_c,), (from_x,), (from_y,)], g_wqkv, 0, NEAR)
        diag, from_cx, from_cy, gain_x, g_wqkv = lax.optimization_barrier((diag, from_cx, from_cy, gain_x, g_wqkv))
        from_cd = [swap(part, 1) for part in diag]
        gain = gain + gain_x
        gain_y = swap(gain, 4)
        g_wqkv = place_call(dev, gw_all, [(from_cx,), (from_cy,)], g_wqkv, 2, FAR)
        from_cd, gain_y, g_wqkv = lax.optimization_barrier((from_cd, gain_y, g_wqkv))
        gain = gain + gain_y
        gain_c = swap(gain, 1)
        g_wqkv = place_call(dev, gw_all, [diag, from_cd], g_wqkv, 2, lambda p, k: FAR(1, k))
        g_gain = (gain + gain_c).reshape(hidden)
        return y_out[None], grad_x[None], g_gain, g_wqkv, g_wout

    seq_spec = P('dp', 'cp', None)
    return jax.shard_map(device_fn, mesh=mesh, in_specs=(seq_spec, P(('dp', 'cp')), P(None), P(None), P(None, None), P(None, None), seq_spec), out_specs=(seq_spec, seq_spec, P('dp'), P('dp', None), P('dp', None)), check_vma=False)
```

```python
import math
import jax
import jax.numpy as jnp
from jax import lax
from jax.experimental import pallas as pl
from jax.experimental.pallas import tpu as pltpu
from jax.sharding import PartitionSpec as P

NORM_EPS = 1e-5
MSCALE = math.sqrt(1.0 + math.log(32.0) / math.log(4096.0))
MASK_VALUE = -1e30
LOG2E = math.log2(math.e)
BF16 = jnp.bfloat16
F32 = jnp.float32
BLK = 512
VMEM_LIMIT = 60 * 2 ** 20
FLOPS_PER_BYTE = 1000
ROWS = 8
NDEV = 8
HEADS = 4
HD = 64
PAIR = 2 * HD
HALF = HD // 2
WIDTH = HEADS * HD
BOTH = range(2)


def dot_nn(a, b):
    return lax.dot_general(a, b, (((1,), (0,)), ((), ())), preferred_element_type=F32)


def dot_nt(a, b):
    return lax.dot_general(a, b, (((1,), (1,)), ((), ())), preferred_element_type=F32)


def inverse_rms(x):
    return lax.rsqrt(jnp.mean(x * x, axis=-1, keepdims=True) + NORM_EPS)


def params(n=1, **kw):
    return pltpu.CompilerParams(dimension_semantics=("arbitrary",) * n, vmem_limit_bytes=VMEM_LIMIT, **kw)


def cost(flops):
    return pl.CostEstimate(flops=int(flops), bytes_accessed=int(flops) // FLOPS_PER_BYTE, transcendentals=0)


def stack(parts):
    return jnp.concatenate(parts, axis=0)


def beside(parts):
    return jnp.concatenate(parts, axis=1)


def column_sum(x):
    return jnp.sum(x, axis=0, keepdims=True)


def span(i, size):
    return slice(i * size, (i + 1) * size)


def block(i, size):
    return pl.ds(pl.multiple_of(i * size, size), size)


def clear(ref):
    ref[...] = jnp.zeros_like(ref)


MESH = pl.DeviceIdType.MESH


class Grid:
    def __init__(self):
        self.me = lax.axis_index('cp')
        self.core = self.me % 2
        self.x = (self.me // 2) % 2
        self.y = self.me // 4

    def flip(self, yf, xf, cf):
        return ((self.y + yf) % 2) * 4 + ((self.x + xf) % 2) * 2 + (self.core + cf) % 2

    def xor(self, mask):
        return self.flip(mask // 4, (mask // 2) % 2, mask % 2)


def barrier(grid):
    sem = pltpu.get_barrier_semaphore()
    for mask in MASKS:
        pl.semaphore_signal(sem, inc=1, device_id={'cp': grid.xor(mask)}, device_id_type=MESH)
    pl.semaphore_wait(sem, len(MASKS))


class Gather:
    SENDS = {
        'xA': '0012', 'yB': '0114', 'xB': '0112', 'yA': '0014', 'own': '0021', 'dA': '2014', 'dB': '4112',
        'cxA': '2011', 'cyB': '4111', 'cxB': '2111', 'cyA': '4011', 'cdA': '6011', 'cdB': '6111',
    }
    ORDER = tuple(SENDS)

    def __init__(self, grid, src, dst, ssem, rsem, far=True):
        self.grid, self.src, self.dst, self.ssem, self.rsem, self.far = grid, src, dst, ssem, rsem, far

    def desc(self, name, arriving=False):
        mask, first, halves, target = map(int, self.SENDS[name])
        k = self.ORDER.index(name)
        dst = self.dst(self.grid.xor(mask ^ target if arriving else mask), first, halves)
        src = dst if (mask or arriving or self.src is None) else self.src(first, halves)
        return pltpu.make_async_remote_copy(src, dst, self.ssem(k), self.rsem(k), device_id={'cp': self.grid.xor(target)}, device_id_type=MESH)

    def send(self, *names):
        for name in names:
            self.desc(name).start()

    def arrived(self, *names):
        for name in names:
            self.desc(name, True).wait_recv()

    def begin(self):
        self.send('xA', 'yB', 'xB', 'yA', 'own')

    def first(self):
        self.arrived('xA', 'yB')
        if self.far:
            self.send('dA', 'dB')
        self.send('cxA', 'cyB')

    def second(self):
        self.arrived('xB', 'yA')
        self.send('cxB', 'cyA')

    def third(self):
        self.arrived('dA', 'dB')
        self.send('cdA', 'cdB')

    def last(self):
        self.arrived('own', 'cxA', 'cyB', 'cxB', 'cyA')
        if self.far:
            self.arrived('cdA', 'cdB')
        self.sent()

    def sent(self):
        for name in self.ORDER:
            if self.far or 'd' not in name:
                self.desc(name).wait_send()


def row_gather(grid, src, dst, piece, ssem, rsem):
    half = piece // 2

    def place(owner, first, halves):
        return dst.at[pl.ds(pl.multiple_of(owner * piece + first * half, half), halves * half)]

    own = None if src is None else lambda first, halves: src.at[pl.ds(first * half, halves * half)]
    return Gather(grid, own, place, lambda k: ssem.at[k], lambda k: rsem.at[k])


COPIES = len(Gather.ORDER)
GATHER_SEMS = [pltpu.SemaphoreType.DMA((COPIES,))] * 2


MASKS = range(1, NDEV)
SEGMENTS = 11, 27, 33


def exchange_o(grid, on_hbm, o_recv, pair, mask, owner, ssem, rsem):
    src = on_hbm.at[block(grid.xor(mask), o_recv.shape[1]), span(pair, PAIR)]
    return pltpu.make_async_remote_copy(src, o_recv.at[owner], ssem.at[mask], rsem.at[mask], device_id={'cp': grid.xor(mask)}, device_id_type=MESH)


def front_kernel(x_hbm, g_ref, pos_ref, inv_ref, w_hbm, dy_hbm,
                 r_all, dy_all, q_hbm, k_hbm, v_hbm, cos_hbm, sin_hbm, o_hbm, on_hbm, lse_hbm, o_recv,
                 wtmp, w_scr, buf, pos_scr, q_st, k_st, cos_st, sin_st, qz_scr, kn_scr, v_scr,
                 acc_scr, m_scr, l_scr, s_scr0, s_scr1, s_scr2, s_scr3, mx_scr, o_scr, on_scr, lse_scr,
                 wsem, lsem, osem, csem, fsem, pssem, prsem, o_ssem, o_rsem, ssem, rsem, dy_ssem, dy_rsem):
    grid = Grid()
    _, hp, hidden = buf.shape
    piece = 2 * hp
    nblk = qz_scr.shape[2] // BLK

    def w_copy(which):
        cols = pl.ds(pl.multiple_of((which * NDEV + grid.me) * WIDTH, WIDTH), WIDTH)
        return pltpu.make_async_copy(w_hbm.at[:, cols], wtmp.at[which], wsem.at[which])

    def pos_copy(mask, owner):
        return pltpu.make_async_remote_copy(pos_ref, pos_scr.at[owner], pssem.at[mask], prsem.at[mask], device_id={'cp': grid.xor(mask)}, device_id_type=MESH)

    def own_half(hbm, u):
        return pltpu.make_async_copy(hbm.at[block(u, hp)], buf.at[2 + u], lsem.at[2 + u])

    def keep(slot, gather, u):
        return pltpu.make_async_copy(buf.at[slot + u], gather.dst(grid.me, u, 1), csem.at[slot + u])

    def o_copy(mask, owner):
        return exchange_o(grid, on_hbm, o_recv, 0, mask, owner, o_ssem, o_rsem)

    gather = row_gather(grid, None, r_all, piece, ssem, rsem)
    gather_dy = row_gather(grid, dy_hbm, dy_all, piece, dy_ssem, dy_rsem)
    for u in BOTH:
        own_half(x_hbm, u).start()
    for which in range(3):
        w_copy(which).start()
    for u in BOTH:
        own_half(x_hbm, u).wait()

        def norm(c, carry):
            some = block(c, HD)
            x = buf[2 + u, some, :].astype(F32)
            buf[u, some, :] = (x * inverse_rms(x) * g_ref[...]).astype(BF16)
            return carry

        lax.fori_loop(0, hp // HD, norm, 0)
        keep(0, gather, u).start()
        own_half(dy_hbm, u).start()
    barrier(grid)
    for mask in MASKS:
        pos_copy(mask, grid.me).start()
    for u in BOTH:
        keep(0, gather, u).wait()
    gather.begin()
    pos_scr[grid.me] = pos_ref[...]
    clear(qz_scr)
    clear(acc_scr)
    for u in BOTH:
        own_half(dy_hbm, u).wait()
        keep(2, gather_dy, u).start()
    for which in range(3):
        w_copy(which).wait()
        w_scr[span(which, WIDTH)] = wtmp[which].T

    inv = inv_ref[...]

    def stores(u, cols):
        pairs = (q_st, q_hbm), (k_st, k_hbm), (cos_st, cos_hbm), (sin_st, sin_hbm)
        return [pltpu.make_async_copy(st.at[u], hbm.at[:, cols], osem.at[u, n]) for n, (st, hbm) in enumerate(pairs)]

    def group(g, carry):
        stage = g // 2
        one = (stage + 2) // 3
        two = stage // 3
        first = (stage // 2) * (1 - two)
        halves = first, 1 - first
        owners = grid.flip(two, one, g % 2), grid.flip(one, two, g % 2)
        offs = [pl.multiple_of(owners[u] * piece + halves[u] * hp, PAIR) for u in BOTH]

        slot = 2 * (g // 7)

        def load(u, slot, rows):
            return pltpu.make_async_copy(r_all.at[rows], buf.at[slot + u], lsem.at[slot + u])

        def loads():
            for u in BOTH:
                load(u, 0, pl.ds(offs[u], hp)).start()

        def partner():
            for mask in MASKS:
                pos_copy(mask, grid.xor(mask)).wait_recv()
            for u in BOTH:
                keep(2, gather_dy, u).wait()
            gather.arrived('own')
            loads()

        def far():
            gather.third()
            gather_dy.begin()
            loads()
            gather.arrived('cdA', 'cdB')
            for u in BOTH:
                load(u, 2, block(2 * grid.xor(7) + u, hp)).start()

        def then_load(event, *names):
            def run():
                event(*names)
                loads()

            return run

        events = (
            partner, then_load(gather.first), then_load(gather.arrived, 'cxA', 'cyB'),
            then_load(gather.second), then_load(gather.arrived, 'cxB', 'cyA'), far,
        )
        for number, event in enumerate(events):
            pl.when(g == number + 1)(event)

        for u in BOTH:
            cols = pl.ds(offs[u], hp)

            @pl.when(g > 0)
            def _():
                load(u, slot, cols).wait()
                for copy in stores(u, cols):
                    copy.wait()

            lines = hp // PAIR
            angles = beside([inv * pos_scr[owners[u], pl.ds(halves[u] * lines + i, 1), :].astype(F32) for i in range(lines)])
            cos = jnp.cos(angles) * MSCALE
            sin = jnp.sin(angles) * MSCALE
            cos_st[u] = cos
            sin_st[u] = sin

            def rope(t):
                t1, t2 = t[:HALF], t[HALF:]
                return stack([t1 * cos - t2 * sin, t2 * cos + t1 * sin]).astype(BF16)

            qkv = dot_nt(w_scr[...], buf[slot + u])
            for h in range(HEADS):
                q = rope(qkv[span(h, HD)]) * BF16(0.125)
                q_st[u, span(h, HD)] = q
                qz_scr[h, span(h % 2, HD), cols] = q
                k_st[u, span(h, HD)] = rope(qkv[span(HEADS + h, HD)])
            kn_scr[cols, :] = k_st[u].T
            v_scr[:, cols] = qkv[2 * WIDTH:].astype(BF16)
            for copy in stores(u, cols):
                copy.start()
        return carry

    lax.fori_loop(0, NDEV, group, 0)
    for u in BOTH:
        for copy in stores(u, block(u, hp)):
            copy.wait()
    v_out = pltpu.make_async_copy(v_scr, v_hbm, fsem.at[0])
    v_out.start()

    bufs = ((s_scr0, s_scr1), (s_scr2, s_scr3))

    def at(i):
        return block(i, BLK)

    def two_heads(pair):
        return block(pair, PAIR)

    def outputs(pair):
        rows = block(pair, ROWS)
        return [
            pltpu.make_async_copy(o_scr.at[two_heads(pair)], o_hbm.at[two_heads(pair)], fsem.at[1]),
            pltpu.make_async_copy(on_scr.at[:, two_heads(pair)], on_hbm.at[:, two_heads(pair)], fsem.at[2]),
            pltpu.make_async_copy(lse_scr.at[rows], lse_hbm.at[rows], fsem.at[3]),
        ]

    def forward(pair, carry):
        m_scr[...] = jnp.full_like(m_scr, MASK_VALUE)
        clear(l_scr)

        def score(i, j, b, h, masked):
            s = dot_nn(kn_scr[at(j), two_heads(pair)], qz_scr[2 * pair + h, :, at(i)])
            if masked:
                krow = lax.broadcasted_iota(jnp.int32, s.shape, 0)
                qcol = lax.broadcasted_iota(jnp.int32, s.shape, 1)
                s = jnp.where(krow <= qcol, s, MASK_VALUE)
            bufs[b][h][...] = s
            row = 2 * b + h
            mx_scr[span(row, 1), :] = jnp.max(s, axis=0, keepdims=True)

        def weigh(i, j, b, h):
            row = span(h, 1)
            m_old = m_scr[row, at(i)]
            m_new = jnp.maximum(m_old, mx_scr[span(2 * b + h, 1), :])
            m_scr[row, at(i)] = m_new
            alpha = jnp.exp2((m_old - m_new) * LOG2E)
            p = jnp.exp2((bufs[b][h][...] - m_new) * LOG2E)
            l_scr[row, at(i)] = l_scr[row, at(i)] * alpha + column_sum(p)
            v = v_scr[pl.ds(pl.multiple_of((2 * pair + h) * HD, HD), HD), at(j)]
            acc_scr[h, :, at(i)] = acc_scr[h, :, at(i)] * alpha + dot_nn(v, p.astype(BF16))

        def both(later, now, b, masked):
            for h in BOTH:
                score(*later, 1 - b, h, masked)
                weigh(*now, b, h)

        for h in BOTH:
            score(0, 0, 0, h, True)

        def diagonal(t, carry):
            i = 2 * t
            both((i + 1, i + 1), (i, i), 0, True)
            e = jnp.minimum(i + 2, nblk - 1)
            both((e, e), (i + 1, i + 1), 1, True)
            return carry

        lax.fori_loop(0, nblk // 2, diagonal, 0)

        def following(i, j):
            wrap = (j + 1) // i
            return i + wrap, (j + 1) * (1 - wrap)

        for h in BOTH:
            score(1, 0, 0, h, False)

        def below(t, carry):
            i, j = carry
            i1, j1 = following(i, j)
            both((i1, j1), (i, j), 0, False)
            i2, j2 = following(i1, j1)
            both((jnp.minimum(i2, nblk - 1), j2), (i1, j1), 1, False)
            return i2, j2

        def segment(g, carry):
            @pl.when((pair == 0) & (g == 1))
            def _():
                gather_dy.first()

            @pl.when((pair == 1) & (g == 0))
            def _():
                gather_dy.second()

            @pl.when((pair == 1) & (g == 2))
            def _():
                gather_dy.third()
                for copy in outputs(0):
                    copy.wait()
                for mask in MASKS:
                    o_copy(mask, grid.me).start()

            a, b, c = SEGMENTS
            start = jnp.where(g == 0, 0, jnp.where(g == 1, a, b))
            stop = jnp.where(g == 0, a, jnp.where(g == 1, b, c))
            return lax.fori_loop(start, stop, below, carry)

        lax.fori_loop(0, len(SEGMENTS), segment, (jnp.int32(1), jnp.int32(0)))

        def finish(i, carry):
            outs = []
            for h in BOTH:
                l = l_scr[span(h, 1), at(i)]
                outs.append((acc_scr[h, :, at(i)] / l).astype(BF16))
                lse_scr[pl.ds(pair * ROWS + h, 1), at(i)] = m_scr[span(h, 1), at(i)] + jnp.log(l)
            o = stack(outs)
            o_scr[two_heads(pair), at(i)] = o
            on_scr[at(i), two_heads(pair)] = o.T
            return carry

        lax.fori_loop(0, nblk, finish, 0)
        for copy in outputs(pair):
            copy.start()
        return carry

    lax.fori_loop(0, 2, forward, 0)
    for copy in outputs(1):
        copy.wait()
    v_out.wait()
    gather.sent()
    gather_dy.last()
    for mask in MASKS:
        pos_copy(mask, grid.me).wait_send()
        o_copy(mask, grid.xor(mask)).wait_recv()
        o_copy(mask, grid.me).wait_send()


def front_call(x, gain, pos, inv_freq, w_qkv, dy):
    piece, hidden = x.shape
    seq = piece * NDEV
    hp = piece // 2
    hbm = pl.BlockSpec(memory_space=pl.ANY)
    vmem = pl.BlockSpec(memory_space=pltpu.VMEM)
    dma = pltpu.SemaphoreType.DMA
    all_b = lambda *shape: jax.ShapeDtypeStruct(shape, BF16)
    all_f = lambda *shape: jax.ShapeDtypeStruct(shape, F32)
    b = lambda *shape: pltpu.VMEM(shape, BF16)
    f = lambda *shape: pltpu.VMEM(shape, F32)
    tr = all_b(WIDTH, seq)
    tab = all_f(HALF, seq)
    return pl.pallas_call(
        front_kernel,
        out_shape=(all_b(seq, hidden), all_b(seq, hidden), tr, tr, tr, tab, tab, tr, all_b(seq, WIDTH), all_f(2 * ROWS, seq), all_b(NDEV, piece, PAIR)),
        in_specs=[hbm, vmem, vmem, vmem, hbm, hbm],
        out_specs=(hbm,) * 11,
        scratch_shapes=[
            b(3, hidden, WIDTH), b(3 * WIDTH, hidden), b(4, hp, hidden), pltpu.VMEM((NDEV, piece // PAIR, PAIR), jnp.int32),
            b(2, WIDTH, hp), b(2, WIDTH, hp), f(2, HALF, hp), f(2, HALF, hp), b(HEADS, PAIR, seq), b(seq, WIDTH), b(WIDTH, seq),
            f(2, HD, seq), f(ROWS, seq), f(ROWS, seq), f(BLK, BLK), f(BLK, BLK), f(BLK, BLK), f(BLK, BLK), f(ROWS, BLK),
            b(WIDTH, seq), b(seq, WIDTH), f(2 * ROWS, seq),
            dma((3,)), dma((4,)), dma((2, 4)), dma((4,)), dma((4,)), dma((NDEV,)), dma((NDEV,)), dma((NDEV,)), dma((NDEV,)),
        ] + GATHER_SEMS * 2,
        compiler_params=pltpu.CompilerParams(collective_id=0, has_side_effects=True, vmem_limit_bytes=VMEM_LIMIT),
        cost_estimate=cost(2 * seq * seq * WIDTH),
        name="front",
    )(x, gain, pos.reshape(piece // PAIR, PAIR), inv_freq.reshape(HALF, 1), w_qkv, dy)


def split3(value):
    hi = value.astype(BF16).astype(F32)
    mid = (value - hi).astype(BF16).astype(F32)
    return hi, mid, value - hi - mid


FIRST, SECOND, THIRD = 6, 9, 2


def bwd_kernel(dy_ref, r_ref, q_ref, o_ref, k_ref, v_ref, lse_ref, cos_ref, sin_ref, w_hbm, on_hbm, x_hbm, o_first,
               y_hbm, o_recv, gwo_all, dn_recv, gw_all, gw_last,
               do_scr, w_scr, gwo_scr, qa_scr, doa_scr, ka_scr, va_scr, dq_scr, dk_scr, dv_scr, dn_scr, gw_scr, o_scr, x_scr, wc_scr, p_scr0, ds_scr0, p_scr1, ds_scr1,
               ysem, wsem, lsem, o_ssem, o_rsem, d_ssem, d_rsem, g_ssem, g_rsem):
    s = pl.program_id(0)
    nblk = do_scr.shape[1] // BLK
    grid = Grid()
    width, hidden = w_scr.shape
    piece = x_hbm.shape[0]
    row64 = lax.broadcasted_iota(jnp.int32, (HD, BLK), 0)

    def blk(t):
        return block(t, BLK)

    def o_copy(mask, owner):
        return exchange_o(grid, on_hbm, o_recv, 1, mask, owner, o_ssem, o_rsem)

    def dn_cols(owner):
        return pl.ds(pl.multiple_of(owner * piece, 128), piece)

    def dn_copy(h, mask, owner):
        src = dn_scr.at[h % 2, :, dn_cols(grid.xor(mask))]
        return pltpu.make_async_remote_copy(src, dn_recv.at[h, owner], d_ssem.at[h, mask], d_rsem.at[h, mask], device_id={'cp': grid.xor(mask)}, device_id_type=MESH)

    def dn_own(h):
        return pltpu.make_async_copy(dn_scr.at[h % 2, :, dn_cols(grid.me)], dn_recv.at[h, grid.me], lsem.at[0])

    def gw_own(h):
        return pltpu.make_async_copy(gw_scr.at[h % 2], gw_all.at[grid.me, h], lsem.at[1])

    def keep_last():
        return pltpu.make_async_copy(gw_scr.at[(HEADS - 1) % 2], gw_last, lsem.at[1])

    def gw_gather(h, far=True):
        half = hidden // 2
        return Gather(grid, None, lambda owner, first, halves: gw_all.at[owner, h, :, pl.ds(first * half, halves * half)], lambda k: g_ssem.at[h, k], lambda k: g_rsem.at[h, k], far)

    def project_y():
        wide = wc_scr.shape[2]

        def chunk(c):
            return span(c, wide)

        def w_chunk(c):
            return pltpu.make_async_copy(w_hbm.at[:, chunk(c)], wc_scr.at[c % 2], ysem.at[c % 2])

        def o_part(src, owner, pair):
            cols = pl.ds(pl.multiple_of(owner * width + pair * PAIR, PAIR), PAIR)
            return pltpu.make_async_copy(src, o_scr.at[:, cols], ysem.at[2])

        parts = [pltpu.make_async_copy(x_hbm, x_scr, ysem.at[2])]
        for pair, recv in enumerate((o_first, o_recv)):
            parts += [o_part(recv.at[grid.xor(mask)], grid.xor(mask), pair) for mask in MASKS]
            parts.append(o_part(on_hbm.at[block(grid.me, piece), span(pair, PAIR)], grid.me, pair))
        w_chunk(0).start()
        for part in parts:
            part.start()
        for part in parts:
            part.wait()
        for c in range(hidden // wide):
            w_chunk(c).wait()
            if c + 1 < hidden // wide:
                w_chunk(c + 1).start()
            part = dot_nn(o_scr[...], wc_scr[c % 2])
            x_scr[:, chunk(c)] = (x_scr[:, chunk(c)].astype(F32) + part).astype(BF16)
        out = pltpu.make_async_copy(x_scr, y_hbm, ysem.at[2])
        out.start()
        out.wait()

    gwo_gather = row_gather(grid, None, gwo_all, width, g_ssem.at[HEADS], g_rsem.at[HEADS])

    @pl.when(s == 0)
    def _():
        w_copy = pltpu.make_async_copy(w_hbm.at[block(grid.me, width)], w_scr, wsem)
        w_copy.start()
        barrier(grid)
        for mask in MASKS:
            o_copy(mask, grid.me).start()
        w_copy.wait()
        clear(gwo_scr)

    @pl.when(s < nblk)
    def _():
        gwo_scr[...] += dot_nn(o_ref[:, blk(s)], dy_ref[...])
        do_scr[:, blk(s)] = dot_nt(w_scr[...], dy_ref[...]).astype(BF16)

    @pl.when(s == nblk)
    def _():
        own = pltpu.make_async_copy(gwo_scr, gwo_gather.dst(grid.me, 0, 2), lsem.at[1])
        own.start()
        own.wait()
        gwo_gather.begin()

    t = s - nblk
    h = t // nblk
    j = t % nblk

    def send_head(h):
        dn_own(h).start()
        for mask in MASKS:
            dn_copy(h, mask, grid.me).start()

    @pl.when((t >= nblk) & (j == 0))
    def _():
        send_head(h - 1)
        gw_own(h - 1).start()

    @pl.when((t >= nblk) & (j == 1))
    def _():
        gw_own(h - 1).wait()
        dn_own(h - 1).wait()
        gw_gather(h - 1).begin()

    @pl.when((t >= 2 * nblk) & (j == 0))
    def _():
        for mask in MASKS:
            dn_copy(h - 2, mask, grid.me).wait_send()

    end = HEADS - 1

    @pl.when(t == 2 * nblk + 1)
    def _():
        for mask in MASKS:
            o_copy(mask, grid.xor(mask)).wait_recv()
        project_y()

    @pl.when((t >= nblk) & (h < end) & (j == FIRST))
    def _():
        gw_gather(h - 1).first()

    @pl.when((h == end) & (j == FIRST))
    def _():
        gw_gather(end - 1, False).first()

    @pl.when((t >= nblk) & (j == SECOND))
    def _():
        gw_gather(h - 1).second()

    @pl.when((t >= 2 * nblk) & (j == THIRD))
    def _():
        gw_gather(h - 2).third()

    @pl.when(t == 5)
    def _():
        gwo_gather.first()

    @pl.when(t == 8)
    def _():
        gwo_gather.second()

    @pl.when(t == nblk + THIRD)
    def _():
        gwo_gather.third()

    @pl.when(t >= 0)
    def _():
        rows = block(h, HD)

        @pl.when(j == 0)
        def _():
            clear(dq_scr)
            gw_scr[h % 2] = jnp.zeros(gw_scr.shape[1:], F32)

            def augment(data, stat):
                hi, mid, lo = split3(-stat)
                extra = jnp.where(row64 == 0, hi, jnp.where(row64 == 1, mid, jnp.where(row64 == 2, lo, 0.0))).astype(BF16)
                return stack([data, extra]).T

            def prep(i, carry):
                cols = blk(i)
                do_h = do_scr[rows, cols]
                delta = column_sum(do_h.astype(F32) * o_ref[rows, cols].astype(F32))
                qa_scr[cols, :] = augment(q_ref[rows, cols], lse_ref[pl.ds((h // 2) * ROWS + h % 2, 1), cols])
                doa_scr[cols, :] = augment(do_h, delta)
                return carry

            lax.fori_loop(0, nblk, prep, 0)

        ones = jnp.where(row64 < 3, 1.0, 0.0).astype(BF16)
        ka_scr[...] = stack([k_ref[rows, :], ones])
        va_scr[...] = stack([v_ref[rows, :], ones])
        clear(dk_scr)
        clear(dv_scr)

        bufs = (p_scr0, ds_scr0), (p_scr1, ds_scr1)

        def scores(i):
            return dot_nn(qa_scr[blk(i), :], ka_scr[...])

        def weights(s, i, b):
            p = jnp.exp2(s * LOG2E)
            bufs[b][0][...] = p.astype(BF16)
            return p

        def score_grads(p, i, b):
            bufs[b][1][...] = (p * dot_nn(doa_scr[blk(i), :], va_scr[...])).astype(BF16)

        def add_dv(i, b):
            dv_scr[...] += dot_nn(do_scr[rows, blk(i)], bufs[b][0][...])

        def add_dk(i, b):
            dk_scr[...] += dot_nn(q_ref[rows, blk(i)], bufs[b][1][...])

        def add_dq(i, b):
            dq_scr[:, blk(i)] += dot_nt(k_ref[rows, :], bufs[b][1][...])

        def both(later, now, b):
            s = scores(later)
            add_dv(now, b)
            p = weights(s, later, 1 - b)
            add_dk(now, b)
            score_grads(p, later, 1 - b)
            add_dq(now, b)

        first = scores(j)
        qrow = lax.broadcasted_iota(jnp.int32, first.shape, 0)
        kcol = lax.broadcasted_iota(jnp.int32, first.shape, 1)
        score_grads(weights(jnp.where(kcol <= qrow, first, MASK_VALUE), j, 0), j, 0)

        def body(u, carry):
            i = j + 2 * u
            both(i + 1, i, 0)
            both(jnp.minimum(i + 2, nblk - 1), i + 1, 1)
            return carry

        lax.fori_loop(0, (nblk - j) // 2, body, 0)

        @pl.when((nblk - j) % 2 == 1)
        def _():
            for add in (add_dv, add_dk, add_dq):
                add(nblk - 1, 0)

        cos = cos_ref[...]
        sin = sin_ref[...]

        def unrope(v, scale):
            v1 = v[:HALF] * scale
            v2 = v[HALF:] * scale
            return [v1 * cos + v2 * sin, v2 * cos - v1 * sin]

        grads = stack(unrope(dq_scr[:, blk(j)], 0.125) + unrope(dk_scr[...], 1.0) + [dv_scr[...]]).astype(BF16)
        dn_scr[h % 2, :, blk(j)] = grads
        gw_scr[h % 2] += dot_nn(grads, r_ref[...])

    @pl.when(s == pl.num_programs(0) - 1)
    def _():
        keep_last().start()
        send_head(end)
        keep_last().wait()
        dn_own(end).wait()
        for mask in MASKS:
            o_copy(mask, grid.me).wait_send()
            for head in range(HEADS):
                dn_copy(head, mask, grid.xor(mask)).wait_recv()
            for head in range(HEADS - 2, HEADS):
                dn_copy(head, mask, grid.me).wait_send()
        gwo_gather.last()
        for head in range(end):
            gw_gather(head, head < end - 1).last()


def bwd_call(dy_all, r_all, q_t, o_t, k_t, v_t, lse, cos_t, sin_t, w_out, o_n, x, o_first):
    seq, hidden = dy_all.shape
    width = q_t.shape[0]
    half = cos_t.shape[0]
    ndev = NDEV
    piece = seq // ndev
    nblk = seq // BLK
    hbm = pl.BlockSpec(memory_space=pl.ANY)
    whole = lambda *shape: pl.BlockSpec(shape, lambda s: (0, 0), pipeline_mode=pl.Buffered(1))
    cols = lambda rows: pl.BlockSpec((rows, BLK), lambda s: (0, lax.rem(s, nblk)))
    rblk = lambda s: jnp.where(s < nblk, 0, lax.rem(s, nblk))
    rows = 3 * HD
    dma = pltpu.SemaphoreType.DMA
    return pl.pallas_call(
        bwd_kernel,
        out_shape=(
            jax.ShapeDtypeStruct((piece, hidden), BF16),
            jax.ShapeDtypeStruct((ndev, piece, PAIR), BF16),
            jax.ShapeDtypeStruct((ndev * width, hidden), F32),
            jax.ShapeDtypeStruct((HEADS, ndev, rows, piece), BF16),
            jax.ShapeDtypeStruct((ndev, HEADS - 1, rows, hidden), F32),
            jax.ShapeDtypeStruct((rows, hidden), F32),
        ),
        grid=(nblk * (1 + HEADS),),
        in_specs=[
            pl.BlockSpec((BLK, hidden), lambda s: (jnp.minimum(s, nblk - 1), 0)),
            pl.BlockSpec((BLK, hidden), lambda s: (rblk(s), 0)),
            whole(width, seq), whole(width, seq),
            cols(width), cols(width),
            whole(2 * ROWS, seq),
            cols(half), cols(half),
            hbm, hbm, hbm, hbm,
        ],
        out_specs=(hbm,) * 6,
        scratch_shapes=[
            pltpu.VMEM((width, seq), BF16), pltpu.VMEM((width, hidden), BF16), pltpu.VMEM((width, hidden), F32),
            pltpu.VMEM((seq, PAIR), BF16), pltpu.VMEM((seq, PAIR), BF16),
            pltpu.VMEM((PAIR, BLK), BF16), pltpu.VMEM((PAIR, BLK), BF16),
            pltpu.VMEM((HD, seq), F32), pltpu.VMEM((HD, BLK), F32), pltpu.VMEM((HD, BLK), F32),
            pltpu.VMEM((2, rows, seq), BF16), pltpu.VMEM((2, rows, hidden), F32),
            pltpu.VMEM((piece, hidden), BF16), pltpu.VMEM((piece, hidden), BF16), pltpu.VMEM((2, hidden, BLK), BF16),
        ] + [pltpu.VMEM((BLK, BLK), BF16)] * 4 + [
            dma((3,)), dma, dma((2,)), dma((ndev,)), dma((ndev,)), dma((HEADS, ndev)), dma((HEADS, ndev)), dma((HEADS + 1, COPIES)), dma((HEADS + 1, COPIES)),
        ],
        compiler_params=params(1, collective_id=2, has_side_effects=True),
        cost_estimate=cost(5 * seq * seq * width),
        name="backward",
    )(dy_all, r_all, q_t, o_t, k_t, v_t, lse, cos_t, sin_t, w_out, o_n, x, o_first)


def flip_bits(m, d):
    return sum((m // k + d // k) % 2 * k for k in (1, 2, 4))


def write_columns(step, steps, rows_of, place_of, out, stage, sem):
    parts = sem.shape[1]
    lanes = stage.shape[2] // parts
    slot = step % 2

    def copies(slot):
        places = [place_of(k) for k in range(parts)]
        return [pltpu.make_async_copy(stage.at[slot, :, span(k, lanes)], out.at[rows, pl.ds(pl.multiple_of(col, PAIR), lanes)], sem.at[slot, k]) for k, (rows, col) in enumerate(places)]

    @pl.when(step >= 2)
    def _():
        for copy in copies(slot):
            copy.wait()

    for k in range(parts):
        stage[slot, :, span(k, lanes)] = rows_of(k).T
    for copy in copies(slot):
        copy.start()

    @pl.when(step == steps - 1)
    def _():
        for copy in copies(1 - slot) + copies(slot):
            copy.wait()


NEAR = lambda p, k: (1 - p) * k + p * (2 + 2 * k)
FAR = lambda p, k: (1 - p) * (3 + 2 * k) + p * (6 + k)


def place_call(dev, gw_all, last, g_wqkv, first, mask_of, third=()):
    _, known, rows, hidden = gw_all.shape
    heads = known - first
    lanes = (heads + 1) * HD
    groups = len(last) // 2
    flat = [part for parts in (*last, *third) for part in parts]

    def kernel(d_ref, *refs):
        w, p = pl.program_id(0), pl.program_id(1)
        known_refs, flat_refs, (_, out, stage, sem) = refs[:2], list(refs[2:2 + len(flat)]), refs[2 + len(flat):]
        ends = [beside([flat_refs.pop(0)[...] for _ in parts]) for parts in (*last, *third)]

        def rows_of(k):
            end = jnp.where(p == 0, ends[k], ends[k - 2])
            rows = [ends[k + 2]] if third else [known_refs[k][0, h] for h in range(heads)]
            return stack(rows + [end])

        def place_of(k):
            return slice(None), (w * NDEV + flip_bits(mask_of(p, k), d_ref[0])) * WIDTH + first * HD

        write_columns(groups * w + p, groups * 3, rows_of, place_of, out, stage, sem)

    def known_spec(k):
        return pl.BlockSpec((1, heads, HD, hidden), lambda w, p, d: (flip_bits(mask_of(p, k), d[0]), first // heads, w, 0))

    hbm = pl.BlockSpec(memory_space=pl.ANY)
    operands = [gw_all, gw_all, *flat, g_wqkv]
    return pl.pallas_call(
        kernel,
        out_shape=jax.ShapeDtypeStruct(g_wqkv.shape, F32),
        grid_spec=pltpu.PrefetchScalarGridSpec(
            num_scalar_prefetch=1,
            grid=(3, groups),
            in_specs=[known_spec(0), known_spec(1)] + [pl.BlockSpec((HD, part.shape[1]), lambda w, p, d: (w, 0)) for part in flat] + [hbm],
            out_specs=hbm,
            scratch_shapes=[pltpu.VMEM((2, hidden, 2 * lanes), F32), pltpu.SemaphoreType.DMA((2, 2))],
        ),
        input_output_aliases={len(operands): 0},
        compiler_params=params(2),
        cost_estimate=cost(20e9),
        name="place",
    )(dev, *operands)


def dx_kernel(d_ref, dn_ref, wq_ref, wk_ref, wv_ref, x_ref, g_ref, dy_ref, wout_ref, y_ref, gw_ref, dx_out, gg_out, wout_out, y_out, gw_out, acc_scr, stage, sem):
    s = pl.program_id(0)
    steps = pl.num_programs(0)
    hidden = acc_scr.shape[0]
    rhs = stack([dn_ref[h, 0, span(w, HD)] for w in range(3) for h in range(HEADS)])
    part = dot_nn(beside([wq_ref[...], wk_ref[...], wv_ref[...]]), rhs)
    wout_out[...] = wout_ref[...]
    y_out[...] = y_ref[...]

    def rows_of(w):
        return stack([gw_ref[0, h, span(w, HD)] for h in BOTH])

    def place_of(w):
        cut = hidden // 2
        owner = flip_bits(FAR(s // 4, s // 2 % 2), d_ref[0])
        return pl.ds(pl.multiple_of(s % 2 * cut, cut), cut), (w * NDEV + owner) * WIDTH

    write_columns(s, steps, rows_of, place_of, gw_out, stage, sem)

    @pl.when(s == 0)
    def _():
        acc_scr[...] = part

    @pl.when(s > 0)
    def _():
        acc_scr[...] += part

    @pl.when(s == steps - 1)
    def _():
        gain = g_ref[...]
        clear(gg_out)

        def tokens(c, carry):
            some = block(c, PAIR)
            dn = acc_scr[:, some].T
            x = x_ref[some, :].astype(F32)
            inv = inverse_rms(x)
            x_hat = x * inv
            gg_out[...] += column_sum(dn * x_hat)
            d_hat = dn * gain
            mean = jnp.mean(d_hat * x_hat, axis=-1, keepdims=True)
            dx_out[some, :] = (dy_ref[some, :].astype(F32) + inv * (d_hat - x_hat * mean)).astype(BF16)
            return carry

        lax.fori_loop(0, x_ref.shape[0] // PAIR, tokens, 0)


def dx_call(dev, dn_recv, w_qkv, x, gain, dy, wout_all, y, gw_all):
    _, ndev, rows, piece = dn_recv.shape
    hidden = w_qkv.shape[0]
    zero = lambda s, d: (0, 0)
    wspec = lambda which: pl.BlockSpec((hidden, WIDTH), lambda s, d: (0, which * ndev + s))
    whole = lambda *shape: pl.BlockSpec(shape, zero, pipeline_mode=pl.Buffered(1))
    rowblk = lambda rows: pl.BlockSpec((rows // ndev, hidden), lambda s, d: (s, 0))
    return pl.pallas_call(
        dx_kernel,
        out_shape=(
            jax.ShapeDtypeStruct((piece, hidden), BF16), jax.ShapeDtypeStruct((1, hidden), F32),
            jax.ShapeDtypeStruct((hidden, hidden), F32), jax.ShapeDtypeStruct((piece, hidden), BF16), jax.ShapeDtypeStruct((hidden, 3 * hidden), F32),
        ),
        grid_spec=pltpu.PrefetchScalarGridSpec(
            num_scalar_prefetch=1,
            grid=(ndev,),
            in_specs=[
                pl.BlockSpec((HEADS, 1, rows, piece), lambda s, d: (0, s, 0, 0)), wspec(0), wspec(1), wspec(2),
                whole(piece, hidden), whole(1, hidden), whole(piece, hidden), rowblk(hidden), rowblk(piece),
                pl.BlockSpec((1, 2, rows, hidden // 2), lambda s, d: (flip_bits(FAR(s // 4, s // 2 % 2), d[0]), 0, 0, s % 2)),
            ],
            out_specs=(whole(piece, hidden), whole(1, hidden), rowblk(hidden), rowblk(piece), pl.BlockSpec(memory_space=pl.ANY)),
            scratch_shapes=[pltpu.VMEM((hidden, piece), F32), pltpu.VMEM((2, hidden // 2, 3 * PAIR), F32), pltpu.SemaphoreType.DMA((2, 3))],
        ),
        compiler_params=params(1),
        cost_estimate=cost(2 * piece * hidden * 3 * hidden),
        name="dx",
    )(dev, dn_recv, w_qkv, w_qkv, w_qkv, x, gain, dy, wout_all, y, gw_all)


def solution(mesh):
    ndev = mesh.shape['cp']

    def device_fn(x_in, positions, long_factor, norm_gain, w_qkv, w_out, grad_y):
        _, piece, hidden = x_in.shape
        seq = piece * ndev
        dev = lax.axis_index('cp').astype(jnp.int32).reshape(1)
        x = x_in[0]
        dy = grad_y[0]
        gain = norm_gain.reshape(1, hidden)
        half = long_factor.shape[0]
        exponent = jnp.arange(half, dtype=F32) * (1.0 / half)
        inv_freq = 1.0 / (long_factor * jnp.power(10000.0, exponent))
        r_all, dy_all, q_t, k_t, v_t, cos_t, sin_t, o_t, o_n, lse, o_first = front_call(x, gain, positions, inv_freq, w_qkv, dy)
        y_out, _, wout_all, dn_recv, gw_all, own = bwd_call(dy_all, r_all, q_t, o_t, k_t, v_t, lse, cos_t, sin_t, w_out, o_n, x, o_first)

        def swap(value, mask):
            return lax.ppermute(value, 'cp', [(i, i ^ mask) for i in range(ndev)])

        cut = hidden // 2

        def third_of(mask, start):
            some = lax.dynamic_slice(gw_all, (dev[0] ^ mask, HEADS - 2, 0, start), (1, 1, own.shape[0], cut))
            return some.reshape(own.shape[0], cut)

        third = swap(third_of(2, 0), 4), swap(third_of(4, cut), 2)
        from_x, from_y, from_c = swap(own, 2), swap(own, 4), swap(own, 1)
        grad_x, gain, g_wout, y_out, g_wqkv = dx_call(dev, dn_recv, w_qkv, x, gain, dy, wout_all, y_out, gw_all)
        third, from_x, from_y, from_c, gain, g_wqkv = lax.optimization_barrier((third, from_x, from_y, from_c, gain, g_wqkv))
        third_c = [swap(part, 1) for part in third]
        diag = swap(from_x[:, :cut], 4), swap(from_y[:, cut:], 2)
        from_cx, from_cy, gain_x = swap(from_x, 1), swap(from_y, 1), swap(gain, 2)
        g_wqkv = place_call(dev, gw_all, [(own,), (from_c,), (from_x,), (from_y,)], g_wqkv, 0, NEAR)
        diag, third_c, from_cx, from_cy, gain_x, g_wqkv = lax.optimization_barrier((diag, third_c, from_cx, from_cy, gain_x, g_wqkv))
        from_cd = [swap(part, 1) for part in diag]
        gain = gain + gain_x
        gain_y = swap(gain, 4)
        g_wqkv = place_call(dev, gw_all, [(from_cx,), (from_cy,)], g_wqkv, 2, FAR)
        from_cd, gain_y, g_wqkv = lax.optimization_barrier((from_cd, gain_y, g_wqkv))
        gain = gain + gain_y
        gain_c = swap(gain, 1)
        g_wqkv = place_call(dev, gw_all, [diag, from_cd], g_wqkv, 2, lambda p, k: FAR(1, k), [third, third_c])
        g_gain = (gain + gain_c).reshape(hidden)
        return y_out[None], grad_x[None], g_gain, g_wqkv, g_wout

    seq_spec = P('dp', 'cp')
    return jax.shard_map(device_fn, mesh=mesh, in_specs=(seq_spec, P(('dp', 'cp')), P(), P(), P(), P(), seq_spec), out_specs=(seq_spec, seq_spec, P('dp'), P('dp'), P('dp')), check_vma=False)
```

```python
import math
import jax
import jax.numpy as jnp
from jax import lax
from jax.experimental import pallas as pl
from jax.experimental.pallas import tpu as pltpu
from jax.sharding import PartitionSpec as P

NORM_EPS = 1e-5
MSCALE = math.sqrt(1.0 + math.log(32.0) / math.log(4096.0))
MASK_VALUE = -1e30
LOG2E = math.log2(math.e)
BF16 = jnp.bfloat16
F32 = jnp.float32
BLK = 512
VMEM_LIMIT = 60 * 2 ** 20
FLOPS_PER_BYTE = 1000
ROWS = 8
NDEV = 8
HEADS = 4
HD = 64
PAIR = 2 * HD
HALF = HD // 2
WIDTH = HEADS * HD
BOTH = range(2)


def dot_nn(a, b):
    return lax.dot_general(a, b, (((1,), (0,)), ((), ())), preferred_element_type=F32)


def dot_nt(a, b):
    return lax.dot_general(a, b, (((1,), (1,)), ((), ())), preferred_element_type=F32)


def inverse_rms(x):
    return lax.rsqrt(jnp.mean(x * x, axis=-1, keepdims=True) + NORM_EPS)


def params(n=1, **kw):
    return pltpu.CompilerParams(dimension_semantics=("arbitrary",) * n, vmem_limit_bytes=VMEM_LIMIT, **kw)


def cost(flops):
    return pl.CostEstimate(flops=int(flops), bytes_accessed=int(flops) // FLOPS_PER_BYTE, transcendentals=0)


def stack(parts):
    return jnp.concatenate(parts, axis=0)


def beside(parts):
    return jnp.concatenate(parts, axis=1)


def column_sum(x):
    return jnp.sum(x, axis=0, keepdims=True)


def span(i, size):
    return slice(i * size, (i + 1) * size)


def block(i, size):
    return pl.ds(pl.multiple_of(i * size, size), size)


def clear(ref):
    ref[...] = jnp.zeros_like(ref)


MESH = pl.DeviceIdType.MESH


class Grid:
    def __init__(self):
        self.me = lax.axis_index('cp')
        self.core = self.me % 2
        self.x = (self.me // 2) % 2
        self.y = self.me // 4

    def flip(self, yf, xf, cf):
        return ((self.y + yf) % 2) * 4 + ((self.x + xf) % 2) * 2 + (self.core + cf) % 2

    def xor(self, mask):
        return self.flip(mask // 4, (mask // 2) % 2, mask % 2)


def barrier(grid):
    sem = pltpu.get_barrier_semaphore()
    for mask in MASKS:
        pl.semaphore_signal(sem, inc=1, device_id={'cp': grid.xor(mask)}, device_id_type=MESH)
    pl.semaphore_wait(sem, len(MASKS))


class Gather:
    SENDS = {
        'xA': '0012', 'yB': '0114', 'xB': '0112', 'yA': '0014', 'own': '0021', 'dA': '2014', 'dB': '4112',
        'cxA': '2011', 'cyB': '4111', 'cxB': '2111', 'cyA': '4011', 'cdA': '6011', 'cdB': '6111',
    }
    ORDER = tuple(SENDS)

    def __init__(self, grid, src, dst, ssem, rsem, far=True):
        self.grid, self.src, self.dst, self.ssem, self.rsem, self.far = grid, src, dst, ssem, rsem, far

    def desc(self, name, arriving=False):
        mask, first, halves, target = map(int, self.SENDS[name])
        k = self.ORDER.index(name)
        dst = self.dst(self.grid.xor(mask ^ target if arriving else mask), first, halves)
        src = dst if (mask or arriving or self.src is None) else self.src(first, halves)
        return pltpu.make_async_remote_copy(src, dst, self.ssem(k), self.rsem(k), device_id={'cp': self.grid.xor(target)}, device_id_type=MESH)

    def send(self, *names):
        for name in names:
            self.desc(name).start()

    def arrived(self, *names):
        for name in names:
            self.desc(name, True).wait_recv()

    def begin(self):
        self.send('xA', 'yB', 'xB', 'yA', 'own')

    def first(self):
        self.arrived('xA', 'yB')
        if self.far:
            self.send('dA', 'dB')
        self.send('cxA', 'cyB')

    def second(self):
        self.arrived('xB', 'yA')
        self.send('cxB', 'cyA')

    def third(self):
        self.arrived('dA', 'dB')
        self.send('cdA', 'cdB')

    def last(self):
        self.arrived('own', 'cxA', 'cyB', 'cxB', 'cyA')
        if self.far:
            self.arrived('cdA', 'cdB')
        self.sent()

    def sent(self):
        for name in self.ORDER:
            if self.far or 'd' not in name:
                self.desc(name).wait_send()


def row_gather(grid, src, dst, piece, ssem, rsem):
    half = piece // 2

    def place(owner, first, halves):
        return dst.at[pl.ds(pl.multiple_of(owner * piece + first * half, half), halves * half)]

    own = None if src is None else lambda first, halves: src.at[pl.ds(first * half, halves * half)]
    return Gather(grid, own, place, lambda k: ssem.at[k], lambda k: rsem.at[k])


COPIES = len(Gather.ORDER)
GATHER_SEMS = [pltpu.SemaphoreType.DMA((COPIES,))] * 2


MASKS = range(1, NDEV)
SEGMENTS = 11, 27, 33


def exchange_o(grid, on_hbm, o_recv, pair, mask, owner, ssem, rsem):
    src = on_hbm.at[block(grid.xor(mask), o_recv.shape[1]), span(pair, PAIR)]
    return pltpu.make_async_remote_copy(src, o_recv.at[owner], ssem.at[mask], rsem.at[mask], device_id={'cp': grid.xor(mask)}, device_id_type=MESH)


def front_kernel(x_hbm, g_ref, pos_ref, inv_ref, w_hbm, dy_hbm,
                 r_all, dy_all, q_hbm, k_hbm, v_hbm, cos_hbm, sin_hbm, o_hbm, on_hbm, lse_hbm, o_recv,
                 wtmp, w_scr, buf, pos_scr, q_st, k_st, cos_st, sin_st, qz_scr, kn_scr, v_scr,
                 acc_scr, m_scr, l_scr, s_scr0, s_scr1, s_scr2, s_scr3, mx_scr, o_scr, on_scr, lse_scr,
                 wsem, lsem, osem, csem, fsem, pssem, prsem, o_ssem, o_rsem, ssem, rsem, dy_ssem, dy_rsem):
    grid = Grid()
    _, hp, hidden = buf.shape
    piece = 2 * hp
    nblk = qz_scr.shape[2] // BLK

    def w_copy(which):
        cols = pl.ds(pl.multiple_of((which * NDEV + grid.me) * WIDTH, WIDTH), WIDTH)
        return pltpu.make_async_copy(w_hbm.at[:, cols], wtmp.at[which], wsem.at[which])

    def pos_copy(mask, owner):
        return pltpu.make_async_remote_copy(pos_ref, pos_scr.at[owner], pssem.at[mask], prsem.at[mask], device_id={'cp': grid.xor(mask)}, device_id_type=MESH)

    def own_half(hbm, u):
        return pltpu.make_async_copy(hbm.at[block(u, hp)], buf.at[2 + u], lsem.at[2 + u])

    def keep(slot, gather, u):
        return pltpu.make_async_copy(buf.at[slot + u], gather.dst(grid.me, u, 1), csem.at[slot + u])

    def o_copy(mask, owner):
        return exchange_o(grid, on_hbm, o_recv, 0, mask, owner, o_ssem, o_rsem)

    gather = row_gather(grid, None, r_all, piece, ssem, rsem)
    gather_dy = row_gather(grid, dy_hbm, dy_all, piece, dy_ssem, dy_rsem)
    for u in BOTH:
        own_half(x_hbm, u).start()
    for which in range(3):
        w_copy(which).start()
    for u in BOTH:
        own_half(x_hbm, u).wait()

        def norm(c, carry):
            some = block(c, HD)
            x = buf[2 + u, some, :].astype(F32)
            buf[u, some, :] = (x * inverse_rms(x) * g_ref[...]).astype(BF16)
            return carry

        lax.fori_loop(0, hp // HD, norm, 0)
        keep(0, gather, u).start()
        own_half(dy_hbm, u).start()
    barrier(grid)
    for mask in MASKS:
        pos_copy(mask, grid.me).start()
    for u in BOTH:
        keep(0, gather, u).wait()
    gather.begin()
    pos_scr[grid.me] = pos_ref[...]
    clear(qz_scr)
    clear(acc_scr)
    for u in BOTH:
        own_half(dy_hbm, u).wait()
        keep(2, gather_dy, u).start()
    for which in range(3):
        w_copy(which).wait()
        w_scr[span(which, WIDTH)] = wtmp[which].T

    inv = inv_ref[...]

    def stores(u, cols):
        pairs = (q_st, q_hbm), (k_st, k_hbm), (cos_st, cos_hbm), (sin_st, sin_hbm)
        return [pltpu.make_async_copy(st.at[u], hbm.at[:, cols], osem.at[u, n]) for n, (st, hbm) in enumerate(pairs)]

    def group(g, carry):
        stage = g // 2
        one = (stage + 2) // 3
        two = stage // 3
        first = (stage // 2) * (1 - two)
        halves = first, 1 - first
        owners = grid.flip(two, one, g % 2), grid.flip(one, two, g % 2)
        offs = [pl.multiple_of(owners[u] * piece + halves[u] * hp, PAIR) for u in BOTH]

        slot = 2 * (g // 7)

        def load(u, slot, rows):
            return pltpu.make_async_copy(r_all.at[rows], buf.at[slot + u], lsem.at[slot + u])

        def loads():
            for u in BOTH:
                load(u, 0, pl.ds(offs[u], hp)).start()

        def partner():
            for mask in MASKS:
                pos_copy(mask, grid.xor(mask)).wait_recv()
            for u in BOTH:
                keep(2, gather_dy, u).wait()
            gather.arrived('own')
            loads()

        def far():
            gather.third()
            gather_dy.begin()
            loads()
            gather.arrived('cdA', 'cdB')
            for u in BOTH:
                load(u, 2, block(2 * grid.xor(7) + u, hp)).start()

        def then_load(event, *names):
            def run():
                event(*names)
                loads()

            return run

        events = (
            partner, then_load(gather.first), then_load(gather.arrived, 'cxA', 'cyB'),
            then_load(gather.second), then_load(gather.arrived, 'cxB', 'cyA'), far,
        )
        for number, event in enumerate(events):
            pl.when(g == number + 1)(event)

        for u in BOTH:
            cols = pl.ds(offs[u], hp)

            @pl.when(g > 0)
            def _():
                load(u, slot, cols).wait()
                for copy in stores(u, cols):
                    copy.wait()

            lines = hp // PAIR
            angles = beside([inv * pos_scr[owners[u], pl.ds(halves[u] * lines + i, 1), :].astype(F32) for i in range(lines)])
            cos = jnp.cos(angles) * MSCALE
            sin = jnp.sin(angles) * MSCALE
            cos_st[u] = cos
            sin_st[u] = sin

            def rope(t):
                t1, t2 = t[:HALF], t[HALF:]
                return stack([t1 * cos - t2 * sin, t2 * cos + t1 * sin]).astype(BF16)

            qkv = dot_nt(w_scr[...], buf[slot + u])
            for h in range(HEADS):
                q = rope(qkv[span(h, HD)]) * BF16(0.125)
                q_st[u, span(h, HD)] = q
                qz_scr[h, span(h % 2, HD), cols] = q
                k_st[u, span(h, HD)] = rope(qkv[span(HEADS + h, HD)])
            kn_scr[cols, :] = k_st[u].T
            v_scr[:, cols] = qkv[2 * WIDTH:].astype(BF16)
            for copy in stores(u, cols):
                copy.start()
        return carry

    lax.fori_loop(0, NDEV, group, 0)
    for u in BOTH:
        for copy in stores(u, block(u, hp)):
            copy.wait()
    v_out = pltpu.make_async_copy(v_scr, v_hbm, fsem.at[0])
    v_out.start()

    bufs = ((s_scr0, s_scr1), (s_scr2, s_scr3))

    def at(i):
        return block(i, BLK)

    def two_heads(pair):
        return block(pair, PAIR)

    def outputs(pair):
        rows = block(pair, ROWS)
        return [
            pltpu.make_async_copy(o_scr.at[two_heads(pair)], o_hbm.at[two_heads(pair)], fsem.at[1]),
            pltpu.make_async_copy(on_scr.at[:, two_heads(pair)], on_hbm.at[:, two_heads(pair)], fsem.at[2]),
            pltpu.make_async_copy(lse_scr.at[rows], lse_hbm.at[rows], fsem.at[3]),
        ]

    def forward(pair, carry):
        m_scr[...] = jnp.full_like(m_scr, MASK_VALUE)
        clear(l_scr)

        def score(i, j, b, h, masked):
            s = dot_nn(kn_scr[at(j), two_heads(pair)], qz_scr[2 * pair + h, :, at(i)])
            if masked:
                krow = lax.broadcasted_iota(jnp.int32, s.shape, 0)
                qcol = lax.broadcasted_iota(jnp.int32, s.shape, 1)
                s = jnp.where(krow <= qcol, s, MASK_VALUE)
            bufs[b][h][...] = s
            row = 2 * b + h
            mx_scr[span(row, 1), :] = jnp.max(s, axis=0, keepdims=True)

        def weigh(i, j, b, h):
            row = span(h, 1)
            m_old = m_scr[row, at(i)]
            m_new = jnp.maximum(m_old, mx_scr[span(2 * b + h, 1), :])
            m_scr[row, at(i)] = m_new
            alpha = jnp.exp2((m_old - m_new) * LOG2E)
            p = jnp.exp2((bufs[b][h][...] - m_new) * LOG2E)
            l_scr[row, at(i)] = l_scr[row, at(i)] * alpha + column_sum(p)
            v = v_scr[pl.ds(pl.multiple_of((2 * pair + h) * HD, HD), HD), at(j)]
            acc_scr[h, :, at(i)] = acc_scr[h, :, at(i)] * alpha + dot_nn(v, p.astype(BF16))

        def both(later, now, b, masked):
            for h in BOTH:
                score(*later, 1 - b, h, masked)
                weigh(*now, b, h)

        for h in BOTH:
            score(0, 0, 0, h, True)

        def diagonal(t, carry):
            i = 2 * t
            both((i + 1, i + 1), (i, i), 0, True)
            e = jnp.minimum(i + 2, nblk - 1)
            both((e, e), (i + 1, i + 1), 1, True)
            return carry

        lax.fori_loop(0, nblk // 2, diagonal, 0)

        def following(i, j):
            wrap = (j + 1) // i
            return i + wrap, (j + 1) * (1 - wrap)

        for h in BOTH:
            score(1, 0, 0, h, False)

        def below(t, carry):
            i, j = carry
            i1, j1 = following(i, j)
            both((i1, j1), (i, j), 0, False)
            i2, j2 = following(i1, j1)
            both((jnp.minimum(i2, nblk - 1), j2), (i1, j1), 1, False)
            return i2, j2

        def segment(g, carry):
            @pl.when((pair == 0) & (g == 1))
            def _():
                gather_dy.first()

            @pl.when((pair == 1) & (g == 0))
            def _():
                gather_dy.second()

            @pl.when((pair == 1) & (g == 2))
            def _():
                gather_dy.third()
                for copy in outputs(0):
                    copy.wait()
                for mask in MASKS:
                    o_copy(mask, grid.me).start()

            a, b, c = SEGMENTS
            start = jnp.where(g == 0, 0, jnp.where(g == 1, a, b))
            stop = jnp.where(g == 0, a, jnp.where(g == 1, b, c))
            return lax.fori_loop(start, stop, below, carry)

        lax.fori_loop(0, len(SEGMENTS), segment, (jnp.int32(1), jnp.int32(0)))

        def finish(i, carry):
            outs = []
            for h in BOTH:
                l = l_scr[span(h, 1), at(i)]
                outs.append((acc_scr[h, :, at(i)] / l).astype(BF16))
                lse_scr[pl.ds(pair * ROWS + h, 1), at(i)] = m_scr[span(h, 1), at(i)] + jnp.log(l)
            o = stack(outs)
            o_scr[two_heads(pair), at(i)] = o
            on_scr[at(i), two_heads(pair)] = o.T
            return carry

        lax.fori_loop(0, nblk, finish, 0)
        for copy in outputs(pair):
            copy.start()
        return carry

    lax.fori_loop(0, 2, forward, 0)
    for copy in outputs(1):
        copy.wait()
    v_out.wait()
    gather.sent()
    gather_dy.last()
    for mask in MASKS:
        pos_copy(mask, grid.me).wait_send()
        o_copy(mask, grid.xor(mask)).wait_recv()
        o_copy(mask, grid.me).wait_send()


def front_call(x, gain, pos, inv_freq, w_qkv, dy):
    piece, hidden = x.shape
    seq = piece * NDEV
    hp = piece // 2
    hbm = pl.BlockSpec(memory_space=pl.ANY)
    vmem = pl.BlockSpec(memory_space=pltpu.VMEM)
    dma = pltpu.SemaphoreType.DMA
    all_b = lambda *shape: jax.ShapeDtypeStruct(shape, BF16)
    all_f = lambda *shape: jax.ShapeDtypeStruct(shape, F32)
    b = lambda *shape: pltpu.VMEM(shape, BF16)
    f = lambda *shape: pltpu.VMEM(shape, F32)
    tr = all_b(WIDTH, seq)
    tab = all_f(HALF, seq)
    return pl.pallas_call(
        front_kernel,
        out_shape=(all_b(seq, hidden), all_b(seq, hidden), tr, tr, tr, tab, tab, tr, all_b(seq, WIDTH), all_f(2 * ROWS, seq), all_b(NDEV, piece, PAIR)),
        in_specs=[hbm, vmem, vmem, vmem, hbm, hbm],
        out_specs=(hbm,) * 11,
        scratch_shapes=[
            b(3, hidden, WIDTH), b(3 * WIDTH, hidden), b(4, hp, hidden), pltpu.VMEM((NDEV, piece // PAIR, PAIR), jnp.int32),
            b(2, WIDTH, hp), b(2, WIDTH, hp), f(2, HALF, hp), f(2, HALF, hp), b(HEADS, PAIR, seq), b(seq, WIDTH), b(WIDTH, seq),
            f(2, HD, seq), f(ROWS, seq), f(ROWS, seq), f(BLK, BLK), f(BLK, BLK), f(BLK, BLK), f(BLK, BLK), f(ROWS, BLK),
            b(WIDTH, seq), b(seq, WIDTH), f(2 * ROWS, seq),
            dma((3,)), dma((4,)), dma((2, 4)), dma((4,)), dma((4,)), dma((NDEV,)), dma((NDEV,)), dma((NDEV,)), dma((NDEV,)),
        ] + GATHER_SEMS * 2,
        compiler_params=pltpu.CompilerParams(collective_id=0, has_side_effects=True, vmem_limit_bytes=VMEM_LIMIT),
        cost_estimate=cost(2 * seq * seq * WIDTH),
        name="front",
    )(x, gain, pos.reshape(piece // PAIR, PAIR), inv_freq.reshape(HALF, 1), w_qkv, dy)


def split3(value):
    hi = value.astype(BF16).astype(F32)
    mid = (value - hi).astype(BF16).astype(F32)
    return hi, mid, value - hi - mid


FIRST, SECOND, THIRD = 6, 9, 2


def bwd_kernel(dy_ref, r_ref, q_ref, o_ref, k_ref, v_ref, lse_ref, cos_ref, sin_ref, w_hbm, on_hbm, x_hbm, o_first,
               y_hbm, o_recv, gwo_all, dn_recv, gw_all, gw_last,
               do_scr, w_scr, gwo_scr, qa_scr, doa_scr, ka_scr, va_scr, dq_scr, dk_scr, dv_scr, dn_scr, gw_scr, o_scr, x_scr, wc_scr, p_scr0, ds_scr0, p_scr1, ds_scr1,
               ysem, wsem, lsem, o_ssem, o_rsem, d_ssem, d_rsem, g_ssem, g_rsem):
    s = pl.program_id(0)
    nblk = do_scr.shape[1] // BLK
    grid = Grid()
    width, hidden = w_scr.shape
    piece = x_hbm.shape[0]
    row64 = lax.broadcasted_iota(jnp.int32, (HD, BLK), 0)

    def blk(t):
        return block(t, BLK)

    def o_copy(mask, owner):
        return exchange_o(grid, on_hbm, o_recv, 1, mask, owner, o_ssem, o_rsem)

    def dn_cols(owner):
        return pl.ds(pl.multiple_of(owner * piece, 128), piece)

    def dn_copy(h, mask, owner):
        src = dn_scr.at[h % 2, :, dn_cols(grid.xor(mask))]
        return pltpu.make_async_remote_copy(src, dn_recv.at[h, owner], d_ssem.at[h, mask], d_rsem.at[h, mask], device_id={'cp': grid.xor(mask)}, device_id_type=MESH)

    def dn_own(h):
        return pltpu.make_async_copy(dn_scr.at[h % 2, :, dn_cols(grid.me)], dn_recv.at[h, grid.me], lsem.at[0])

    def gw_own(h):
        return pltpu.make_async_copy(gw_scr.at[h % 2], gw_all.at[grid.me, h], lsem.at[1])

    def keep_last():
        return pltpu.make_async_copy(gw_scr.at[(HEADS - 1) % 2], gw_last, lsem.at[1])

    def gw_gather(h, far=True):
        half = hidden // 2
        return Gather(grid, None, lambda owner, first, halves: gw_all.at[owner, h, :, pl.ds(first * half, halves * half)], lambda k: g_ssem.at[h, k], lambda k: g_rsem.at[h, k], far)

    def project_y():
        wide = wc_scr.shape[2]

        def chunk(c):
            return span(c, wide)

        def w_chunk(c):
            return pltpu.make_async_copy(w_hbm.at[:, chunk(c)], wc_scr.at[c % 2], ysem.at[c % 2])

        def o_part(src, owner, pair):
            cols = pl.ds(pl.multiple_of(owner * width + pair * PAIR, PAIR), PAIR)
            return pltpu.make_async_copy(src, o_scr.at[:, cols], ysem.at[2])

        parts = [pltpu.make_async_copy(x_hbm, x_scr, ysem.at[2])]
        for pair, recv in enumerate((o_first, o_recv)):
            parts += [o_part(recv.at[grid.xor(mask)], grid.xor(mask), pair) for mask in MASKS]
            parts.append(o_part(on_hbm.at[block(grid.me, piece), span(pair, PAIR)], grid.me, pair))
        w_chunk(0).start()
        for part in parts:
            part.start()
        for part in parts:
            part.wait()
        for c in range(hidden // wide):
            w_chunk(c).wait()
            if c + 1 < hidden // wide:
                w_chunk(c + 1).start()
            part = dot_nn(o_scr[...], wc_scr[c % 2])
            x_scr[:, chunk(c)] = (x_scr[:, chunk(c)].astype(F32) + part).astype(BF16)
        out = pltpu.make_async_copy(x_scr, y_hbm, ysem.at[2])
        out.start()
        out.wait()

    gwo_gather = row_gather(grid, None, gwo_all, width, g_ssem.at[HEADS], g_rsem.at[HEADS])

    @pl.when(s == 0)
    def _():
        w_copy = pltpu.make_async_copy(w_hbm.at[block(grid.me, width)], w_scr, wsem)
        w_copy.start()
        barrier(grid)
        for mask in MASKS:
            o_copy(mask, grid.me).start()
        w_copy.wait()
        clear(gwo_scr)

    @pl.when(s < nblk)
    def _():
        gwo_scr[...] += dot_nn(o_ref[:, blk(s)], dy_ref[...])
        do_scr[:, blk(s)] = dot_nt(w_scr[...], dy_ref[...]).astype(BF16)

    @pl.when(s == nblk)
    def _():
        own = pltpu.make_async_copy(gwo_scr, gwo_gather.dst(grid.me, 0, 2), lsem.at[1])
        own.start()
        own.wait()
        gwo_gather.begin()

    t = s - nblk
    h = t // nblk
    j = t % nblk

    def send_head(h):
        dn_own(h).start()
        for mask in MASKS:
            dn_copy(h, mask, grid.me).start()

    @pl.when((t >= nblk) & (j == 0))
    def _():
        send_head(h - 1)
        gw_own(h - 1).start()

    @pl.when((t >= nblk) & (j == 1))
    def _():
        gw_own(h - 1).wait()
        dn_own(h - 1).wait()
        gw_gather(h - 1).begin()

    @pl.when((t >= 2 * nblk) & (j == 0))
    def _():
        for mask in MASKS:
            dn_copy(h - 2, mask, grid.me).wait_send()

    end = HEADS - 1

    @pl.when(t == 2 * nblk + 1)
    def _():
        for mask in MASKS:
            o_copy(mask, grid.xor(mask)).wait_recv()
        project_y()

    @pl.when((t >= nblk) & (h < end) & (j == FIRST))
    def _():
        gw_gather(h - 1).first()

    @pl.when((h == end) & (j == FIRST))
    def _():
        gw_gather(end - 1, False).first()

    @pl.when((t >= nblk) & (j == SECOND))
    def _():
        gw_gather(h - 1).second()

    @pl.when((t >= 2 * nblk) & (j == THIRD))
    def _():
        gw_gather(h - 2).third()

    @pl.when(t == 5)
    def _():
        gwo_gather.first()

    @pl.when(t == 8)
    def _():
        gwo_gather.second()

    @pl.when(t == nblk + THIRD)
    def _():
        gwo_gather.third()

    @pl.when(t >= 0)
    def _():
        rows = block(h, HD)

        @pl.when(j == 0)
        def _():
            clear(dq_scr)
            gw_scr[h % 2] = jnp.zeros(gw_scr.shape[1:], F32)

            def augment(data, stat):
                hi, mid, lo = split3(-stat)
                extra = jnp.where(row64 == 0, hi, jnp.where(row64 == 1, mid, jnp.where(row64 == 2, lo, 0.0))).astype(BF16)
                return stack([data, extra]).T

            def prep(i, carry):
                cols = blk(i)
                do_h = do_scr[rows, cols]
                delta = column_sum(do_h.astype(F32) * o_ref[rows, cols].astype(F32))
                qa_scr[cols, :] = augment(q_ref[rows, cols], lse_ref[pl.ds((h // 2) * ROWS + h % 2, 1), cols])
                doa_scr[cols, :] = augment(do_h, delta)
                return carry

            lax.fori_loop(0, nblk, prep, 0)

        ones = jnp.where(row64 < 3, 1.0, 0.0).astype(BF16)
        ka_scr[...] = stack([k_ref[rows, :], ones])
        va_scr[...] = stack([v_ref[rows, :], ones])
        clear(dk_scr)
        clear(dv_scr)

        bufs = (p_scr0, ds_scr0), (p_scr1, ds_scr1)

        def scores(i):
            return dot_nn(qa_scr[blk(i), :], ka_scr[...])

        def weights(s, i, b):
            p = jnp.exp2(s * LOG2E)
            bufs[b][0][...] = p.astype(BF16)
            return p

        def score_grads(p, i, b):
            bufs[b][1][...] = (p * dot_nn(doa_scr[blk(i), :], va_scr[...])).astype(BF16)

        def add_dv(i, b):
            dv_scr[...] += dot_nn(do_scr[rows, blk(i)], bufs[b][0][...])

        def add_dk(i, b):
            dk_scr[...] += dot_nn(q_ref[rows, blk(i)], bufs[b][1][...])

        def add_dq(i, b):
            dq_scr[:, blk(i)] += dot_nt(k_ref[rows, :], bufs[b][1][...])

        def both(later, now, b):
            s = scores(later)
            add_dv(now, b)
            p = weights(s, later, 1 - b)
            add_dk(now, b)
            score_grads(p, later, 1 - b)
            add_dq(now, b)

        first = scores(j)
        qrow = lax.broadcasted_iota(jnp.int32, first.shape, 0)
        kcol = lax.broadcasted_iota(jnp.int32, first.shape, 1)
        score_grads(weights(jnp.where(kcol <= qrow, first, MASK_VALUE), j, 0), j, 0)

        def body(u, carry):
            i = j + 2 * u
            both(i + 1, i, 0)
            both(jnp.minimum(i + 2, nblk - 1), i + 1, 1)
            return carry

        lax.fori_loop(0, (nblk - j) // 2, body, 0)

        @pl.when((nblk - j) % 2 == 1)
        def _():
            for add in (add_dv, add_dk, add_dq):
                add(nblk - 1, 0)

        cos = cos_ref[...]
        sin = sin_ref[...]

        def unrope(v, scale):
            v1 = v[:HALF] * scale
            v2 = v[HALF:] * scale
            return [v1 * cos + v2 * sin, v2 * cos - v1 * sin]

        grads = stack(unrope(dq_scr[:, blk(j)], 0.125) + unrope(dk_scr[...], 1.0) + [dv_scr[...]]).astype(BF16)
        dn_scr[h % 2, :, blk(j)] = grads
        gw_scr[h % 2] += dot_nn(grads, r_ref[...])

    @pl.when(s == pl.num_programs(0) - 1)
    def _():
        keep_last().start()
        send_head(end)
        keep_last().wait()
        dn_own(end).wait()
        for mask in MASKS:
            o_copy(mask, grid.me).wait_send()
            for head in range(HEADS):
                dn_copy(head, mask, grid.xor(mask)).wait_recv()
            for head in range(HEADS - 2, HEADS):
                dn_copy(head, mask, grid.me).wait_send()
        gwo_gather.last()
        for head in range(end):
            gw_gather(head, head < end - 1).last()


def bwd_call(dy_all, r_all, q_t, o_t, k_t, v_t, lse, cos_t, sin_t, w_out, o_n, x, o_first):
    seq, hidden = dy_all.shape
    width = q_t.shape[0]
    half = cos_t.shape[0]
    ndev = NDEV
    piece = seq // ndev
    nblk = seq // BLK
    hbm = pl.BlockSpec(memory_space=pl.ANY)
    whole = lambda *shape: pl.BlockSpec(shape, lambda s: (0, 0), pipeline_mode=pl.Buffered(1))
    cols = lambda rows: pl.BlockSpec((rows, BLK), lambda s: (0, lax.rem(s, nblk)))
    rblk = lambda s: jnp.where(s < nblk, 0, lax.rem(s, nblk))
    rows = 3 * HD
    dma = pltpu.SemaphoreType.DMA
    return pl.pallas_call(
        bwd_kernel,
        out_shape=(
            jax.ShapeDtypeStruct((piece, hidden), BF16),
            jax.ShapeDtypeStruct((ndev, piece, PAIR), BF16),
            jax.ShapeDtypeStruct((ndev * width, hidden), F32),
            jax.ShapeDtypeStruct((HEADS, ndev, rows, piece), BF16),
            jax.ShapeDtypeStruct((ndev, HEADS - 1, rows, hidden), F32),
            jax.ShapeDtypeStruct((rows, hidden), F32),
        ),
        grid=(nblk * (1 + HEADS),),
        in_specs=[
            pl.BlockSpec((BLK, hidden), lambda s: (jnp.minimum(s, nblk - 1), 0)),
            pl.BlockSpec((BLK, hidden), lambda s: (rblk(s), 0)),
            whole(width, seq), whole(width, seq),
            cols(width), cols(width),
            whole(2 * ROWS, seq),
            cols(half), cols(half),
            hbm, hbm, hbm, hbm,
        ],
        out_specs=(hbm,) * 6,
        scratch_shapes=[
            pltpu.VMEM((width, seq), BF16), pltpu.VMEM((width, hidden), BF16), pltpu.VMEM((width, hidden), F32),
            pltpu.VMEM((seq, PAIR), BF16), pltpu.VMEM((seq, PAIR), BF16),
            pltpu.VMEM((PAIR, BLK), BF16), pltpu.VMEM((PAIR, BLK), BF16),
            pltpu.VMEM((HD, seq), F32), pltpu.VMEM((HD, BLK), F32), pltpu.VMEM((HD, BLK), F32),
            pltpu.VMEM((2, rows, seq), BF16), pltpu.VMEM((2, rows, hidden), F32),
            pltpu.VMEM((piece, hidden), BF16), pltpu.VMEM((piece, hidden), BF16), pltpu.VMEM((2, hidden, BLK), BF16),
        ] + [pltpu.VMEM((BLK, BLK), BF16)] * 4 + [
            dma((3,)), dma, dma((2,)), dma((ndev,)), dma((ndev,)), dma((HEADS, ndev)), dma((HEADS, ndev)), dma((HEADS + 1, COPIES)), dma((HEADS + 1, COPIES)),
        ],
        compiler_params=params(1, collective_id=2, has_side_effects=True),
        cost_estimate=cost(5 * seq * seq * width),
        name="backward",
    )(dy_all, r_all, q_t, o_t, k_t, v_t, lse, cos_t, sin_t, w_out, o_n, x, o_first)


def flip_bits(m, d):
    return sum((m // k + d // k) % 2 * k for k in (1, 2, 4))


def write_columns(step, steps, rows_of, place_of, out, stage, sem):
    parts = sem.shape[1]
    lanes = stage.shape[2] // parts
    slot = step % 2

    def copies(slot):
        places = [place_of(k) for k in range(parts)]
        return [pltpu.make_async_copy(stage.at[slot, :, span(k, lanes)], out.at[rows, pl.ds(pl.multiple_of(col, PAIR), lanes)], sem.at[slot, k]) for k, (rows, col) in enumerate(places)]

    @pl.when(step >= 2)
    def _():
        for copy in copies(slot):
            copy.wait()

    for k in range(parts):
        stage[slot, :, span(k, lanes)] = rows_of(k).T
    for copy in copies(slot):
        copy.start()

    @pl.when(step == steps - 1)
    def _():
        for copy in copies(1 - slot) + copies(slot):
            copy.wait()


NEAR = lambda p, k: (1 - p) * k + p * (2 + 2 * k)
FAR = lambda p, k: (1 - p) * (3 + 2 * k) + p * (6 + k)


def place_call(dev, gw_all, last, g_wqkv, first, mask_of, third=()):
    _, known, rows, hidden = gw_all.shape
    heads = known - first
    lanes = (heads + 1) * HD
    groups = len(last) // 2
    flat = [part for parts in (*last, *third) for part in parts]

    def kernel(d_ref, *refs):
        w, p = pl.program_id(0), pl.program_id(1)
        known_refs, flat_refs, (_, out, stage, sem) = refs[:2], list(refs[2:2 + len(flat)]), refs[2 + len(flat):]
        ends = [beside([flat_refs.pop(0)[...] for _ in parts]) for parts in (*last, *third)]

        def rows_of(k):
            end = jnp.where(p == 0, ends[k], ends[k - 2])
            rows = [ends[k + 2]] if third else [known_refs[k][0, h] for h in range(heads)]
            return stack(rows + [end])

        def place_of(k):
            return slice(None), (w * NDEV + flip_bits(mask_of(p, k), d_ref[0])) * WIDTH + first * HD

        write_columns(groups * w + p, groups * 3, rows_of, place_of, out, stage, sem)

    def known_spec(k):
        return pl.BlockSpec((1, heads, HD, hidden), lambda w, p, d: (flip_bits(mask_of(p, k), d[0]), first // heads, w, 0))

    hbm = pl.BlockSpec(memory_space=pl.ANY)
    operands = [gw_all, gw_all, *flat, g_wqkv]
    return pl.pallas_call(
        kernel,
        out_shape=jax.ShapeDtypeStruct(g_wqkv.shape, F32),
        grid_spec=pltpu.PrefetchScalarGridSpec(
            num_scalar_prefetch=1,
            grid=(3, groups),
            in_specs=[known_spec(0), known_spec(1)] + [pl.BlockSpec((HD, part.shape[1]), lambda w, p, d: (w, 0)) for part in flat] + [hbm],
            out_specs=hbm,
            scratch_shapes=[pltpu.VMEM((2, hidden, 2 * lanes), F32), pltpu.SemaphoreType.DMA((2, 2))],
        ),
        input_output_aliases={len(operands): 0},
        compiler_params=params(2),
        cost_estimate=cost(20e9),
        name="place",
    )(dev, *operands)


def dx_kernel(d_ref, dn_ref, wq_ref, wk_ref, wv_ref, x_hbm, g_ref, dy_hbm, wout_ref, y_ref, gw_ref, dx_out, gg_out, wout_out, y_out, gw_out, acc_scr, stage, x_ref, dy_ref, sem, own_sem):
    s = pl.program_id(0)
    steps = pl.num_programs(0)
    loads = [pltpu.make_async_copy(src, dst, own_sem.at[k]) for k, (src, dst) in enumerate(((x_hbm, x_ref), (dy_hbm, dy_ref)))]

    @pl.when(s == 0)
    def _():
        for load in loads:
            load.start()

    hidden = acc_scr.shape[0]
    rhs = stack([dn_ref[h, 0, span(w, HD)] for w in range(3) for h in range(HEADS)])
    part = dot_nn(beside([wq_ref[...], wk_ref[...], wv_ref[...]]), rhs)
    wout_out[...] = wout_ref[...]
    y_out[...] = y_ref[...]

    def rows_of(w):
        return stack([gw_ref[0, h, span(w, HD)] for h in BOTH])

    def place_of(w):
        cut = hidden // 2
        owner = flip_bits(FAR(s // 4, s // 2 % 2), d_ref[0])
        return pl.ds(pl.multiple_of(s % 2 * cut, cut), cut), (w * NDEV + owner) * WIDTH

    write_columns(s, steps, rows_of, place_of, gw_out, stage, sem)

    @pl.when(s == 0)
    def _():
        acc_scr[...] = part

    @pl.when(s > 0)
    def _():
        acc_scr[...] += part

    @pl.when(s == steps - 1)
    def _():
        gain = g_ref[...]
        clear(gg_out)
        for load in loads:
            load.wait()

        def tokens(c, carry):
            some = block(c, PAIR)
            dn = acc_scr[:, some].T
            x = x_ref[some, :].astype(F32)
            inv = inverse_rms(x)
            x_hat = x * inv
            gg_out[...] += column_sum(dn * x_hat)
            d_hat = dn * gain
            mean = jnp.mean(d_hat * x_hat, axis=-1, keepdims=True)
            dx_out[some, :] = (dy_ref[some, :].astype(F32) + inv * (d_hat - x_hat * mean)).astype(BF16)
            return carry

        lax.fori_loop(0, x_ref.shape[0] // PAIR, tokens, 0)


def dx_call(dev, dn_recv, w_qkv, x, gain, dy, wout_all, y, gw_all):
    _, ndev, rows, piece = dn_recv.shape
    hidden = w_qkv.shape[0]
    zero = lambda s, d: (0, 0)
    hbm = pl.BlockSpec(memory_space=pl.ANY)
    wspec = lambda which: pl.BlockSpec((hidden, WIDTH), lambda s, d: (0, which * ndev + s))
    whole = lambda *shape: pl.BlockSpec(shape, zero, pipeline_mode=pl.Buffered(1))
    rowblk = lambda rows: pl.BlockSpec((rows // ndev, hidden), lambda s, d: (s, 0))
    return pl.pallas_call(
        dx_kernel,
        out_shape=(
            jax.ShapeDtypeStruct((piece, hidden), BF16), jax.ShapeDtypeStruct((1, hidden), F32),
            jax.ShapeDtypeStruct((hidden, hidden), F32), jax.ShapeDtypeStruct((piece, hidden), BF16), jax.ShapeDtypeStruct((hidden, 3 * hidden), F32),
        ),
        grid_spec=pltpu.PrefetchScalarGridSpec(
            num_scalar_prefetch=1,
            grid=(ndev,),
            in_specs=[
                pl.BlockSpec((HEADS, 1, rows, piece), lambda s, d: (0, s, 0, 0)), wspec(0), wspec(1), wspec(2),
                hbm, whole(1, hidden), hbm, rowblk(hidden), rowblk(piece),
                pl.BlockSpec((1, 2, rows, hidden // 2), lambda s, d: (flip_bits(FAR(s // 4, s // 2 % 2), d[0]), 0, 0, s % 2)),
            ],
            out_specs=(whole(piece, hidden), whole(1, hidden), rowblk(hidden), rowblk(piece), hbm),
            scratch_shapes=[pltpu.VMEM((hidden, piece), F32), pltpu.VMEM((2, hidden // 2, 3 * PAIR), F32)] + [pltpu.VMEM((piece, hidden), BF16)] * 2 + [pltpu.SemaphoreType.DMA((2, 3)), pltpu.SemaphoreType.DMA((2,))],
        ),
        compiler_params=params(1),
        cost_estimate=cost(2 * piece * hidden * 3 * hidden),
        name="dx",
    )(dev, dn_recv, w_qkv, w_qkv, w_qkv, x, gain, dy, wout_all, y, gw_all)


def solution(mesh):
    ndev = mesh.shape['cp']

    def device_fn(x_in, positions, long_factor, norm_gain, w_qkv, w_out, grad_y):
        _, piece, hidden = x_in.shape
        seq = piece * ndev
        dev = lax.axis_index('cp').astype(jnp.int32).reshape(1)
        x = x_in[0]
        dy = grad_y[0]
        gain = norm_gain.reshape(1, hidden)
        half = long_factor.shape[0]
        exponent = jnp.arange(half, dtype=F32) * (1.0 / half)
        inv_freq = 1.0 / (long_factor * jnp.power(10000.0, exponent))
        r_all, dy_all, q_t, k_t, v_t, cos_t, sin_t, o_t, o_n, lse, o_first = front_call(x, gain, positions, inv_freq, w_qkv, dy)
        y_out, _, wout_all, dn_recv, gw_all, own = bwd_call(dy_all, r_all, q_t, o_t, k_t, v_t, lse, cos_t, sin_t, w_out, o_n, x, o_first)

        def swap(value, mask):
            return lax.ppermute(value, 'cp', [(i, i ^ mask) for i in range(ndev)])

        cut = hidden // 2

        def third_of(mask, start):
            some = lax.dynamic_slice(gw_all, (dev[0] ^ mask, HEADS - 2, 0, start), (1, 1, own.shape[0], cut))
            return some.reshape(own.shape[0], cut)

        third = swap(third_of(2, 0), 4), swap(third_of(4, cut), 2)
        from_x, from_y, from_c = swap(own, 2), swap(own, 4), swap(own, 1)
        grad_x, gain, g_wout, y_out, g_wqkv = dx_call(dev, dn_recv, w_qkv, x, gain, dy, wout_all, y_out, gw_all)
        from_x, from_y, from_c, gain, g_wqkv = lax.optimization_barrier((from_x, from_y, from_c, gain, g_wqkv))
        diag = swap(from_x[:, :cut], 4), swap(from_y[:, cut:], 2)
        from_cx, from_cy, gain_x = swap(from_x, 1), swap(from_y, 1), swap(gain, 2)
        g_wqkv = place_call(dev, gw_all, [(own,), (from_c,), (from_x,), (from_y,)], g_wqkv, 0, NEAR)
        diag, third, from_cx, from_cy, gain_x, g_wqkv = lax.optimization_barrier((diag, third, from_cx, from_cy, gain_x, g_wqkv))
        third_c = [swap(part, 1) for part in third]
        from_cd = [swap(part, 1) for part in diag]
        gain = gain + gain_x
        gain_y = swap(gain, 4)
        g_wqkv = place_call(dev, gw_all, [(from_cx,), (from_cy,)], g_wqkv, 2, FAR)
        from_cd, third_c, gain_y, g_wqkv = lax.optimization_barrier((from_cd, third_c, gain_y, g_wqkv))
        gain = gain + gain_y
        gain_c = swap(gain, 1)
        g_wqkv = place_call(dev, gw_all, [diag, from_cd], g_wqkv, 2, lambda p, k: FAR(1, k), [third, third_c])
        g_gain = (gain + gain_c).reshape(hidden)
        return y_out[None], grad_x[None], g_gain, g_wqkv, g_wout

    seq_spec = P('dp', 'cp')
    return jax.shard_map(device_fn, mesh=mesh, in_specs=(seq_spec, P(('dp', 'cp')), P(), P(), P(), P(), seq_spec), out_specs=(seq_spec, seq_spec, P('dp'), P('dp'), P('dp')), check_vma=False)
```
